32 devices in a mesh: nodes: 8 (over y, x, core), heads: 4 (over z).
Axes of the slice: x: 2, y: 2, z: 4, core: 2. Of those that a mesh axis runs over, the one named last changes fastest.
Arguments:
- features: bfloat16 [32768, 256], P(('nodes', 'heads')), may hold values from -6 to 6
- target: float32 [32768], P(('nodes', 'heads')), may hold values from -6 to 6
- counts: int32 [256], replicated, may hold values from 1 to 128, as said below
- neighbours: int32 [256, 8], P('nodes'), may hold values from 0 to 255, as said below
- edge_kinds: int32 [256, 9], P('nodes'), may hold values from 0 to 63
- enc_weight: float32 [256, 512], P('heads'), may hold values from -0.375 to 0.375
- enc_first: float32 [256, 512], P('heads'), may hold values from -0.0625 to 0.0625
- enc_second: float32 [256, 512], P('heads'), may hold values from 1.5258789e-05 to 0.00048828125
- qkv_weight: float32 [512, 1536], P('heads'), may hold values from -0.25 to 0.25
- qkv_first: float32 [512, 1536], P('heads'), may hold values from -0.0625 to 0.0625
- qkv_second: float32 [512, 1536], P('heads'), may hold values from 1.5258789e-05 to 0.00048828125
- out_weight: float32 [512, 512], P('heads'), may hold values from -2 to 2
- out_first: float32 [512, 512], P('heads'), may hold values from -0.125 to 0.125
- out_second: float32 [512, 512], P('heads'), may hold values from 6.1035156e-05 to 0.001953125
- up_weight: float32 [512, 2048], P('heads'), may hold values from -0.25 to 0.25
- up_first: float32 [512, 2048], P('heads'), may hold values from -0.0625 to 0.0625
- up_second: float32 [512, 2048], P('heads'), may hold values from 1.5258789e-05 to 0.00048828125
- down_weight: float32 [2048, 512], P('heads'), may hold values from -0.125 to 0.125
- down_first: float32 [2048, 512], P('heads'), may hold values from -0.0625 to 0.0625
- down_second: float32 [2048, 512], P('heads'), may hold values from 1.5258789e-05 to 0.00048828125
- vec_weight: float32 [6, 512], P(None, 'heads')
- vec_first: float32 [6, 512], P(None, 'heads'), may hold values from -0.125 to 0.125
- vec_second: float32 [6, 512], P(None, 'heads'), may hold values from 6.1035156e-05 to 0.001953125
Outputs:
- loss_out: float32 [1], replicated
- enc_new: float32 [256, 512], P('heads')
- enc_first_new: float32 [256, 512], P('heads')
- enc_second_new: float32 [256, 512], P('heads')
- qkv_new: float32 [512, 1536], P('heads')
- qkv_first_new: float32 [512, 1536], P('heads')
- qkv_second_new: float32 [512, 1536], P('heads')
- out_new: float32 [512, 512], P('heads')
- out_first_new: float32 [512, 512], P('heads')
- out_second_new: float32 [512, 512], P('heads')
- up_new: float32 [512, 2048], P('heads')
- up_first_new: float32 [512, 2048], P('heads')
- up_second_new: float32 [512, 2048], P('heads')
- down_new: float32 [2048, 512], P('heads')
- down_first_new: float32 [2048, 512], P('heads')
- down_second_new: float32 [2048, 512], P('heads')
- vec_new: float32 [6, 512], P(None, 'heads')
- vec_first_new: float32 [6, 512], P(None, 'heads')
- vec_second_new: float32 [6, 512], P(None, 'heads')
- enc_copy: bfloat16 [256, 512], P('heads')
- qkv_copy: bfloat16 [512, 1536], P('heads')
- out_copy: bfloat16 [512, 512], P('heads')
- up_copy: bfloat16 [512, 2048], P('heads')
- down_copy: bfloat16 [2048, 512], P('heads')
The draws below stay inside these ranges and needn't reach their ends.
Inputs may be any that keep to these rules, and one draw needn't show every extreme that they name: `counts`: live slots of a block come first; the first block of every 32 consecutive blocks is full. Each block's 8 neighbours are distinct, differ from the block, and lie among the blocks of its own run of 32 consecutive blocks or of the runs just before and after it, the last run followed by the first.
All inputs are finite; a program needn't handle non-finite values.
Results may differ from the reference program's by a relative error of at most 0.0019.
The reference program's roundings to bfloat16 on the way count: a program that leaves them out, or rounds other values in their place, can miss the bound.
Values may be sent and summed in bfloat16 or wider, within the bound.
A program may use at most 256 MiB of HBM per device.

```python
import math
import jax
import jax.numpy as jnp
from jax import lax

D = 512
HEADS = 8
FF = 2048
FEAT = 256
BLOCK = 128
NBR = 8
SLOTS = 9
EDGE_TYPES = 64
ADAM_STEP = 3
BLK_DEV = 8
GROUP = 32
NBLOCKS = 256
NODES = 32768


def draw_counts(key, part):
    floor_key, count_key = jax.random.split(key)
    device_total = NBLOCKS // BLK_DEV
    floor_rows = jax.random.randint(floor_key, (device_total, 1), BLOCK // 4, BLOCK + 1, dtype=jnp.int32)
    drawn_rows = jax.random.randint(count_key, (device_total, BLK_DEV), floor_rows, BLOCK + 1, dtype=jnp.int32).reshape(NBLOCKS)
    block_ids = jnp.arange(NBLOCKS, dtype=jnp.int32)
    return jnp.where(block_ids % GROUP == 0, BLOCK, drawn_rows).astype(jnp.int32)


def draw_neighbours(key, part):
    window = 3 * GROUP
    spot_ids = jnp.arange(window, dtype=jnp.int32)
    scores = jax.random.randint(key, (NBLOCKS, window), 0, 1 << 20, dtype=jnp.int32) * window + spot_ids[None, :]
    block_ids = jnp.arange(NBLOCKS, dtype=jnp.int32)
    own_spot = block_ids % GROUP + GROUP
    scores = jnp.where(spot_ids[None, :] == own_spot[:, None], -1, scores)
    _, chosen = lax.top_k(scores, NBR)
    group_total = NBLOCKS // GROUP
    picked_group = (block_ids[:, None] // GROUP - 1 + chosen // GROUP) % group_total
    return (picked_group * GROUP + chosen % GROUP).astype(jnp.int32)


def draw_vec_weight(key, part):
    base_draw = jax.random.normal(key, (6, D), jnp.float32)
    row_scale = jnp.array([0.5, 0.2, 0.2, 0.2, D ** (-0.5), 1.0], jnp.float32)
    row_shift = jnp.array([0.0, 1.0, 1.0, 1.0, 0.0, 0.0], jnp.float32)
    return base_draw * row_scale[:, None] + row_shift[:, None]


def set_ends(drawn, rng, smallest, top_value):
    longest = drawn.shape.index(max(drawn.shape))
    spots = []
    for shift in (0, 1):
        where = [jax.random.randint(jax.random.fold_in(rng, axis), (), 0, length) for axis, length in enumerate(drawn.shape)]
        where[longest] = (where[longest] + shift) % drawn.shape[longest]
        spots.append(tuple(where))
    return drawn.at[spots[0]].set(smallest).at[spots[1]].set(top_value)


def block_levels(stream_key, extent, shards, smallest, largest):
    gain = 1.0
    for dim, parts in shards:
        heights = jax.random.uniform(jax.random.fold_in(jax.random.fold_in(stream_key, 6), dim), (parts,), jnp.float32, smallest / len(shards), largest / len(shards))
        gain = gain * jnp.repeat(jnp.exp(heights), extent[dim] // parts).reshape((-1,) + (1,) * (len(extent) - 1 - dim))
    return gain


def bell_draw(own_key, dims, spread, bound, cuts=(), held_as=jnp.bfloat16):
    gain = block_levels(own_key, dims, cuts, -0.22, 0.18) if cuts else 1.0
    result = jax.random.normal(own_key, dims, jnp.float32) * spread * gain
    return jnp.minimum(jnp.maximum(result, -bound), bound).astype(held_as)


def setup_inputs(seed: int = 0) -> dict:
    keys = jax.random.split(jax.random.key(seed), 24)
    return {
        "features": bell_draw(keys[0], (NODES, FEAT), 1.0, 6.0, ((0, 32),)),
        "target": bell_draw(keys[1], (NODES,), 1.0, 6.0, ((0, 32),), jnp.float32),
        "counts": draw_counts(jax.random.fold_in(keys[23], 71), 0),
        "neighbours": draw_neighbours(jax.random.fold_in(keys[23], 71), 0),
        "edge_kinds": set_ends(jax.random.randint(keys[4], (NBLOCKS, SLOTS), 0, EDGE_TYPES), jax.random.fold_in(keys[4], 1), 0, EDGE_TYPES - 1).astype(jnp.int32),
        "enc_weight": bell_draw(keys[5], (FEAT, D), FEAT ** -0.5, 0.375, ((0, 4),), jnp.float32),
        "enc_first": bell_draw(keys[6], (FEAT, D), (2.0 * NODES ** -0.5), 0.0625, ((0, 4),), jnp.float32),
        "enc_second": jnp.clip(jnp.exp(math.log(0.00048828125) - 3.465736 * jax.random.uniform(keys[7], (FEAT, D), jnp.float32) ** block_levels(keys[7], (FEAT, D), ((0, 4),), -0.2, 0.2)), 1.52587890625e-05, 0.00048828125),
        "qkv_weight": bell_draw(keys[8], (D, 3 * D), D ** -0.5, 0.25, ((0, 4),), jnp.float32),
        "qkv_first": bell_draw(keys[9], (D, 3 * D), (2.0 * NODES ** -0.5), 0.0625, ((0, 4),), jnp.float32),
        "qkv_second": jnp.clip(jnp.exp(math.log(0.00048828125) - 3.465736 * jax.random.uniform(keys[10], (D, 3 * D), jnp.float32) ** block_levels(keys[10], (D, 3 * D), ((0, 4),), -0.2, 0.2)), 1.52587890625e-05, 0.00048828125),
        "out_weight": bell_draw(keys[11], (D, D), (D // 64) ** -0.5, 2.0, ((0, 4),), jnp.float32),
        "out_first": bell_draw(keys[12], (D, D), (4.0 * NODES ** -0.5), 0.125, ((0, 4),), jnp.float32),
        "out_second": jnp.clip(jnp.exp(math.log(0.001953125) - 3.465736 * jax.random.uniform(keys[13], (D, D), jnp.float32) ** block_levels(keys[13], (D, D), ((0, 4),), -0.2, 0.2)), 6.103515625e-05, 0.001953125),
        "up_weight": bell_draw(keys[14], (D, FF), D ** -0.5, 0.25, ((0, 4),), jnp.float32),
        "up_first": bell_draw(keys[15], (D, FF), (2.0 * NODES ** -0.5), 0.0625, ((0, 4),), jnp.float32),
        "up_second": jnp.clip(jnp.exp(math.log(0.00048828125) - 3.465736 * jax.random.uniform(keys[16], (D, FF), jnp.float32) ** block_levels(keys[16], (D, FF), ((0, 4),), -0.2, 0.2)), 1.52587890625e-05, 0.00048828125),
        "down_weight": bell_draw(keys[17], (FF, D), FF ** -0.5, 0.125, ((0, 4),), jnp.float32),
        "down_first": bell_draw(keys[18], (FF, D), (2.0 * NODES ** -0.5), 0.0625, ((0, 4),), jnp.float32),
        "down_second": jnp.clip(jnp.exp(math.log(0.00048828125) - 3.465736 * jax.random.uniform(keys[19], (FF, D), jnp.float32) ** block_levels(keys[19], (FF, D), ((0, 4),), -0.2, 0.2)), 1.52587890625e-05, 0.00048828125),
        "vec_weight": draw_vec_weight(jax.random.fold_in(keys[23], 71), 0),
        "vec_first": bell_draw(keys[21], (6, D), (4.0 * NODES ** -0.5), 0.125, ((1, 4),), jnp.float32),
        "vec_second": jnp.clip(jnp.exp(math.log(0.001953125) - 3.465736 * jax.random.uniform(keys[22], (6, D), jnp.float32) ** block_levels(keys[22], (6, D), ((1, 4),), -0.2, 0.2)), 6.103515625e-05, 0.001953125),
    }


@jax.custom_vjp
def low(v):
    return lax.optimization_barrier(v.astype(jnp.bfloat16)).astype(jnp.float32)

@jax.custom_vjp
def low_back(v):
    return v

def low_keep(v):
    return (low(v), None)

def low_pass(kept, grad):
    return (grad,)

def back_keep(v):
    return (v, None)

def back_low(kept, grad):
    return (low(grad),)
low.defvjp(low_keep, low_pass)
low_back.defvjp(back_keep, back_low)
highest = lax.Precision.HIGHEST
beta_one = 0.5
beta_two = 0.5
learn_rate = 0.02
weight_decay = 0.1
adam_eps = 1e-08
norm_eps = 1e-05

def normalize(values):
    average = lax.optimization_barrier(jnp.mean(values, axis=-1, keepdims=True))
    centred = values - average
    variance = lax.optimization_barrier(jnp.mean(centred * centred, axis=-1, keepdims=True))
    return centred * lax.rsqrt(variance + norm_eps)

def adamw(weight, first_moment, second, gradient):
    first_new = beta_one * first_moment + (1.0 - beta_one) * gradient
    second_new = beta_two * second + (1.0 - beta_two) * gradient * gradient
    first_hat = first_new / (1.0 - beta_one ** ADAM_STEP)
    second_hat = second_new / (1.0 - beta_two ** ADAM_STEP)
    weight_new = weight - learn_rate * (first_hat / (jnp.sqrt(second_hat) + adam_eps) + weight_decay * weight)
    return (weight_new, first_new, second_new)

def forward(enc_copy, qkv_copy, out_copy, up_copy, down_copy, vec_copy, features, target, counts, neighbours, edge_kinds):
    head_size = D // HEADS
    slot_count = NBR + 1
    dev_rows = BLK_DEV * BLOCK
    dev_count = NBLOCKS // BLK_DEV
    enc_bias = vec_copy[0]
    gain_one = vec_copy[1]
    gain_two = vec_copy[2]
    gain_three = vec_copy[3]
    head_vec = vec_copy[4]
    edge_bias = vec_copy[5].reshape(D // HEADS, HEADS)

    def encode(feature_rows):
        resid_rows = low_back(jnp.dot(feature_rows, enc_copy, precision=highest)) + enc_bias
        act_one = low(normalize(resid_rows) * gain_one)
        qkv_rows = low(low_back(jnp.dot(act_one, qkv_copy, precision=highest)))
        return (resid_rows, qkv_rows)
    resid_in, qkv_all = lax.map(jax.checkpoint(encode), features.reshape(dev_count, dev_rows, FEAT))
    qkv_blocks = qkv_all.reshape(NBLOCKS, BLOCK, HEADS, 3, head_size)
    queries = qkv_blocks[:, :, :, 0]
    keys_all = qkv_blocks[:, :, :, 1]
    values_all = qkv_blocks[:, :, :, 2]
    block_ids = jnp.arange(NBLOCKS, dtype=jnp.int32)[:, None]
    key_ids = jnp.concatenate([block_ids, neighbours.astype(jnp.int32)], axis=1)
    kind_hot = jax.nn.one_hot(edge_kinds, D // HEADS, dtype=jnp.float32)
    slot_bias = jnp.einsum('bst,th->bsh', kind_hot, edge_bias, precision=highest)
    key_live = jnp.arange(BLOCK, dtype=jnp.int32)[None, None, :] < counts[key_ids][:, :, None]
    step_count = NBLOCKS // 4

    def attend(inputs):
        query_part, ids_part, bias_part, live_part = inputs
        key_part = keys_all[ids_part].reshape(4, slot_count * BLOCK, HEADS, head_size)
        value_part = values_all[ids_part].reshape(4, slot_count * BLOCK, HEADS, head_size)
        raw_scores = low_back(jnp.einsum('bqhe,bkhe->bhqk', query_part, key_part, precision=highest) * head_size ** (-0.5))
        bias_keys = jnp.transpose(jnp.repeat(bias_part, BLOCK, axis=1), (0, 2, 1))
        scores = jnp.where(live_part.reshape(4, 1, 1, slot_count * BLOCK), raw_scores + bias_keys[:, :, None, :], -1e+30)
        attn_probs = low(jax.nn.softmax(scores, axis=-1))
        out_part = jnp.einsum('bhqk,bkhe->bqhe', attn_probs, value_part, precision=highest)
        return low(low_back(out_part)).reshape(4 * BLOCK, D)
    attn_all = lax.map(jax.checkpoint(attend), (queries.reshape(step_count, 4, BLOCK, HEADS, head_size), key_ids.reshape(step_count, 4, slot_count), slot_bias.reshape(step_count, 4, slot_count, HEADS), key_live.reshape(step_count, 4, slot_count, BLOCK)))
    row_live = (jnp.arange(BLOCK, dtype=jnp.int32)[None, :] < counts[:, None]).reshape(dev_count, dev_rows)

    def finish(inputs):
        resid_rows, attn_rows, target_rows, live_rows = inputs
        hidden_one = resid_rows + low_back(jnp.dot(attn_rows, out_copy, precision=highest))
        act_two = low(normalize(hidden_one) * gain_two)
        up_val = low_back(jnp.dot(act_two, up_copy, precision=highest))
        act_up = low(jax.nn.gelu(up_val))
        hidden_two = hidden_one + low_back(jnp.dot(act_up, down_copy, precision=highest))
        predicted = jnp.dot(normalize(hidden_two) * gain_three, head_vec, precision=highest)
        pred_error = predicted - target_rows
        return jnp.sum(jnp.where(live_rows, pred_error * pred_error, 0.0))
    partial_sums = lax.map(jax.checkpoint(finish), (resid_in, attn_all.reshape(dev_count, dev_rows, D), target.reshape(dev_count, dev_rows), row_live))
    return jnp.sum(partial_sums) / jnp.sum(counts).astype(jnp.float32)

def reference(features, target, counts, neighbours, edge_kinds, enc_weight, enc_first, enc_second, qkv_weight, qkv_first, qkv_second, out_weight, out_first, out_second, up_weight, up_first, up_second, down_weight, down_first, down_second, vec_weight, vec_first, vec_second):
    feature_data = features.astype(jnp.float32)

    def loss_of(enc_copy, qkv_copy, out_copy, up_copy, down_copy, vec_copy):
        return forward(enc_copy, qkv_copy, out_copy, up_copy, down_copy, vec_copy, feature_data, target, counts, neighbours, edge_kinds)
    loss_value, pull_back = jax.vjp(loss_of, low(enc_weight), low(qkv_weight), low(out_weight), low(up_weight), low(down_weight), low(vec_weight))
    gradients = pull_back(jnp.ones_like(loss_value))
    enc_res = adamw(enc_weight, enc_first, enc_second, gradients[0])
    qkv_res = adamw(qkv_weight, qkv_first, qkv_second, gradients[1])
    out_res = adamw(out_weight, out_first, out_second, gradients[2])
    up_res = adamw(up_weight, up_first, up_second, gradients[3])
    down_res = adamw(down_weight, down_first, down_second, gradients[4])
    vec_res = adamw(vec_weight, vec_first, vec_second, gradients[5])
    return (loss_value.reshape(1), enc_res[0], enc_res[1], enc_res[2], qkv_res[0], qkv_res[1], qkv_res[2], out_res[0], out_res[1], out_res[2], up_res[0], up_res[1], up_res[2], down_res[0], down_res[1], down_res[2], vec_res[0], vec_res[1], vec_res[2], enc_res[0].astype(jnp.bfloat16), qkv_res[0].astype(jnp.bfloat16), out_res[0].astype(jnp.bfloat16), up_res[0].astype(jnp.bfloat16), down_res[0].astype(jnp.bfloat16))
```

```python
import functools

import jax
import jax.numpy as jnp
from jax import lax
from jax.experimental import pallas as pl
from jax.experimental.pallas import tpu as pltpu
from jax.sharding import PartitionSpec as P

BLOCK = 128
NT = (((1,), (1,)), ((), ()))
NN = (((1,), (0,)), ((), ()))
f32 = jnp.float32
bf16 = jnp.bfloat16


def dotf(a, b, dims):
    return lax.dot_general(a, b, dims, preferred_element_type=f32)


def head_rows(x, hl, hs, cp):
    if hl == 1:
        return x
    lane = lax.broadcasted_iota(jnp.int32, (BLOCK, cp), 1)
    zero = jnp.zeros_like(x)
    return jnp.concatenate([jnp.where(lane // hs == h, x, zero) for h in range(hl)], axis=0)


def ones_lane(hl, cp, ka):
    rows = hl * BLOCK
    lane = lax.broadcasted_iota(jnp.int32, (rows, ka - cp), 1)
    return jnp.where(lane == 0, 1.0, 0.0).astype(bf16)


def attend_kernel(hl, hs, cp, ka, slots, pos_ref, q_ref, brow_ref, kaug_ref, vt_ref, o_ref, lse_ref, s_ref, p_ref):
    b = pl.program_id(0)
    rows = hl * BLOCK
    q2 = head_rows(q_ref[...], hl, hs, cp)
    qa = jnp.concatenate([q2, ones_lane(hl, cp, ka)], axis=1) if ka > cp else q2
    top = None
    for s in range(slots):
        p = pos_ref[b * slots + s]
        ks = kaug_ref[pl.ds(pl.multiple_of(p * BLOCK, BLOCK), BLOCK), :]
        sc = dotf(ks, qa, NT)
        s_ref[s] = sc
        t = jnp.max(sc, axis=0, keepdims=True) + brow_ref[0, s:s + 1, :]
        top = t if top is None else jnp.maximum(top, t)
    tot = jnp.zeros((1, rows), f32)
    for s in range(slots):
        e = jnp.exp(s_ref[s] - (top - brow_ref[0, s:s + 1, :]))
        s_ref[s] = e
        tot = tot + jnp.sum(e, axis=0, keepdims=True)
    lse_ref[0] = top + jnp.log(tot)
    inv = 1.0 / tot
    vs = []
    for s in range(slots):
        p_ref[s * BLOCK:(s + 1) * BLOCK, :] = (s_ref[s] * inv).astype(bf16)
        vs.append(vt_ref[pos_ref[b * slots + s]])
    ot = dotf(jnp.concatenate(vs, axis=1), p_ref[...], NN)
    parts = [ot[h * hs:(h + 1) * hs, h * BLOCK:(h + 1) * BLOCK] for h in range(hl)]
    if hl * hs < cp:
        parts.append(jnp.zeros((cp - hl * hs, BLOCK), f32))
    o_ref[...] = jnp.concatenate(parts, axis=0).T.astype(bf16)


def attend(pos, q, brow, kaug, vt, hl, hs):
    cp, ka = q.shape[1], kaug.shape[1]
    nb = q.shape[0] // BLOCK
    slots = brow.shape[1]
    rows = hl * BLOCK
    whole = lambda a: pl.BlockSpec(a.shape, lambda i, *_: (0,) * a.ndim, pipeline_mode=pl.Buffered(1))
    return pl.pallas_call(
        functools.partial(attend_kernel, hl, hs, cp, ka, slots),
        grid_spec=pltpu.PrefetchScalarGridSpec(
            num_scalar_prefetch=1, grid=(nb,),
            in_specs=[pl.BlockSpec((BLOCK, cp), lambda i, *_: (i, 0)),
                      pl.BlockSpec((1, slots, rows), lambda i, *_: (i, 0, 0)),
                      whole(kaug), whole(vt)],
            out_specs=[pl.BlockSpec((BLOCK, cp), lambda i, *_: (i, 0)),
                       pl.BlockSpec((1, 1, rows), lambda i, *_: (i, 0, 0))],
            scratch_shapes=[pltpu.VMEM((slots, BLOCK, rows), f32), pltpu.VMEM((slots * BLOCK, rows), bf16)]),
        out_shape=[jax.ShapeDtypeStruct(q.shape, bf16), jax.ShapeDtypeStruct((nb, 1, rows), f32)],
        compiler_params=pltpu.CompilerParams(vmem_limit_bytes=60 << 20),
        name="attend",
    )(pos, q, brow, kaug, vt)


def attend_back_kernel(hl, hs, cp, ka, slots, scale, pos_ref, q_ref, do_ref, o_ref, lse_ref, brow_ref, kaug_ref, v_ref, kt_ref,
                       dq_ref, dkv_ref, edge_ref):
    b = pl.program_id(0)
    rows = hl * BLOCK

    @pl.when(b == 0)
    def _():
        dkv_ref[...] = jnp.zeros_like(dkv_ref)

    q2 = head_rows(q_ref[...], hl, hs, cp)
    qa = jnp.concatenate([q2, ones_lane(hl, cp, ka)], axis=1) if ka > cp else q2
    do = do_ref[...]
    do2 = head_rows(do, hl, hs, cp)
    prod = (do.astype(f32) * o_ref[...].astype(f32)).T
    dd = jnp.concatenate([jnp.sum(prod[h * hs:(h + 1) * hs], axis=0, keepdims=True) for h in range(hl)], axis=1)
    lse = lse_ref[0]
    dqt = jnp.zeros((cp, rows), f32)
    for s in range(slots):
        p = pos_ref[b * slots + s]
        at = pl.ds(pl.multiple_of(p * BLOCK, BLOCK), BLOCK)
        sc = dotf(kaug_ref[at, :], qa, NT)
        pr = jnp.exp(sc - (lse - brow_ref[0, s:s + 1, :]))
        dp = dotf(v_ref[at, :], do2, NT)
        ds = pr * (dp - dd)
        edge_ref[0, s:s + 1, :] = jnp.sum(ds, axis=0, keepdims=True)
        dsl = ds.astype(bf16)
        dv = dotf(pr.astype(bf16), do2, NN)
        dk = dotf(dsl, q2, NN)
        dkv_ref[at, 0:cp] += dk
        dkv_ref[at, cp:2 * cp] += dv
        dqt = dqt + dotf(kt_ref[p], dsl, NN)
    parts = [dqt[h * hs:(h + 1) * hs, h * BLOCK:(h + 1) * BLOCK] for h in range(hl)]
    if hl * hs < cp:
        parts.append(jnp.zeros((cp - hl * hs, BLOCK), f32))
    dq_ref[...] = (jnp.concatenate(parts, axis=0).T * scale).astype(bf16)


def attend_back(pos, q, do, o, lse, brow, kaug, v, kt, hl, hs):
    cp, ka = q.shape[1], kaug.shape[1]
    nb = q.shape[0] // BLOCK
    slots = brow.shape[1]
    rows = hl * BLOCK
    whole = lambda a: pl.BlockSpec(a.shape, lambda i, *_: (0,) * a.ndim, pipeline_mode=pl.Buffered(1))
    tile = pl.BlockSpec((BLOCK, cp), lambda i, *_: (i, 0))
    return pl.pallas_call(
        functools.partial(attend_back_kernel, hl, hs, cp, ka, slots, hs ** -0.5),
        grid_spec=pltpu.PrefetchScalarGridSpec(
            num_scalar_prefetch=1, grid=(nb,),
            in_specs=[tile, tile, tile,
                      pl.BlockSpec((1, 1, rows), lambda i, *_: (i, 0, 0)),
                      pl.BlockSpec((1, slots, rows), lambda i, *_: (i, 0, 0)),
                      whole(kaug), whole(v), whole(kt)],
            out_specs=[tile, pl.BlockSpec((v.shape[0], 2 * cp), lambda i, *_: (0, 0), pipeline_mode=pl.Buffered(1)),
                       pl.BlockSpec((1, slots, rows), lambda i, *_: (i, 0, 0))]),
        out_shape=[jax.ShapeDtypeStruct(q.shape, bf16), jax.ShapeDtypeStruct((v.shape[0], 2 * cp), f32),
                   jax.ShapeDtypeStruct((nb, slots, rows), f32)],
        compiler_params=pltpu.CompilerParams(vmem_limit_bytes=60 << 20),
        name="attend_back",
    )(pos, q, do, o, lse, brow, kaug, v, kt)
norm_eps = 1e-05


def encode_kernel(cp, ka, cols, scale, per_group, cnt_ref, fp_ref, fo_ref, fn_ref, enc_ref, bias_ref, gain_ref, w_ref,
                  kaug_ref, kt_ref, v_ref, vt_ref, q_ref, x_ref):
    i = pl.program_id(0)
    group = i // per_group
    tile = x_ref.shape[0]
    for g, ref in enumerate((fp_ref, fo_ref, fn_ref)):
        @pl.when(group == g)
        def _(ref=ref):
            x_ref[...] = ref[...]
    resid = dotf(x_ref[...], enc_ref[...], NN) + bias_ref[...]
    centred = resid - jnp.mean(resid, axis=-1, keepdims=True)
    variance = jnp.mean(centred * centred, axis=-1, keepdims=True)
    act = (centred * lax.rsqrt(variance + norm_eps) * gain_ref[...]).astype(bf16)
    kv = dotf(act, w_ref[:, cp:], NN).astype(bf16)
    key, value = kv[:, :cp], kv[:, cp:]
    row = lax.broadcasted_iota(jnp.int32, (BLOCK, 128), 0)
    lane = lax.broadcasted_iota(jnp.int32, (BLOCK, 128), 1)
    first = i * (tile // BLOCK)
    dead = jnp.concatenate(
        [jnp.where((row >= cnt_ref[first + j]) & (lane == cols % 128), -1e30, 0.0) for j in range(tile // BLOCK)], axis=0).astype(bf16)
    if ka > cp:
        kaug_ref[:, :cp] = key
        kaug_ref[:, cp:] = dead
    else:
        kaug_ref[...] = key + dead
    v_ref[...] = value
    for j in range(tile // BLOCK):
        kt_ref[j] = key[j * BLOCK:(j + 1) * BLOCK].T
        vt_ref[j] = value[j * BLOCK:(j + 1) * BLOCK].T

    @pl.when(group == 1)
    def _():
        q = (dotf(act, w_ref[:, :cp], NN) * scale).astype(bf16)
        if ka == cp:
            lanes = lax.broadcasted_iota(jnp.int32, q.shape, 1)
            q = jnp.where(lanes == cols, jnp.ones_like(q), q)
        q_ref[...] = q


def encode(counts, prev, own, nxt, enc, bias, gain, w, cp, ka, cols, scale, tile=512):
    rows, feat = own.shape
    width = enc.shape[1]
    per = rows // tile
    blocks = tile // BLOCK
    whole = lambda a: pl.BlockSpec(a.shape, lambda i, *_: (0,) * a.ndim, pipeline_mode=pl.Buffered(1))
    part = lambda g: pl.BlockSpec((tile, feat), lambda i, *_: (jnp.clip(i - g * per, 0, per - 1), 0))
    return pl.pallas_call(
        functools.partial(encode_kernel, cp, ka, cols, scale, per),
        grid_spec=pltpu.PrefetchScalarGridSpec(
            num_scalar_prefetch=1, grid=(3 * per,),
            in_specs=[part(0), part(1), part(2), whole(enc), whole(bias), whole(gain), whole(w)],
            out_specs=[pl.BlockSpec((tile, ka), lambda i, *_: (i, 0)),
                       pl.BlockSpec((blocks, cp, BLOCK), lambda i, *_: (i, 0, 0)),
                       pl.BlockSpec((tile, cp), lambda i, *_: (i, 0)),
                       pl.BlockSpec((blocks, cp, BLOCK), lambda i, *_: (i, 0, 0)),
                       pl.BlockSpec((tile, cp), lambda i, *_: (jnp.clip(i - per, 0, per - 1), 0))],
            scratch_shapes=[pltpu.VMEM((tile, feat), bf16)]),
        out_shape=[jax.ShapeDtypeStruct((3 * rows, ka), bf16),
                   jax.ShapeDtypeStruct((3 * rows // BLOCK, cp, BLOCK), bf16),
                   jax.ShapeDtypeStruct((3 * rows, cp), bf16),
                   jax.ShapeDtypeStruct((3 * rows // BLOCK, cp, BLOCK), bf16),
                   jax.ShapeDtypeStruct((rows, cp), bf16)],
        compiler_params=pltpu.CompilerParams(vmem_limit_bytes=60 << 20),
        name="encode",
    )(counts, prev, own, nxt, enc, bias, gain, w)


def encode_back_kernel(cp, per_group, fp_ref, fo_ref, fn_ref, dkv_ref, dq_ref, enct_ref, bias_ref, gain_ref, wq_ref, wkv_ref,
                       dw_ref, denc_ref, dgain_ref, dbias_ref, x_ref, g_ref):
    i = pl.program_id(0)
    group = i // per_group
    tile = x_ref.shape[0]
    width = enct_ref.shape[0]
    reps = tile // 128

    @pl.when(i == 0)
    def _():
        for ref in (dw_ref, denc_ref, dgain_ref, dbias_ref):
            ref[...] = jnp.zeros_like(ref)

    for g, ref in enumerate((fp_ref, fo_ref, fn_ref)):
        @pl.when(group == g)
        def _(ref=ref):
            x_ref[...] = ref[...]
    x = x_ref[...]
    wide = lambda c: jnp.concatenate([c] * reps, axis=1)
    fold = lambda a: functools.reduce(jnp.add, [a[:, r * 128:(r + 1) * 128] for r in range(reps)])
    resid = dotf(enct_ref[...], x, NT) + wide(bias_ref[...])
    centred = resid - jnp.sum(resid, axis=0, keepdims=True) * (1.0 / width)
    variance = jnp.sum(centred * centred, axis=0, keepdims=True) * (1.0 / width)
    inv = lax.rsqrt(variance + norm_eps)
    norm = centred * inv
    gain = wide(gain_ref[...])
    act = (norm * gain).astype(bf16)
    dkv = dkv_ref[...].astype(bf16)
    g_ref[...] = dotf(wkv_ref[...], dkv, NT)
    dw_ref[:, cp:] += dotf(act, dkv, NN)

    @pl.when(group == 1)
    def _():
        dq = dq_ref[...]
        g_ref[...] += dotf(wq_ref[...], dq, NT)
        dw_ref[:, :cp] += dotf(act, dq, NN)

    grad = g_ref[...]
    dgain_ref[...] += fold(grad * norm)
    back = grad * gain
    mean_one = jnp.sum(back, axis=0, keepdims=True) * (1.0 / width)
    mean_two = jnp.sum(back * norm, axis=0, keepdims=True) * (1.0 / width)
    din = inv * (back - mean_one - norm * mean_two)
    dbias_ref[...] += fold(din)
    denc_ref[...] += dotf(din.astype(bf16), x, NN)


def encode_back(prev, own, nxt, dkv, dq, enct, bias, gain, wq, wkv, tile=512):
    rows, feat = own.shape
    width = enct.shape[0]
    cp = dq.shape[1]
    per = rows // tile
    whole = lambda a: pl.BlockSpec(a.shape, lambda i: (0,) * a.ndim, pipeline_mode=pl.Buffered(1))
    part = lambda g: pl.BlockSpec((tile, feat), lambda i: (jnp.clip(i - g * per, 0, per - 1), 0))
    keep = lambda s: pl.BlockSpec(s, lambda i: (0,) * len(s), pipeline_mode=pl.Buffered(1))
    shapes = [(width, 3 * cp), (width, feat), (width, 128), (width, 128)]
    return pl.pallas_call(
        functools.partial(encode_back_kernel, cp, per),
        grid=(3 * per,),
        in_specs=[part(0), part(1), part(2), pl.BlockSpec((tile, 2 * cp), lambda i: (i, 0)),
                  pl.BlockSpec((tile, cp), lambda i: (jnp.clip(i - per, 0, per - 1), 0)),
                  whole(enct), whole(bias), whole(gain), whole(wq), whole(wkv)],
        out_specs=[keep(s) for s in shapes],
        out_shape=[jax.ShapeDtypeStruct(s, f32) for s in shapes],
        scratch_shapes=[pltpu.VMEM((tile, feat), bf16), pltpu.VMEM((width, tile), f32)],
        compiler_params=pltpu.CompilerParams(vmem_limit_bytes=60 << 20),
        name="encode_back",
    )(prev, own, nxt, dkv, dq, enct, bias, gain, wq, wkv)
D = 512
HEADS = 8
NBR = 8
ADAM_STEP = 3
highest = lax.Precision.HIGHEST
beta_one = 0.5
beta_two = 0.5
learn_rate = 0.02
weight_decay = 0.1
adam_eps = 1e-08


def normalize(values):
    average = jnp.mean(values, axis=-1, keepdims=True)
    centred = values - average
    variance = jnp.mean(centred * centred, axis=-1, keepdims=True)
    return centred * lax.rsqrt(variance + norm_eps)


def adamw(weight, first_moment, second, gradient):
    first_new = beta_one * first_moment + (1.0 - beta_one) * gradient
    second_new = beta_two * second + (1.0 - beta_two) * gradient * gradient
    first_hat = first_new / (1.0 - beta_one**ADAM_STEP)
    second_hat = second_new / (1.0 - beta_two**ADAM_STEP)
    weight_new = weight - learn_rate * (
        first_hat / (jnp.sqrt(second_hat) + adam_eps) + weight_decay * weight
    )
    return (weight_new, first_new, second_new)


def spread_flat(gradient, heads_count, nodes_count):
    return jnp.transpose(gradient.reshape(heads_count, nodes_count, -1), (1, 0, 2)).reshape(-1)


def from_behind(value, axis, steps):
    count = lax.axis_size(axis)
    pairs = [(source, (source + steps) % count) for source in range(count)]
    return lax.ppermute(value, axis, pairs)


def local(
    features, target, counts, neighbours, edge_kinds,
    enc_weight, enc_first, enc_second, qkv_weight, qkv_first, qkv_second,
    out_weight, out_first, out_second, up_weight, up_first, up_second,
    down_weight, down_first, down_second, vec_weight, vec_first, vec_second,
):
    heads_count = lax.axis_size("heads")
    nodes_count = lax.axis_size("nodes")
    head_index = lax.axis_index("heads")
    node_index = lax.axis_index("nodes")
    row_count = features.shape[0]
    own_blocks = row_count // BLOCK
    group_blocks = own_blocks * heads_count
    group_rows = group_blocks * BLOCK
    hl = HEADS // heads_count
    hs = D // HEADS
    cols = hl * hs
    cp = -(-cols // 128) * 128
    ka = -(-(cols + 1) // 128) * 128
    kinds = D // HEADS
    slots = NBR + 1
    low = lambda a: a.astype(bf16)
    gather = lambda a, axis: lax.all_gather(low(a), "heads", axis=axis, tiled=True)

    own_feat = lax.all_gather(features, "heads", axis=0, tiled=True)
    prev_feat = from_behind(own_feat, "nodes", 1)
    next_feat = from_behind(own_feat, "nodes", -1)
    enc_b = gather(enc_weight, 0)
    vectors = gather(vec_weight, 1).astype(f32)
    qkv_cols = lax.all_to_all(low(qkv_weight), "heads", split_axis=1, concat_axis=0, tiled=True)
    qkv_cols = jnp.transpose(qkv_cols.reshape(D, hl, 3, hs), (0, 2, 1, 3)).reshape(D, 3, cols)
    qkv_cols = jnp.pad(qkv_cols, ((0, 0), (0, 0), (0, cp - cols))).reshape(D, 3 * cp)
    out_b, up_b, down_b = gather(out_weight, 0), gather(up_weight, 0), gather(down_weight, 0)

    enc_bias, gain_one, gain_two, gain_three, head_vec = (vectors[r] for r in range(5))
    edge_local = lax.dynamic_slice_in_dim(vectors[5].reshape(kinds, HEADS), head_index * hl, hl, 1)
    own_counts = lax.dynamic_slice_in_dim(counts, (node_index * heads_count + head_index) * own_blocks, own_blocks)
    row_live = (jnp.arange(BLOCK, dtype=jnp.int32)[None, :] < own_counts[:, None]).reshape(row_count).astype(f32)
    live_total = jnp.sum(counts).astype(f32)

    def group_counts(offset):
        return lax.dynamic_slice_in_dim(counts, (node_index + offset) % nodes_count * group_blocks, group_blocks)

    pool_counts = jnp.concatenate([group_counts(nodes_count - 1), group_counts(0), group_counts(1)])
    relative = (neighbours // group_blocks - node_index + 1) % nodes_count
    nbr_pos = relative * group_blocks + neighbours % group_blocks
    self_pos = group_blocks + jnp.arange(group_blocks, dtype=jnp.int32)
    key_pos = jnp.concatenate([self_pos[:, None], nbr_pos], axis=1).reshape(-1)
    kind_hot = jax.nn.one_hot(edge_kinds, kinds, dtype=f32)
    slot_bias = jnp.einsum("bst,th->bsh", kind_hot, edge_local, precision=highest)
    bias_rows = jnp.repeat(slot_bias, BLOCK, axis=2)

    kaug, kt, value, vt, query = encode(
        pool_counts, prev_feat, own_feat, next_feat, enc_b, enc_bias[None], gain_one[None], qkv_cols, cp, ka, cols, hs**-0.5)
    attn_group, lse = attend(key_pos, query, bias_rows, kaug, vt, hl, hs)
    attn_rows = lax.all_to_all(attn_group[:, :cols], "heads", split_axis=0, concat_axis=1, tiled=True)

    resid_in = jnp.dot(features, enc_b, preferred_element_type=f32) + enc_bias
    hidden_one = resid_in + jnp.dot(attn_rows, out_b, preferred_element_type=f32)
    norm_two, norm_two_pull = jax.vjp(normalize, hidden_one)
    act_two = low(norm_two * gain_two)
    up_val = jnp.dot(act_two, up_b, preferred_element_type=f32)
    gelu_val, gelu_pull = jax.vjp(jax.nn.gelu, up_val)
    act_up = low(gelu_val)
    hidden_two = hidden_one + jnp.dot(act_up, down_b, preferred_element_type=f32)
    norm_three, norm_three_pull = jax.vjp(normalize, hidden_two)
    scaled = norm_three * gain_three
    predicted = jnp.sum(scaled * head_vec, axis=-1)
    pred_error = predicted - target
    local_loss = jnp.sum(row_live * pred_error * pred_error)
    total_loss = lax.psum(local_loss, ("nodes", "heads"))
    grad_pred = 2.0 * row_live * pred_error / live_total
    grad_scaled = grad_pred[:, None] * head_vec
    grad_head_vec = jnp.sum(grad_pred[:, None] * scaled, axis=0)
    grad_gain_three = jnp.sum(grad_scaled * norm_three, axis=0)
    grad_two = norm_three_pull(grad_scaled * gain_three)[0]
    grad_two_low = low(grad_two)
    grad_down = jnp.einsum("rf,rd->fd", act_up, grad_two_low, preferred_element_type=f32)
    grad_act = jnp.einsum("rd,fd->rf", grad_two_low, down_b, preferred_element_type=f32)
    grad_up_low = low(gelu_pull(grad_act)[0])
    grad_up = jnp.einsum("rd,rf->df", act_two, grad_up_low, preferred_element_type=f32)
    grad_act_two = jnp.einsum("rf,df->rd", grad_up_low, up_b, preferred_element_type=f32)
    grad_gain_two = jnp.sum(grad_act_two * norm_two, axis=0)
    grad_one = grad_two + norm_two_pull(grad_act_two * gain_two)[0]
    grad_one_low = low(grad_one)
    grad_out = jnp.einsum("rc,rd->cd", attn_rows, grad_one_low, preferred_element_type=f32)
    grad_attn = low(jnp.einsum("rd,cd->rc", grad_one_low, out_b, preferred_element_type=f32))

    grad_heads = lax.all_to_all(grad_attn, "heads", split_axis=1, concat_axis=0, tiled=True)
    grad_heads = jnp.pad(grad_heads, ((0, 0), (0, cp - cols)))
    dq, dkv, edge_sums = attend_back(key_pos, query, grad_heads, attn_group, lse, bias_rows, kaug, value, kt, hl, hs)
    slot_sums = jnp.sum(edge_sums.reshape(group_blocks, slots, hl, BLOCK), axis=3)
    edge_grad = jnp.einsum("bst,bsh->th", kind_hot, slot_sums, precision=highest)
    columns = lambda a: jnp.broadcast_to(a[:, None], (D, 128))
    dw, denc_t, dgain, dbias = encode_back(
        prev_feat, own_feat, next_feat, dkv, dq, enc_b.T, columns(enc_bias), columns(gain_one), qkv_cols[:, :cp], qkv_cols[:, cp:])

    grad_qkv = jnp.transpose(dw.reshape(D, 3, cp)[:, :, :cols].reshape(D, 3, hl, hs), (0, 2, 1, 3)).reshape(D, 3 * cols)
    grad_gain_one = jnp.sum(dgain, axis=1)
    grad_enc_bias = jnp.sum(dbias, axis=1) + jnp.sum(grad_one, axis=0)
    grad_enc = denc_t.T + jnp.einsum("rf,rd->fd", features, grad_one_low, preferred_element_type=f32)
    edge_full = lax.dynamic_update_slice(jnp.zeros((kinds, HEADS), f32), edge_grad, (jnp.int32(0), head_index * hl))
    grad_vec = jnp.stack([grad_enc_bias, grad_gain_one, grad_gain_two, grad_gain_three, grad_head_vec, edge_full.reshape(D)])

    vec_rows = jnp.transpose(grad_vec.reshape(6, heads_count, -1), (1, 0, 2))

    def reduced(gradient, like):
        piece = lax.psum_scatter(spread_flat(gradient, heads_count, nodes_count), ("nodes", "heads"), scatter_dimension=0, tiled=True)
        return lax.all_gather(piece, "nodes", axis=0, tiled=True).reshape(like.shape)

    qkv_part = lax.all_to_all(grad_qkv, "heads", split_axis=0, concat_axis=1, tiled=True)
    summed = (
        reduced(grad_enc, enc_weight), lax.psum(qkv_part, "nodes"), reduced(grad_out, out_weight), reduced(grad_up, up_weight),
        reduced(grad_down, down_weight), reduced(vec_rows, vec_weight),
    )
    enc_res = adamw(enc_weight, enc_first, enc_second, summed[0])
    qkv_res = adamw(qkv_weight, qkv_first, qkv_second, summed[1])
    out_res = adamw(out_weight, out_first, out_second, summed[2])
    up_res = adamw(up_weight, up_first, up_second, summed[3])
    down_res = adamw(down_weight, down_first, down_second, summed[4])
    vec_res = adamw(vec_weight, vec_first, vec_second, summed[5])
    loss_value = (total_loss / live_total).reshape(1)
    return (
        loss_value, *enc_res, *qkv_res, *out_res, *up_res, *down_res, *vec_res,
        low(enc_res[0]), low(qkv_res[0]), low(out_res[0]), low(up_res[0]), low(down_res[0]),
    )


def solution(mesh):
    rows = P("heads", None)
    both = P(("nodes", "heads"))
    lanes = P(None, "heads")
    in_specs = (P(("nodes", "heads"), None), both, P(), P("nodes", None), P("nodes", None)) + (rows,) * 15 + (lanes,) * 3
    out_specs = (P(),) + (rows,) * 15 + (lanes,) * 3 + (rows,) * 5
    return jax.shard_map(local, mesh=mesh, in_specs=in_specs, out_specs=out_specs, check_vma=False)
```

```python
import functools

import jax
import jax.numpy as jnp
from jax import lax
from jax.experimental import pallas as pl
from jax.experimental.pallas import tpu as pltpu
from jax.sharding import PartitionSpec as P

BLOCK = 128
NT = (((1,), (1,)), ((), ()))
NN = (((1,), (0,)), ((), ()))
f32 = jnp.float32
bf16 = jnp.bfloat16


def dotf(a, b, dims):
    return lax.dot_general(a, b, dims, preferred_element_type=f32)


def head_rows(x, hl, hs, cp):
    if hl == 1:
        return x
    lane = lax.broadcasted_iota(jnp.int32, (BLOCK, cp), 1)
    zero = jnp.zeros_like(x)
    return jnp.concatenate([jnp.where(lane // hs == h, x, zero) for h in range(hl)], axis=0)


def ones_lane(hl, cp, ka):
    rows = hl * BLOCK
    lane = lax.broadcasted_iota(jnp.int32, (rows, ka - cp), 1)
    return jnp.where(lane == 0, 1.0, 0.0).astype(bf16)


def attend_kernel(hl, hs, cp, ka, slots, pos_ref, q_ref, brow_ref, kaug_ref, vt_ref, o_ref, lse_ref, s_ref, p_ref):
    b = pl.program_id(0)
    rows = hl * BLOCK
    q2 = head_rows(q_ref[...], hl, hs, cp)
    qa = jnp.concatenate([q2, ones_lane(hl, cp, ka)], axis=1) if ka > cp else q2
    top = None
    for s in range(slots):
        p = pos_ref[b * slots + s]
        ks = kaug_ref[pl.ds(pl.multiple_of(p * BLOCK, BLOCK), BLOCK), :]
        sc = dotf(ks, qa, NT)
        s_ref[s] = sc
        t = jnp.max(sc, axis=0, keepdims=True) + brow_ref[0, s:s + 1, :]
        top = t if top is None else jnp.maximum(top, t)
    tot = jnp.zeros((1, rows), f32)
    for s in range(slots):
        e = jnp.exp(s_ref[s] - (top - brow_ref[0, s:s + 1, :]))
        s_ref[s] = e
        tot = tot + jnp.sum(e, axis=0, keepdims=True)
    lse_ref[0] = top + jnp.log(tot)
    inv = 1.0 / tot
    vs = []
    for s in range(slots):
        p_ref[s * BLOCK:(s + 1) * BLOCK, :] = (s_ref[s] * inv).astype(bf16)
        vs.append(vt_ref[pos_ref[b * slots + s]])
    ot = dotf(jnp.concatenate(vs, axis=1), p_ref[...], NN)
    parts = [ot[h * hs:(h + 1) * hs, h * BLOCK:(h + 1) * BLOCK] for h in range(hl)]
    if hl * hs < cp:
        parts.append(jnp.zeros((cp - hl * hs, BLOCK), f32))
    o_ref[...] = jnp.concatenate(parts, axis=0).T.astype(bf16)


def attend(pos, q, brow, kaug, vt, hl, hs):
    cp, ka = q.shape[1], kaug.shape[1]
    nb = q.shape[0] // BLOCK
    slots = brow.shape[1]
    rows = hl * BLOCK
    whole = lambda a: pl.BlockSpec(a.shape, lambda i, *_: (0,) * a.ndim, pipeline_mode=pl.Buffered(1))
    return pl.pallas_call(
        functools.partial(attend_kernel, hl, hs, cp, ka, slots),
        grid_spec=pltpu.PrefetchScalarGridSpec(
            num_scalar_prefetch=1, grid=(nb,),
            in_specs=[pl.BlockSpec((BLOCK, cp), lambda i, *_: (i, 0)),
                      pl.BlockSpec((1, slots, rows), lambda i, *_: (i, 0, 0)),
                      whole(kaug), whole(vt)],
            out_specs=[pl.BlockSpec((BLOCK, cp), lambda i, *_: (i, 0)),
                       pl.BlockSpec((1, 1, rows), lambda i, *_: (i, 0, 0))],
            scratch_shapes=[pltpu.VMEM((slots, BLOCK, rows), f32), pltpu.VMEM((slots * BLOCK, rows), bf16)]),
        out_shape=[jax.ShapeDtypeStruct(q.shape, bf16), jax.ShapeDtypeStruct((nb, 1, rows), f32)],
        compiler_params=pltpu.CompilerParams(vmem_limit_bytes=60 << 20),
        cost_estimate=pl.CostEstimate(flops=nb * 10**9, bytes_accessed=3 * 10**7, transcendentals=0),
        name="attend",
    )(pos, q, brow, kaug, vt)


def attend_back_kernel(hl, hs, cp, ka, slots, scale, pos_ref, q_ref, do_ref, o_ref, lse_ref, brow_ref, kaug_ref, v_ref, kt_ref,
                       dq_ref, dkv_ref, edge_ref):
    b = pl.program_id(0)
    rows = hl * BLOCK

    @pl.when(b == 0)
    def _():
        dkv_ref[...] = jnp.zeros_like(dkv_ref)

    q2 = head_rows(q_ref[...], hl, hs, cp)
    qa = jnp.concatenate([q2, ones_lane(hl, cp, ka)], axis=1) if ka > cp else q2
    do = do_ref[...]
    do2 = head_rows(do, hl, hs, cp)
    prod = (do.astype(f32) * o_ref[...].astype(f32)).T
    dd = jnp.concatenate([jnp.sum(prod[h * hs:(h + 1) * hs], axis=0, keepdims=True) for h in range(hl)], axis=1)
    lse = lse_ref[0]
    dqt = jnp.zeros((cp, rows), f32)
    for s in range(slots):
        p = pos_ref[b * slots + s]
        at = pl.ds(pl.multiple_of(p * BLOCK, BLOCK), BLOCK)
        sc = dotf(kaug_ref[at, :], qa, NT)
        pr = jnp.exp(sc - (lse - brow_ref[0, s:s + 1, :]))
        dp = dotf(v_ref[at, :], do2, NT)
        ds = pr * (dp - dd)
        edge_ref[0, s:s + 1, :] = jnp.sum(ds, axis=0, keepdims=True)
        dsl = ds.astype(bf16)
        dv = dotf(pr.astype(bf16), do2, NN)
        dk = dotf(dsl, q2, NN)
        dkv_ref[at, 0:cp] += dk
        dkv_ref[at, cp:2 * cp] += dv
        dqt = dqt + dotf(kt_ref[p], dsl, NN)
    parts = [dqt[h * hs:(h + 1) * hs, h * BLOCK:(h + 1) * BLOCK] for h in range(hl)]
    if hl * hs < cp:
        parts.append(jnp.zeros((cp - hl * hs, BLOCK), f32))
    dq_ref[...] = (jnp.concatenate(parts, axis=0).T * scale).astype(bf16)


def attend_back(pos, q, do, o, lse, brow, kaug, v, kt, hl, hs):
    cp, ka = q.shape[1], kaug.shape[1]
    nb = q.shape[0] // BLOCK
    slots = brow.shape[1]
    rows = hl * BLOCK
    whole = lambda a: pl.BlockSpec(a.shape, lambda i, *_: (0,) * a.ndim, pipeline_mode=pl.Buffered(1))
    tile = pl.BlockSpec((BLOCK, cp), lambda i, *_: (i, 0))
    return pl.pallas_call(
        functools.partial(attend_back_kernel, hl, hs, cp, ka, slots, hs ** -0.5),
        grid_spec=pltpu.PrefetchScalarGridSpec(
            num_scalar_prefetch=1, grid=(nb,),
            in_specs=[tile, tile, tile,
                      pl.BlockSpec((1, 1, rows), lambda i, *_: (i, 0, 0)),
                      pl.BlockSpec((1, slots, rows), lambda i, *_: (i, 0, 0)),
                      whole(kaug), whole(v), whole(kt)],
            out_specs=[tile, pl.BlockSpec((v.shape[0], 2 * cp), lambda i, *_: (0, 0), pipeline_mode=pl.Buffered(1)),
                       pl.BlockSpec((1, slots, rows), lambda i, *_: (i, 0, 0))]),
        out_shape=[jax.ShapeDtypeStruct(q.shape, bf16), jax.ShapeDtypeStruct((v.shape[0], 2 * cp), f32),
                   jax.ShapeDtypeStruct((nb, slots, rows), f32)],
        compiler_params=pltpu.CompilerParams(vmem_limit_bytes=60 << 20),
        cost_estimate=pl.CostEstimate(flops=nb * 2 * 10**9, bytes_accessed=6 * 10**7, transcendentals=0),
        name="attend_back",
    )(pos, q, do, o, lse, brow, kaug, v, kt)
norm_eps = 1e-05


def encode_kernel(cp, ka, cols, scale, per_group, cnt_ref, fp_ref, fo_ref, fn_ref, enc_ref, bias_ref, gain_ref, w_ref,
                  kaug_ref, kt_ref, v_ref, vt_ref, q_ref, x_ref):
    i = pl.program_id(0)
    group = i // per_group
    tile = x_ref.shape[0]
    for g, ref in enumerate((fp_ref, fo_ref, fn_ref)):
        @pl.when(group == g)
        def _(ref=ref):
            x_ref[...] = ref[...]
    resid = dotf(x_ref[...], enc_ref[...], NN) + bias_ref[...]
    centred = resid - jnp.mean(resid, axis=-1, keepdims=True)
    variance = jnp.mean(centred * centred, axis=-1, keepdims=True)
    act = (centred * lax.rsqrt(variance + norm_eps) * gain_ref[...]).astype(bf16)
    kv = dotf(act, w_ref[:, cp:], NN).astype(bf16)
    key, value = kv[:, :cp], kv[:, cp:]
    row = lax.broadcasted_iota(jnp.int32, (BLOCK, 128), 0)
    lane = lax.broadcasted_iota(jnp.int32, (BLOCK, 128), 1)
    first = i * (tile // BLOCK)
    dead = jnp.concatenate(
        [jnp.where((row >= cnt_ref[first + j]) & (lane == cols % 128), -1e30, 0.0) for j in range(tile // BLOCK)], axis=0).astype(bf16)
    if ka > cp:
        kaug_ref[:, :cp] = key
        kaug_ref[:, cp:] = dead
    else:
        kaug_ref[...] = key + dead
    v_ref[...] = value
    for j in range(tile // BLOCK):
        kt_ref[j] = key[j * BLOCK:(j + 1) * BLOCK].T
        vt_ref[j] = value[j * BLOCK:(j + 1) * BLOCK].T

    @pl.when(group == 1)
    def _():
        q = (dotf(act, w_ref[:, :cp], NN) * scale).astype(bf16)
        if ka == cp:
            lanes = lax.broadcasted_iota(jnp.int32, q.shape, 1)
            q = jnp.where(lanes == cols, jnp.ones_like(q), q)
        q_ref[...] = q


def encode(counts, prev, own, nxt, enc, bias, gain, w, cp, ka, cols, scale, tile=512):
    rows, feat = own.shape
    width = enc.shape[1]
    per = rows // tile
    blocks = tile // BLOCK
    whole = lambda a: pl.BlockSpec(a.shape, lambda i, *_: (0,) * a.ndim, pipeline_mode=pl.Buffered(1))
    part = lambda g: pl.BlockSpec((tile, feat), lambda i, *_: (jnp.clip(i - g * per, 0, per - 1), 0))
    return pl.pallas_call(
        functools.partial(encode_kernel, cp, ka, cols, scale, per),
        grid_spec=pltpu.PrefetchScalarGridSpec(
            num_scalar_prefetch=1, grid=(3 * per,),
            in_specs=[part(0), part(1), part(2), whole(enc), whole(bias), whole(gain), whole(w)],
            out_specs=[pl.BlockSpec((tile, ka), lambda i, *_: (i, 0)),
                       pl.BlockSpec((blocks, cp, BLOCK), lambda i, *_: (i, 0, 0)),
                       pl.BlockSpec((tile, cp), lambda i, *_: (i, 0)),
                       pl.BlockSpec((blocks, cp, BLOCK), lambda i, *_: (i, 0, 0)),
                       pl.BlockSpec((tile, cp), lambda i, *_: (jnp.clip(i - per, 0, per - 1), 0))],
            scratch_shapes=[pltpu.VMEM((tile, feat), bf16)]),
        out_shape=[jax.ShapeDtypeStruct((3 * rows, ka), bf16),
                   jax.ShapeDtypeStruct((3 * rows // BLOCK, cp, BLOCK), bf16),
                   jax.ShapeDtypeStruct((3 * rows, cp), bf16),
                   jax.ShapeDtypeStruct((3 * rows // BLOCK, cp, BLOCK), bf16),
                   jax.ShapeDtypeStruct((rows, cp), bf16)],
        compiler_params=pltpu.CompilerParams(vmem_limit_bytes=60 << 20),
        cost_estimate=pl.CostEstimate(flops=rows * 6 * 10**6, bytes_accessed=3 * 10**7, transcendentals=0),
        name="encode",
    )(counts, prev, own, nxt, enc, bias, gain, w)


def encode_back_kernel(cp, per_group, fp_ref, fo_ref, fn_ref, dkv_ref, dq_ref, enct_ref, bias_ref, gain_ref, wq_ref, wkv_ref,
                       dw_ref, denc_ref, dgain_ref, dbias_ref, x_ref, g_ref):
    i = pl.program_id(0)
    group = i // per_group
    tile = x_ref.shape[0]
    width = enct_ref.shape[0]
    reps = tile // 128

    @pl.when(i == 0)
    def _():
        for ref in (dw_ref, denc_ref, dgain_ref, dbias_ref):
            ref[...] = jnp.zeros_like(ref)

    for g, ref in enumerate((fp_ref, fo_ref, fn_ref)):
        @pl.when(group == g)
        def _(ref=ref):
            x_ref[...] = ref[...]
    x = x_ref[...]
    wide = lambda c: jnp.concatenate([c] * reps, axis=1)
    fold = lambda a: functools.reduce(jnp.add, [a[:, r * 128:(r + 1) * 128] for r in range(reps)])
    resid = dotf(enct_ref[...], x, NT) + wide(bias_ref[...])
    centred = resid - jnp.sum(resid, axis=0, keepdims=True) * (1.0 / width)
    variance = jnp.sum(centred * centred, axis=0, keepdims=True) * (1.0 / width)
    inv = lax.rsqrt(variance + norm_eps)
    norm = centred * inv
    gain = wide(gain_ref[...])
    act = (norm * gain).astype(bf16)
    dkv = dkv_ref[...].astype(bf16)
    g_ref[...] = dotf(wkv_ref[...], dkv, NT)
    dw_ref[:, cp:] += dotf(act, dkv, NN)

    @pl.when(group == 1)
    def _():
        dq = dq_ref[...]
        g_ref[...] += dotf(wq_ref[...], dq, NT)
        dw_ref[:, :cp] += dotf(act, dq, NN)

    grad = g_ref[...]
    dgain_ref[...] += fold(grad * norm)
    back = grad * gain
    mean_one = jnp.sum(back, axis=0, keepdims=True) * (1.0 / width)
    mean_two = jnp.sum(back * norm, axis=0, keepdims=True) * (1.0 / width)
    din = inv * (back - mean_one - norm * mean_two)
    dbias_ref[...] += fold(din)
    denc_ref[...] += dotf(din.astype(bf16), x, NN)


def encode_back(prev, own, nxt, dkv, dq, enct, bias, gain, wq, wkv, tile=512):
    rows, feat = own.shape
    width = enct.shape[0]
    cp = dq.shape[1]
    per = rows // tile
    whole = lambda a: pl.BlockSpec(a.shape, lambda i: (0,) * a.ndim, pipeline_mode=pl.Buffered(1))
    part = lambda g: pl.BlockSpec((tile, feat), lambda i: (jnp.clip(i - g * per, 0, per - 1), 0))
    keep = lambda s: pl.BlockSpec(s, lambda i: (0,) * len(s), pipeline_mode=pl.Buffered(1))
    shapes = [(width, 3 * cp), (width, feat), (width, 128), (width, 128)]
    return pl.pallas_call(
        functools.partial(encode_back_kernel, cp, per),
        grid=(3 * per,),
        in_specs=[part(0), part(1), part(2), pl.BlockSpec((tile, 2 * cp), lambda i: (i, 0)),
                  pl.BlockSpec((tile, cp), lambda i: (jnp.clip(i - per, 0, per - 1), 0)),
                  whole(enct), whole(bias), whole(gain), whole(wq), whole(wkv)],
        out_specs=[keep(s) for s in shapes],
        out_shape=[jax.ShapeDtypeStruct(s, f32) for s in shapes],
        scratch_shapes=[pltpu.VMEM((tile, feat), bf16), pltpu.VMEM((width, tile), f32)],
        compiler_params=pltpu.CompilerParams(vmem_limit_bytes=60 << 20),
        cost_estimate=pl.CostEstimate(flops=rows * 10**7, bytes_accessed=4 * 10**7, transcendentals=0),
        name="encode_back",
    )(prev, own, nxt, dkv, dq, enct, bias, gain, wq, wkv)
MESH = pl.DeviceIdType.MESH


def send(src, dst, sems, slot, node, head):
    copy = pltpu.make_async_remote_copy(
        src_ref=src, dst_ref=dst, send_sem=sems[0].at[slot], recv_sem=sems[1].at[slot], device_id=(node, head), device_id_type=MESH)
    copy.start()
    return copy


def greet(nodes, heads, node, head):
    barrier = pltpu.get_barrier_semaphore()
    for s in range(1, nodes):
        pl.semaphore_signal(barrier, inc=1, device_id=(lax.rem(node + s, nodes), head), device_id_type=MESH)
    for s in range(1, heads):
        pl.semaphore_signal(barrier, inc=1, device_id=(node, lax.rem(head + s, heads)), device_id_type=MESH)
    pl.semaphore_wait(barrier, nodes + heads - 2)


def finish_kernel(nodes, heads, *refs):
    (qkv, enc, vec, *bulk), refs = refs[:6], refs[6:]
    (out_q, out_e, out_v, *out_b), refs = refs[:6], refs[6:]
    (q_half, q_one, q_two, q_part, q_sum, q_own, e_half, e_one, e_two, e_sum, e_three, e_own, v_half, v_two, v_three, v_one, v_sum), refs = refs[:17], refs[17:]
    s_one, r_one, s_two, r_two, s_three, r_three, s_four, r_four, s_bulk, r_bulk, s_pass, r_pass, l_sem = refs
    node, head = lax.axis_index("nodes"), lax.axis_index("heads")
    chips = nodes // 2
    chip, side = lax.div(node, 2), lax.rem(node, 2)
    twin = chip * 2 + 1 - side
    greet(nodes, heads, node, head)
    first = [send(ref.at[:, :, 1 - side], dst, (s_one, r_one), i, twin, head) for i, (ref, dst) in enumerate(((qkv, q_half), (enc, e_half)))]
    first.append(send(vec, v_half, (s_one, r_one), 2, twin, head))
    keep = [pltpu.make_async_copy(src, dst.at[node], l_sem.at[i]) for i, (src, dst) in enumerate(zip(bulk, out_b))]
    for copy in keep:
        copy.start()
    spread = []
    for s in range(chips):
        other = lax.rem(chip + s, chips) * 2 + side if s else twin
        spread.append([send(src, dst.at[node], (s_bulk, r_bulk), s * 3 + i, other, head) for i, (src, dst) in enumerate(zip(bulk, out_b))])
    for copy in first:
        copy.wait()
    q_one[...] = qkv[:, :, side] + q_half[...]
    e_one[...] = enc[:, :, side] + e_half[...]
    v_one[...] = vec[...] + v_half[...]
    second = []
    for s in range(1, chips):
        there = lax.rem(chip + s, chips)
        target = there * 2 + side
        i = (s - 1) * 3
        second.append(send(q_one.at[:, there], q_two.at[s - 1], (s_two, r_two), i, target, head))
        second.append(send(e_one.at[:, there], e_two.at[s - 1], (s_two, r_two), i + 1, target, head))
        second.append(send(v_one, v_two.at[s - 1], (s_two, r_two), i + 2, target, head))
    for copy in second:
        copy.wait()
    q_part[...] = functools.reduce(jnp.add, [q_two[s] for s in range(chips - 1)], q_one[:, chip])
    e_sum[...] = functools.reduce(jnp.add, [e_two[s] for s in range(chips - 1)], e_one[:, chip])
    v_sum[...] = functools.reduce(jnp.add, [v_two[s] for s in range(chips - 1)], v_one[...])
    third = []
    for s in range(1, heads):
        there = lax.rem(head + s, heads)
        i = (s - 1) * 3
        third.append(send(q_part.at[there], q_sum.at[head], (s_three, r_three), i, node, there))
        third.append(send(e_sum.at[there], e_three.at[s - 1], (s_three, r_three), i + 1, node, there))
        third.append(send(v_sum, v_three.at[s - 1], (s_three, r_three), i + 2, node, there))
    for copy in third:
        copy.wait()
    q_sum[pl.ds(head, 1)] = q_part[pl.ds(head, 1)]
    e_own[...] = functools.reduce(jnp.add, [e_three[s] for s in range(heads - 1)], e_sum[head])
    out_v[...] = functools.reduce(jnp.add, [v_three[s] for s in range(heads - 1)], v_sum[...])
    fourth = []
    for s in range(1, nodes):
        there = lax.rem(node + s, nodes)
        fourth.append(send(q_sum, out_q.at[node], (s_four, r_four), (s - 1) * 2, there, head))
        fourth.append(send(e_own, out_e.at[node], (s_four, r_four), (s - 1) * 2 + 1, there, head))
    out_q[node] = q_sum[...]
    out_e[node] = e_own[...]
    for copy in keep:
        copy.wait()
    passed = []
    for s in range(chips):
        for copy in spread[s]:
            copy.wait()
        if s:
            origin = lax.rem(chip + chips - s, chips) * 2 + side
            passed += [send(dst.at[origin], dst.at[origin], (s_pass, r_pass), (s - 1) * 3 + i, twin, head) for i, dst in enumerate(out_b)]
    for copy in passed:
        copy.wait()
    for copy in fourth:
        copy.wait()


def finish(qkv, enc, vec, bulk, nodes, heads):
    chips = nodes // 2
    split = lambda a: a.reshape(heads, chips, 2, -1, a.shape[-1])
    qkv, enc = split(qkv), split(enc)
    vm = lambda *s: pltpu.VMEM(s, f32)
    rq, wq, re, we = *qkv.shape[3:], *enc.shape[3:]
    dma = pltpu.SemaphoreType.DMA
    wv = vec.shape
    scratch = [vm(heads, chips, rq, wq), vm(heads, chips, rq, wq), vm(chips - 1, heads, rq, wq), vm(heads, rq, wq), vm(heads, rq, wq), vm(8, 128),
               vm(heads, chips, re, we), vm(heads, chips, re, we), vm(chips - 1, heads, re, we), vm(heads, re, we), vm(heads - 1, re, we), vm(re, we),
               vm(*wv), vm(chips - 1, *wv), vm(heads - 1, *wv), vm(*wv), vm(*wv)]
    counts = (3, 3, 3 * chips - 3, 3 * chips - 3, 3 * heads - 3, 3 * heads - 3, 2 * nodes - 2, 2 * nodes - 2, 3 * chips, 3 * chips, 3 * chips - 3, 3 * chips - 3, 3)
    out_shape = [jax.ShapeDtypeStruct(s, f32) for s in [(nodes, heads, rq, wq), (nodes, re, we), wv] + [(nodes, *b.shape) for b in bulk]]
    spec = pl.BlockSpec(memory_space=pltpu.VMEM)
    return pl.pallas_call(
        functools.partial(finish_kernel, nodes, heads),
        in_specs=[spec] * 6, out_specs=[spec] * 6, out_shape=out_shape,
        scratch_shapes=scratch + [dma((n,)) for n in counts],
        compiler_params=pltpu.CompilerParams(collective_id=1, has_side_effects=True, vmem_limit_bytes=48 << 20),
        name="finish",
    )(qkv, enc, vec, *bulk)
D = 512
HEADS = 8
NBR = 8
ADAM_STEP = 3
highest = lax.Precision.HIGHEST
beta_one = 0.5
beta_two = 0.5
learn_rate = 0.02
weight_decay = 0.1
adam_eps = 1e-08


def normalize(values):
    average = jnp.mean(values, axis=-1, keepdims=True)
    centred = values - average
    variance = jnp.mean(centred * centred, axis=-1, keepdims=True)
    return centred * lax.rsqrt(variance + norm_eps)


def adamw(weight, first_moment, second, gradient):
    first_new = beta_one * first_moment + (1.0 - beta_one) * gradient
    second_new = beta_two * second + (1.0 - beta_two) * gradient * gradient
    first_hat = first_new / (1.0 - beta_one**ADAM_STEP)
    second_hat = second_new / (1.0 - beta_two**ADAM_STEP)
    weight_new = weight - learn_rate * (
        first_hat / (jnp.sqrt(second_hat) + adam_eps) + weight_decay * weight
    )
    return (weight_new, first_new, second_new)


def core_sum(gradient, heads_count, nodes_count):
    node_index = lax.axis_index("nodes")
    parts = gradient.reshape(heads_count, nodes_count // 2, 2, -1, gradient.shape[-1])
    side = node_index % 2
    kept = lax.dynamic_index_in_dim(parts, side, 2, False)
    sent = lax.dynamic_index_in_dim(parts, 1 - side, 2, False)
    return kept + lax.ppermute(sent, "nodes", [(i, i ^ 1) for i in range(nodes_count)])


def chip_sum(parts, nodes_count):
    chips = nodes_count // 2
    chip = lax.axis_index("nodes") // 2
    total = lax.dynamic_index_in_dim(parts, chip, 1, False)
    for step in range(1, chips):
        sent = lax.dynamic_index_in_dim(parts, chip ^ step, 1, False)
        total = total + lax.ppermute(sent, "nodes", [(i, i ^ (2 * step)) for i in range(nodes_count)])
    return total


def plane_sum(parts):
    return jnp.sum(lax.all_to_all(parts, "heads", split_axis=0, concat_axis=0, tiled=True), axis=0)


def from_behind(value, axis, steps):
    count = lax.axis_size(axis)
    pairs = [(source, (source + steps) % count) for source in range(count)]
    return lax.ppermute(value, axis, pairs)


def local(
    features, target, counts, neighbours, edge_kinds,
    enc_weight, enc_first, enc_second, qkv_weight, qkv_first, qkv_second,
    out_weight, out_first, out_second, up_weight, up_first, up_second,
    down_weight, down_first, down_second, vec_weight, vec_first, vec_second,
):
    heads_count = lax.axis_size("heads")
    nodes_count = lax.axis_size("nodes")
    head_index = lax.axis_index("heads")
    node_index = lax.axis_index("nodes")
    row_count = features.shape[0]
    own_blocks = row_count // BLOCK
    group_blocks = own_blocks * heads_count
    group_rows = group_blocks * BLOCK
    hl = HEADS // heads_count
    hs = D // HEADS
    cols = hl * hs
    cp = -(-cols // 128) * 128
    ka = -(-(cols + 1) // 128) * 128
    kinds = D // HEADS
    slots = NBR + 1
    low = lambda a: a.astype(bf16)
    gather = lambda a, axis: lax.all_gather(low(a), "heads", axis=axis, tiled=True)

    own_feat = lax.all_gather(features, "heads", axis=0, tiled=True)
    prev_feat = from_behind(own_feat, "nodes", 1)
    next_feat = from_behind(own_feat, "nodes", -1)
    enc_b = gather(enc_weight, 0)
    vectors = gather(vec_weight, 1).astype(f32)
    qkv_cols = lax.all_to_all(low(qkv_weight), "heads", split_axis=1, concat_axis=0, tiled=True)
    qkv_cols = jnp.transpose(qkv_cols.reshape(D, hl, 3, hs), (0, 2, 1, 3)).reshape(D, 3, cols)
    qkv_cols = jnp.pad(qkv_cols, ((0, 0), (0, 0), (0, cp - cols))).reshape(D, 3 * cp)
    out_b, up_b, down_b = gather(out_weight, 0), gather(up_weight, 0), gather(down_weight, 0)

    enc_bias, gain_one, gain_two, gain_three, head_vec = (vectors[r] for r in range(5))
    edge_local = lax.dynamic_slice_in_dim(vectors[5].reshape(kinds, HEADS), head_index * hl, hl, 1)
    own_counts = lax.dynamic_slice_in_dim(counts, (node_index * heads_count + head_index) * own_blocks, own_blocks)
    row_live = (jnp.arange(BLOCK, dtype=jnp.int32)[None, :] < own_counts[:, None]).reshape(row_count).astype(f32)
    live_total = jnp.sum(counts).astype(f32)

    def group_counts(offset):
        return lax.dynamic_slice_in_dim(counts, (node_index + offset) % nodes_count * group_blocks, group_blocks)

    pool_counts = jnp.concatenate([group_counts(nodes_count - 1), group_counts(0), group_counts(1)])
    relative = (neighbours // group_blocks - node_index + 1) % nodes_count
    nbr_pos = relative * group_blocks + neighbours % group_blocks
    self_pos = group_blocks + jnp.arange(group_blocks, dtype=jnp.int32)
    key_pos = jnp.concatenate([self_pos[:, None], nbr_pos], axis=1).reshape(-1)
    kind_hot = jax.nn.one_hot(edge_kinds, kinds, dtype=f32)
    slot_bias = jnp.einsum("bst,th->bsh", kind_hot, edge_local, precision=highest)
    bias_rows = jnp.repeat(slot_bias, BLOCK, axis=2)

    kaug, kt, value, vt, query = encode(
        pool_counts, prev_feat, own_feat, next_feat, enc_b, enc_bias[None], gain_one[None], qkv_cols, cp, ka, cols, hs**-0.5)
    attn_group, lse = attend(key_pos, query, bias_rows, kaug, vt, hl, hs)
    attn_rows = lax.all_to_all(attn_group[:, :cols], "heads", split_axis=0, concat_axis=1, tiled=True)

    resid_in = jnp.dot(features, enc_b, preferred_element_type=f32) + enc_bias
    hidden_one = resid_in + jnp.dot(attn_rows, out_b, preferred_element_type=f32)
    norm_two, norm_two_pull = jax.vjp(normalize, hidden_one)
    act_two = low(norm_two * gain_two)
    up_val = jnp.dot(act_two, up_b, preferred_element_type=f32)
    gelu_val, gelu_pull = jax.vjp(jax.nn.gelu, up_val)
    act_up = low(gelu_val)
    hidden_two = hidden_one + jnp.dot(act_up, down_b, preferred_element_type=f32)
    norm_three, norm_three_pull = jax.vjp(normalize, hidden_two)
    scaled = norm_three * gain_three
    predicted = jnp.sum(scaled * head_vec, axis=-1)
    pred_error = predicted - target
    local_loss = jnp.sum(row_live * pred_error * pred_error)
    grad_pred = 2.0 * row_live * pred_error / live_total
    grad_scaled = grad_pred[:, None] * head_vec
    grad_head_vec = jnp.sum(grad_pred[:, None] * scaled, axis=0)
    grad_gain_three = jnp.sum(grad_scaled * norm_three, axis=0)
    grad_two = norm_three_pull(grad_scaled * gain_three)[0]
    grad_two_low = low(grad_two)
    grad_down = jnp.einsum("rf,rd->fd", act_up, grad_two_low, preferred_element_type=f32)
    grad_act = jnp.einsum("rd,fd->rf", grad_two_low, down_b, preferred_element_type=f32)
    grad_up_low = low(gelu_pull(grad_act)[0])
    grad_up = jnp.einsum("rd,rf->df", act_two, grad_up_low, preferred_element_type=f32)
    grad_act_two = jnp.einsum("rf,df->rd", grad_up_low, up_b, preferred_element_type=f32)
    grad_gain_two = jnp.sum(grad_act_two * norm_two, axis=0)
    grad_one = grad_two + norm_two_pull(grad_act_two * gain_two)[0]
    grad_one_low = low(grad_one)
    grad_out = jnp.einsum("rc,rd->cd", attn_rows, grad_one_low, preferred_element_type=f32)
    grad_attn = low(jnp.einsum("rd,cd->rc", grad_one_low, out_b, preferred_element_type=f32))

    grad_heads = lax.all_to_all(grad_attn, "heads", split_axis=1, concat_axis=0, tiled=True)
    grad_heads = jnp.pad(grad_heads, ((0, 0), (0, cp - cols)))
    dq, dkv, edge_sums = attend_back(key_pos, query, grad_heads, attn_group, lse, bias_rows, kaug, value, kt, hl, hs)
    slot_sums = jnp.sum(edge_sums.reshape(group_blocks, slots, hl, BLOCK), axis=3)
    edge_grad = jnp.einsum("bst,bsh->th", kind_hot, slot_sums, precision=highest)
    columns = lambda a: jnp.broadcast_to(a[:, None], (D, 128))
    dw, denc_t, dgain, dbias = encode_back(
        prev_feat, own_feat, next_feat, dkv, dq, enc_b.T, columns(enc_bias), columns(gain_one), qkv_cols[:, :cp], qkv_cols[:, cp:])

    grad_gain_one = jnp.sum(dgain, axis=1)
    grad_enc_bias = jnp.sum(dbias, axis=1) + jnp.sum(grad_one, axis=0)
    grad_enc = denc_t.T + jnp.einsum("rf,rd->fd", features, grad_one_low, preferred_element_type=f32)
    edge_full = lax.dynamic_update_slice(jnp.zeros((kinds, HEADS), f32), edge_grad, (jnp.int32(0), head_index * hl))
    grad_vec = jnp.stack([grad_enc_bias, grad_gain_one, grad_gain_two, grad_gain_three, grad_head_vec, edge_full.reshape(D),
                          jnp.full((D,), local_loss)])
    def reduced(gradient):
        return plane_sum(chip_sum(core_sum(gradient, heads_count, nodes_count), nodes_count))

    dw_sum, enc_sum, vec_total, *bulk = finish(
        dw, grad_enc, jnp.pad(grad_vec, ((0, 1), (0, 0))), [reduced(grad_out), reduced(grad_up), reduced(grad_down)], nodes_count, heads_count)
    total_loss = vec_total[6, 0]
    vec_sum = lax.dynamic_slice_in_dim(vec_total[:6], head_index * (D // heads_count), D // heads_count, 1)
    qkv_sum = jnp.transpose(dw_sum, (0, 2, 1, 3)).reshape(-1, heads_count, 3, cp)[..., :cols].reshape(-1, heads_count, 3, hl, hs)
    qkv_sum = jnp.transpose(qkv_sum, (0, 1, 3, 2, 4)).reshape(qkv_weight.shape)
    flat = lambda a: a.reshape(-1, a.shape[-1])
    summed = (flat(enc_sum), qkv_sum, flat(bulk[0]), flat(bulk[1]), flat(bulk[2]), vec_sum)
    enc_res = adamw(enc_weight, enc_first, enc_second, summed[0])
    qkv_res = adamw(qkv_weight, qkv_first, qkv_second, summed[1])
    out_res = adamw(out_weight, out_first, out_second, summed[2])
    up_res = adamw(up_weight, up_first, up_second, summed[3])
    down_res = adamw(down_weight, down_first, down_second, summed[4])
    vec_res = adamw(vec_weight, vec_first, vec_second, summed[5])
    loss_value = (total_loss / live_total).reshape(1)
    return (
        loss_value, *enc_res, *qkv_res, *out_res, *up_res, *down_res, *vec_res,
        low(enc_res[0]), low(qkv_res[0]), low(out_res[0]), low(up_res[0]), low(down_res[0]),
    )


def solution(mesh):
    rows = P("heads", None)
    both = P(("nodes", "heads"))
    lanes = P(None, "heads")
    in_specs = (P(("nodes", "heads"), None), both, P(), P("nodes", None), P("nodes", None)) + (rows,) * 15 + (lanes,) * 3
    out_specs = (P(),) + (rows,) * 15 + (lanes,) * 3 + (rows,) * 5
    return jax.shard_map(local, mesh=mesh, in_specs=in_specs, out_specs=out_specs, check_vma=False)
```

```python
import functools

import jax
import jax.numpy as jnp
from jax import lax
from jax.experimental import pallas as pl
from jax.experimental.pallas import tpu as pltpu
from jax.sharding import PartitionSpec as P

BLOCK = 128
NT = (((1,), (1,)), ((), ()))
NN = (((1,), (0,)), ((), ()))
f32 = jnp.float32
bf16 = jnp.bfloat16


def dotf(a, b, dims):
    return lax.dot_general(a, b, dims, preferred_element_type=f32)


def head_rows(x, hl, hs, cp):
    if hl == 1:
        return x
    lane = lax.broadcasted_iota(jnp.int32, (BLOCK, cp), 1)
    zero = jnp.zeros_like(x)
    return jnp.concatenate([jnp.where(lane // hs == h, x, zero) for h in range(hl)], axis=0)


def ones_lane(hl, cp, ka):
    rows = hl * BLOCK
    lane = lax.broadcasted_iota(jnp.int32, (rows, ka - cp), 1)
    return jnp.where(lane == 0, 1.0, 0.0).astype(bf16)


def attend_kernel(hl, hs, cp, ka, slots, block_of, pos_ref, q_ref, brow_ref, kaug_ref, vt_ref, o_ref, lse_ref, s_ref, p_ref):
    b = block_of(pl.program_id(0))
    rows = hl * BLOCK
    q2 = head_rows(q_ref[...], hl, hs, cp)
    qa = jnp.concatenate([q2, ones_lane(hl, cp, ka)], axis=1) if ka > cp else q2
    top = None
    spots = [pl.ds(pl.multiple_of(pos_ref[b * slots + s] * BLOCK, BLOCK), BLOCK) for s in range(slots)]
    scores = dotf(jnp.concatenate([kaug_ref[at, :] for at in spots], axis=0), qa, NT)
    for s in range(slots):
        sc = scores[s * BLOCK:(s + 1) * BLOCK]
        s_ref[s] = sc
        t = jnp.max(sc, axis=0, keepdims=True) + brow_ref[0, s:s + 1, :]
        top = t if top is None else jnp.maximum(top, t)
    tot = jnp.zeros((1, rows), f32)
    for s in range(slots):
        e = jnp.exp(s_ref[s] - (top - brow_ref[0, s:s + 1, :]))
        s_ref[s] = e
        tot = tot + jnp.sum(e, axis=0, keepdims=True)
    lse_ref[0] = top + jnp.log(tot)
    inv = 1.0 / tot
    vs = []
    for s in range(slots):
        p_ref[s * BLOCK:(s + 1) * BLOCK, :] = (s_ref[s] * inv).astype(bf16)
        vs.append(vt_ref[pos_ref[b * slots + s]])
    ot = dotf(jnp.concatenate(vs, axis=1), p_ref[...], NN)
    parts = [ot[h * hs:(h + 1) * hs, h * BLOCK:(h + 1) * BLOCK] for h in range(hl)]
    if hl * hs < cp:
        parts.append(jnp.zeros((cp - hl * hs, BLOCK), f32))
    o_ref[...] = jnp.concatenate(parts, axis=0).T.astype(bf16)


def attend(part, own, pos, q, brow, kaug, vt, hl, hs):
    cp, ka = q.shape[1], kaug.shape[1]
    nb = q.shape[0] // BLOCK // 2
    half = own // 2
    block_of = lambda i: lax.div(i, half) * own + part * half + lax.rem(i, half)
    slots = brow.shape[1]
    rows = hl * BLOCK
    whole = lambda a: pl.BlockSpec(a.shape, lambda i, *_: (0,) * a.ndim, pipeline_mode=pl.Buffered(1))
    return pl.pallas_call(
        functools.partial(attend_kernel, hl, hs, cp, ka, slots, block_of),
        grid_spec=pltpu.PrefetchScalarGridSpec(
            num_scalar_prefetch=1, grid=(nb,),
            in_specs=[pl.BlockSpec((BLOCK, cp), lambda i, *_: (block_of(i), 0)),
                      pl.BlockSpec((1, slots, rows), lambda i, *_: (block_of(i), 0, 0)),
                      whole(kaug), whole(vt)],
            out_specs=[pl.BlockSpec((BLOCK, cp), lambda i, *_: (i, 0)),
                       pl.BlockSpec((1, 1, rows), lambda i, *_: (i, 0, 0))],
            scratch_shapes=[pltpu.VMEM((slots, BLOCK, rows), f32), pltpu.VMEM((slots * BLOCK, rows), bf16)]),
        out_shape=[jax.ShapeDtypeStruct((nb * BLOCK, cp), bf16), jax.ShapeDtypeStruct((nb, 1, rows), f32)],
        cost_estimate=pl.CostEstimate(flops=nb * 10**9, bytes_accessed=3 * 10**7, transcendentals=0),
        compiler_params=pltpu.CompilerParams(vmem_limit_bytes=60 << 20),
        name="attend",
    )(pos, q, brow, kaug, vt)


def attend_back_kernel(hl, hs, cp, ka, slots, scale, block_of, pos_ref, q_ref, do_ref, oa_ref, ob_ref, la_ref, lb_ref, brow_ref, kaug_ref, v_ref, kt_ref,
                       dq_ref, dkv_ref, edge_ref, p_ref, d_ref):
    i = pl.program_id(0)
    b = block_of(i)
    late = i >= pl.num_programs(0) // 2
    rows = hl * BLOCK

    @pl.when(i == 0)
    def _():
        dkv_ref[...] = jnp.zeros_like(dkv_ref)

    q2 = head_rows(q_ref[...], hl, hs, cp)
    qa = jnp.concatenate([q2, ones_lane(hl, cp, ka)], axis=1) if ka > cp else q2
    do = do_ref[...]
    do2 = head_rows(do, hl, hs, cp)
    prod = (do.astype(f32) * jnp.where(late, ob_ref[...], oa_ref[...]).astype(f32)).T
    dd = jnp.concatenate([jnp.sum(prod[h * hs:(h + 1) * hs], axis=0, keepdims=True) for h in range(hl)], axis=1)
    lse = jnp.where(late, lb_ref[0], la_ref[0])
    spots = [pl.ds(pl.multiple_of(pos_ref[b * slots + s] * BLOCK, BLOCK), BLOCK) for s in range(slots)]
    scores = dotf(jnp.concatenate([kaug_ref[at, :] for at in spots], axis=0), qa, NT)
    grads = dotf(jnp.concatenate([v_ref[at, :] for at in spots], axis=0), do2, NT)
    for s in range(slots):
        here = slice(s * BLOCK, (s + 1) * BLOCK)
        pr = jnp.exp(scores[here] - (lse - brow_ref[0, s:s + 1, :]))
        ds = pr * (grads[here] - dd)
        edge_ref[0, s:s + 1, :] = jnp.sum(ds, axis=0, keepdims=True)
        p_ref[here, :] = pr.astype(bf16)
        d_ref[here, :] = ds.astype(bf16)
    dv = dotf(p_ref[...], do2, NN)
    dk = dotf(d_ref[...], q2, NN)
    dqt = dotf(jnp.concatenate([kt_ref[pos_ref[b * slots + s]] for s in range(slots)], axis=1), d_ref[...], NN)
    for s, at in enumerate(spots):
        here = slice(s * BLOCK, (s + 1) * BLOCK)
        dkv_ref[at, 0:cp] += dk[here]
        dkv_ref[at, cp:2 * cp] += dv[here]
    parts = [dqt[h * hs:(h + 1) * hs, h * BLOCK:(h + 1) * BLOCK] for h in range(hl)]
    if hl * hs < cp:
        parts.append(jnp.zeros((cp - hl * hs, BLOCK), f32))
    dq_ref[...] = (jnp.concatenate(parts, axis=0).T * scale).astype(bf16)


def attend_back(own, pos, q, do, outs, lses, brow, kaug, v, kt, hl, hs):
    cp, ka = q.shape[1], kaug.shape[1]
    nb = q.shape[0] // BLOCK
    slots = brow.shape[1]
    rows = hl * BLOCK
    half, mid = own // 2, nb // 2
    block_of = lambda i: lax.div(lax.rem(i, mid), half) * own + lax.div(i, mid) * half + lax.rem(i, half)
    whole = lambda a: pl.BlockSpec(a.shape, lambda i, *_: (0,) * a.ndim, pipeline_mode=pl.Buffered(1))
    tile = pl.BlockSpec((BLOCK, cp), lambda i, *_: (block_of(i), 0))
    early = lambda i: jnp.minimum(i, mid - 1)
    late = lambda i: jnp.maximum(i - mid, 0)
    return pl.pallas_call(
        functools.partial(attend_back_kernel, hl, hs, cp, ka, slots, hs ** -0.5, block_of),
        grid_spec=pltpu.PrefetchScalarGridSpec(
            num_scalar_prefetch=1, grid=(nb,),
            in_specs=[tile, tile,
                      pl.BlockSpec((BLOCK, cp), lambda i, *_: (early(i), 0)), pl.BlockSpec((BLOCK, cp), lambda i, *_: (late(i), 0)),
                      pl.BlockSpec((1, 1, rows), lambda i, *_: (early(i), 0, 0)), pl.BlockSpec((1, 1, rows), lambda i, *_: (late(i), 0, 0)),
                      pl.BlockSpec((1, slots, rows), lambda i, *_: (block_of(i), 0, 0)),
                      whole(kaug), whole(v), whole(kt)],
            out_specs=[tile, pl.BlockSpec((v.shape[0], 2 * cp), lambda i, *_: (0, 0), pipeline_mode=pl.Buffered(1)),
                       pl.BlockSpec((1, slots, rows), lambda i, *_: (block_of(i), 0, 0))],
            scratch_shapes=[pltpu.VMEM((slots * BLOCK, rows), bf16)] * 2),
        out_shape=[jax.ShapeDtypeStruct(q.shape, bf16), jax.ShapeDtypeStruct((v.shape[0], 2 * cp), f32),
                   jax.ShapeDtypeStruct((nb, slots, rows), f32)],
        cost_estimate=pl.CostEstimate(flops=nb * 2 * 10**9, bytes_accessed=6 * 10**7, transcendentals=0),
        compiler_params=pltpu.CompilerParams(vmem_limit_bytes=60 << 20),
        name="attend_back",
    )(pos, q, do, *outs, *lses, brow, kaug, v, kt)
norm_eps = 1e-05


def encode_kernel(cp, ka, cols, scale, per_group, cnt_ref, x_ref, enc_ref, bias_ref, gain_ref, w_ref,
                  kaug_ref, kt_ref, v_ref, vt_ref, q_ref):
    i = pl.program_id(0)
    group = i // per_group
    tile = x_ref.shape[0]
    resid = dotf(x_ref[...], enc_ref[...], NN) + bias_ref[...]
    centred = resid - jnp.mean(resid, axis=-1, keepdims=True)
    variance = jnp.mean(centred * centred, axis=-1, keepdims=True)
    act = (centred * lax.rsqrt(variance + norm_eps) * gain_ref[...]).astype(bf16)
    kv = dotf(act, w_ref[:, cp:], NN).astype(bf16)
    key, value = kv[:, :cp], kv[:, cp:]
    row = lax.broadcasted_iota(jnp.int32, (BLOCK, 128), 0)
    lane = lax.broadcasted_iota(jnp.int32, (BLOCK, 128), 1)
    first = i * (tile // BLOCK)
    dead = jnp.concatenate(
        [jnp.where((row >= cnt_ref[first + j]) & (lane == cols % 128), -1e30, 0.0) for j in range(tile // BLOCK)], axis=0).astype(bf16)
    if ka > cp:
        kaug_ref[:, :cp] = key
        kaug_ref[:, cp:] = dead
    else:
        kaug_ref[...] = key + dead
    v_ref[...] = value
    for j in range(tile // BLOCK):
        kt_ref[j] = key[j * BLOCK:(j + 1) * BLOCK].T
        vt_ref[j] = value[j * BLOCK:(j + 1) * BLOCK].T

    @pl.when(group == 1)
    def _():
        q = (dotf(act, w_ref[:, :cp], NN) * scale).astype(bf16)
        if ka == cp:
            lanes = lax.broadcasted_iota(jnp.int32, q.shape, 1)
            q = jnp.where(lanes == cols, jnp.ones_like(q), q)
        q_ref[...] = q


def encode(counts, feats, enc, bias, gain, w, cp, ka, cols, scale, tile=512):
    rows, feat = feats.shape[0] // 3, feats.shape[1]
    width = enc.shape[1]
    per = rows // tile
    blocks = tile // BLOCK
    whole = lambda a: pl.BlockSpec(a.shape, lambda i, *_: (0,) * a.ndim, pipeline_mode=pl.Buffered(1))
    return pl.pallas_call(
        functools.partial(encode_kernel, cp, ka, cols, scale, per),
        grid_spec=pltpu.PrefetchScalarGridSpec(
            num_scalar_prefetch=1, grid=(3 * per,),
            in_specs=[pl.BlockSpec((tile, feat), lambda i, *_: (i, 0)), whole(enc), whole(bias), whole(gain), whole(w)],
            out_specs=[pl.BlockSpec((tile, ka), lambda i, *_: (i, 0)),
                       pl.BlockSpec((blocks, cp, BLOCK), lambda i, *_: (i, 0, 0)),
                       pl.BlockSpec((tile, cp), lambda i, *_: (i, 0)),
                       pl.BlockSpec((blocks, cp, BLOCK), lambda i, *_: (i, 0, 0)),
                       pl.BlockSpec((tile, cp), lambda i, *_: (jnp.clip(i - per, 0, per - 1), 0))]),
        out_shape=[jax.ShapeDtypeStruct((3 * rows, ka), bf16),
                   jax.ShapeDtypeStruct((3 * rows // BLOCK, cp, BLOCK), bf16),
                   jax.ShapeDtypeStruct((3 * rows, cp), bf16),
                   jax.ShapeDtypeStruct((3 * rows // BLOCK, cp, BLOCK), bf16),
                   jax.ShapeDtypeStruct((rows, cp), bf16)],
        compiler_params=pltpu.CompilerParams(vmem_limit_bytes=60 << 20),
        cost_estimate=pl.CostEstimate(flops=rows * 6 * 10**6, bytes_accessed=3 * 10**7, transcendentals=0),
        name="encode",
    )(counts, feats, enc, bias, gain, w)


def encode_back_kernel(cp, per_group, x_ref, dkv_ref, dq_ref, enct_ref, bias_ref, gain_ref, wq_ref, wkv_ref,
                       dw_ref, denc_ref, dgain_ref, dbias_ref, g_ref):
    i = pl.program_id(0)
    group = i // per_group
    tile = x_ref.shape[0]
    width = enct_ref.shape[0]
    reps = tile // 128

    @pl.when(i == 0)
    def _():
        for ref in (dw_ref, denc_ref, dgain_ref, dbias_ref):
            ref[...] = jnp.zeros_like(ref)

    x = x_ref[...]
    wide = lambda c: jnp.concatenate([c] * reps, axis=1)
    fold = lambda a: functools.reduce(jnp.add, [a[:, r * 128:(r + 1) * 128] for r in range(reps)])
    resid = dotf(enct_ref[...], x, NT) + wide(bias_ref[...])
    centred = resid - jnp.sum(resid, axis=0, keepdims=True) * (1.0 / width)
    variance = jnp.sum(centred * centred, axis=0, keepdims=True) * (1.0 / width)
    inv = lax.rsqrt(variance + norm_eps)
    norm = centred * inv
    gain = wide(gain_ref[...])
    act = (norm * gain).astype(bf16)
    dkv = dkv_ref[...].astype(bf16)
    g_ref[...] = dotf(wkv_ref[...], dkv, NT)
    dw_ref[:, cp:] += dotf(act, dkv, NN)

    @pl.when(group == 1)
    def _():
        dq = dq_ref[...]
        g_ref[...] += dotf(wq_ref[...], dq, NT)
        dw_ref[:, :cp] += dotf(act, dq, NN)

    grad = g_ref[...]
    dgain_ref[...] += fold(grad * norm)
    back = grad * gain
    mean_one = jnp.sum(back, axis=0, keepdims=True) * (1.0 / width)
    mean_two = jnp.sum(back * norm, axis=0, keepdims=True) * (1.0 / width)
    din = inv * (back - mean_one - norm * mean_two)
    dbias_ref[...] += fold(din)
    denc_ref[...] += dotf(din.astype(bf16), x, NN)


def encode_back(feats, dkv, dq, enct, bias, gain, wq, wkv, tile=512):
    rows, feat = feats.shape[0] // 3, feats.shape[1]
    width = enct.shape[0]
    cp = dq.shape[1]
    per = rows // tile
    whole = lambda a: pl.BlockSpec(a.shape, lambda i: (0,) * a.ndim, pipeline_mode=pl.Buffered(1))
    keep = lambda s: pl.BlockSpec(s, lambda i: (0,) * len(s), pipeline_mode=pl.Buffered(1))
    shapes = [(width, 3 * cp), (width, feat), (width, 128), (width, 128)]
    return pl.pallas_call(
        functools.partial(encode_back_kernel, cp, per),
        grid=(3 * per,),
        in_specs=[pl.BlockSpec((tile, feat), lambda i: (i, 0)), pl.BlockSpec((tile, 2 * cp), lambda i: (i, 0)),
                  pl.BlockSpec((tile, cp), lambda i: (jnp.clip(i - per, 0, per - 1), 0)),
                  whole(enct), whole(bias), whole(gain), whole(wq), whole(wkv)],
        out_specs=[keep(s) for s in shapes],
        out_shape=[jax.ShapeDtypeStruct(s, f32) for s in shapes],
        scratch_shapes=[pltpu.VMEM((width, tile), f32)],
        compiler_params=pltpu.CompilerParams(vmem_limit_bytes=60 << 20),
        cost_estimate=pl.CostEstimate(flops=rows * 10**7, bytes_accessed=4 * 10**7, transcendentals=0),
        name="encode_back",
    )(feats, dkv, dq, enct, bias, gain, wq, wkv)


def row_norm(values):
    centred = values - jnp.mean(values, axis=-1, keepdims=True)
    inv = lax.rsqrt(jnp.mean(centred * centred, axis=-1, keepdims=True) + norm_eps)
    return centred * inv, inv


def norm_back(grad, norm, inv):
    return inv * (grad - jnp.mean(grad, axis=-1, keepdims=True) - norm * jnp.mean(grad * norm, axis=-1, keepdims=True))


def dense_kernel(first, chunk, total_ref, attn_ref, feat_ref, side_ref, vec_ref, enc_ref, out_ref, up_ref, down_ref, *refs):
    if not first:
        olds, refs = refs[:5], refs[5:]
    gattn_ref, ddown_ref, dup_ref, dout_ref, denc_ref, dvec_ref, u_ref, g_ref = refs
    i = pl.program_id(0)

    @pl.when(i == 0)
    def _():
        for n, ref in enumerate((ddown_ref, dup_ref, dout_ref, denc_ref, dvec_ref)):
            ref[...] = jnp.zeros_like(ref) if first else olds[n][...]

    heads = attn_ref.shape[0]
    ff = up_ref.shape[1]
    bias, gain_two, gain_three, head_vec = (vec_ref[r:r + 1, :] for r in range(4))
    target, live = side_ref[:, 0:1], side_ref[:, 1:2]
    attn = jnp.concatenate([attn_ref[h] for h in range(heads)], axis=1)
    feat = feat_ref[...]
    hidden_one = dotf(feat, enc_ref[...], NN) + bias + dotf(attn, out_ref[...], NN)
    norm_two, inv_two = row_norm(hidden_one)
    act_two = (norm_two * gain_two).astype(bf16)
    root = 0.7978845608028654
    acts = []
    for c in range(0, ff, chunk):
        u = dotf(act_two, up_ref[:, c:c + chunk], NN)
        square = u * u
        half = 0.5 * (1.0 + jnp.tanh(root * (u + 0.044715 * (u * square))))
        act = (u * half).astype(bf16)
        u_ref[:, c:c + chunk] = half + 2.0 * u * half * (1.0 - half) * (root * (1.0 + 0.134145 * square))
        g_ref[:, c:c + chunk] = act
    hidden_two = hidden_one + dotf(g_ref[...], down_ref[...], NN)
    norm_three, inv_three = row_norm(hidden_two)
    scaled = norm_three * gain_three
    error = jnp.sum(scaled * head_vec, axis=-1, keepdims=True) - target
    weighed = live * error
    grad_pred = 2.0 * weighed / total_ref[0]
    grad_two = norm_back(grad_pred * (head_vec * gain_three), norm_three, inv_three)
    low_two = grad_two.astype(bf16)
    act_two_t = act_two.T
    for c in range(0, ff, chunk):
        ddown_ref[c:c + chunk, :] += dotf(g_ref[:, c:c + chunk].T, low_two, NN)
        grad_up = (u_ref[:, c:c + chunk] * dotf(low_two, down_ref[c:c + chunk, :], NT)).astype(bf16)
        dup_ref[:, c:c + chunk] += dotf(act_two_t, grad_up, NN)
        g_ref[:, c:c + chunk] = grad_up
    grad_act_two = dotf(g_ref[...], up_ref[...], NT)
    grad_one = grad_two + norm_back(grad_act_two * gain_two, norm_two, inv_two)
    low_one = grad_one.astype(bf16)
    dout_ref[...] += dotf(attn.T, low_one, NN)
    denc_ref[...] += dotf(feat.T, low_one, NN)
    gattn = dotf(low_one, out_ref[...], NT).astype(bf16)
    width = gattn.shape[1] // heads
    for h in range(heads):
        gattn_ref[h] = gattn[:, h * width:(h + 1) * width]
    down = lambda a: jnp.sum(a, axis=0, keepdims=True)
    loss = jnp.broadcast_to(jnp.sum(weighed * error, axis=0, keepdims=True), (1, bias.shape[1]))
    dvec_ref[...] += jnp.concatenate(
        [down(grad_one), down(grad_act_two * norm_two), down(grad_pred * head_vec * norm_three), down(grad_pred * scaled), loss,
         jnp.zeros((3, bias.shape[1]), f32)], axis=0)


def dense(part, total, attn, feat, side, vec, enc, out_w, up_w, down_w, olds=None, tile=256, chunk=512):
    heads, rows, cols = attn.shape
    width, ff = up_w.shape
    per = rows // tile
    first = olds is None
    whole = lambda a: pl.BlockSpec(a.shape, lambda i: (0,) * a.ndim, pipeline_mode=pl.Buffered(1))
    keep = lambda s: pl.BlockSpec(s, lambda i: (0,) * len(s), pipeline_mode=pl.Buffered(1))
    shapes = [(ff, width), (width, ff), (width, width), (feat.shape[1], width), (8, width)]
    olds = () if first else tuple(olds)
    return pl.pallas_call(
        functools.partial(dense_kernel, first, chunk),
        grid=(per,),
        in_specs=[pl.BlockSpec(memory_space=pltpu.SMEM),
                  pl.BlockSpec((heads, tile, cols), lambda i: (0, i, 0)),
                  pl.BlockSpec((tile, feat.shape[1]), lambda i: (part * per + i, 0)),
                  pl.BlockSpec((tile, side.shape[1]), lambda i: (part * per + i, 0)),
                  whole(vec), whole(enc), whole(out_w), whole(up_w), whole(down_w)] + [whole(o) for o in olds],
        out_specs=[pl.BlockSpec((heads, tile, cols), lambda i: (0, i, 0))] + [keep(s) for s in shapes],
        out_shape=[jax.ShapeDtypeStruct((heads, rows, cols), bf16)] + [jax.ShapeDtypeStruct(s, f32) for s in shapes],
        scratch_shapes=[pltpu.VMEM((tile, ff), f32), pltpu.VMEM((tile, ff), bf16)],
        compiler_params=pltpu.CompilerParams(vmem_limit_bytes=60 << 20),
        cost_estimate=pl.CostEstimate(flops=rows * 5 * 10**7, bytes_accessed=3 * 10**7, transcendentals=0),
        name="dense",
    )(total, attn, feat, side, vec, enc, out_w, up_w, down_w, *olds)
MESH = pl.DeviceIdType.MESH


def front_kernel(nodes, heads, feat, enc, qkv, vec, out_f, out_e, out_q, out_v, up_s, up_r, down_s, down_r, halo_s, halo_r, w_s, w_r, l_sem):
    node, head = lax.axis_index("nodes"), lax.axis_index("heads")
    after, before = lax.rem(node + 1, nodes), lax.rem(node + nodes - 1, nodes)
    barrier = pltpu.get_barrier_semaphore()
    for other in (after, before):
        pl.semaphore_signal(barrier, inc=1, device_id=(other, head), device_id_type=MESH)
    for s in range(1, heads):
        pl.semaphore_signal(barrier, inc=1, device_id=(node, lax.rem(head + s, heads)), device_id_type=MESH)
    pl.semaphore_wait(barrier, heads + 1)

    own = [pltpu.make_async_copy(feat, out_f.at[1, head], l_sem.at[0]),
           pltpu.make_async_copy(enc, out_e.at[head], l_sem.at[1]),
           pltpu.make_async_copy(qkv.at[head], out_q.at[head], l_sem.at[2]),
           pltpu.make_async_copy(vec, out_v.at[head], l_sem.at[3])]

    def relay(step, upward):
        shard = head - step if upward else head + step
        shard = jnp.clip(shard, 0, heads - 1)
        target = jnp.clip(head + 1 if upward else head - 1, 0, heads - 1)
        sems = (up_s, up_r) if upward else (down_s, down_r)
        src = feat if step == 0 else out_f.at[1, shard]
        return pltpu.make_async_remote_copy(
            src_ref=src, dst_ref=out_f.at[1, shard], send_sem=sems[0].at[step], recv_sem=sems[1].at[step],
            device_id=(node, target), device_id_type=MESH)

    def halo(shard, src, way):
        return pltpu.make_async_remote_copy(
            src_ref=src, dst_ref=out_f.at[0 if way == 0 else 2, shard], send_sem=halo_s.at[way, shard], recv_sem=halo_r.at[way, shard],
            device_id=(after if way == 0 else before, head), device_id_type=MESH)

    def sends(step, upward):
        return (head - step >= 0) & (head + 1 <= heads - 1) if upward else (head + step <= heads - 1) & (head - 1 >= 0)

    def gets(step, upward):
        return head - 1 - step >= 0 if upward else head + 1 + step <= heads - 1

    for step in range(heads - 1):
        for upward in (True, False):
            @pl.when(sends(step, upward))
            def _(step=step, upward=upward):
                relay(step, upward).start()
        if step == 0:
            for way in range(2):
                halo(head, feat, way).start()
            for copy in own:
                copy.start()
        if step == heads - 2:
            weights = []
            for s in range(1, heads):
                there = lax.rem(head + s, heads)
                for i, (src, dst) in enumerate(((enc, out_e.at[head]), (qkv.at[there], out_q.at[head]), (vec, out_v.at[head]))):
                    slot = (s - 1) * 3 + i
                    weights.append(pltpu.make_async_remote_copy(
                        src_ref=src, dst_ref=dst, send_sem=w_s.at[slot], recv_sem=w_r.at[slot], device_id=(node, there), device_id_type=MESH))
                    weights[-1].start()
        for upward in (True, False):
            @pl.when(gets(step, upward))
            def _(step=step, upward=upward):
                relay(step, upward).wait_recv()
                shard = head - 1 - step if upward else head + 1 + step
                for way in range(2):
                    halo(shard, out_f.at[1, shard], way).start()
    for step in range(heads - 1):
        for upward in (True, False):
            @pl.when(sends(step, upward))
            def _(step=step, upward=upward):
                relay(step, upward).wait_send()
    for copy in own + weights:
        copy.wait()
    for shard in range(heads):
        for way in range(2):
            halo(shard, feat, way).wait()


def front(feat, enc, qkv, vec, nodes, heads):
    dma = pltpu.SemaphoreType.DMA
    vmem, anywhere = pl.BlockSpec(memory_space=pltpu.VMEM), pl.BlockSpec(memory_space=pl.ANY)
    n = 3 * (heads - 1)
    return pl.pallas_call(
        functools.partial(front_kernel, nodes, heads),
        in_specs=[vmem] * 4, out_specs=[anywhere] + [vmem] * 3,
        out_shape=[jax.ShapeDtypeStruct((3, heads, *feat.shape), feat.dtype), jax.ShapeDtypeStruct((heads, *enc.shape), enc.dtype),
                   jax.ShapeDtypeStruct(qkv.shape, qkv.dtype), jax.ShapeDtypeStruct((heads, *vec.shape), vec.dtype)],
        scratch_shapes=[dma((heads - 1,))] * 4 + [dma((2, heads))] * 2 + [dma((n,))] * 2 + [dma((4,))],
        compiler_params=pltpu.CompilerParams(collective_id=2, has_side_effects=True, vmem_limit_bytes=24 << 20),
        name="front",
    )(feat, enc, qkv, vec)


def pair_kernel(nodes, heads, down, up, out, slab, got_d, got_u, got_o, own_d, own_u, own_o, s_sem, r_sem, l_sem):
    node, head = lax.axis_index("nodes"), lax.axis_index("heads")
    chips = nodes // 2
    chip, side = lax.div(node, 2), lax.rem(node, 2)
    twin = chip * 2 + 1 - side
    barrier = pltpu.get_barrier_semaphore()
    pl.semaphore_signal(barrier, inc=1, device_id=(twin, head), device_id_type=MESH)
    pl.semaphore_wait(barrier, 1)
    moves = []
    for i, (src, got, own) in enumerate(((down, got_d, own_d), (up, got_u, own_u), (out, got_o, own_o))):
        local = pltpu.make_async_copy(src.at[:, :, side], own, l_sem.at[i])
        remote = pltpu.make_async_remote_copy(
            src_ref=src.at[:, :, 1 - side], dst_ref=got, send_sem=s_sem.at[i], recv_sem=r_sem.at[i], device_id=(twin, head), device_id_type=MESH)
        local.start()
        remote.start()
        moves.append((local, remote))
    width = out.shape[-1]
    at = 0
    for (local, remote), got, own in zip(moves, (got_d, got_u, got_o), (own_d, own_u, own_o)):
        local.wait()
        remote.wait()
        rows = own.shape[2]
        for c in range(0, own.shape[3], width):
            for s in range(chips):
                there = lax.rem(chip + s, chips)
                slab[s, :, at:at + rows, :] = own[:, there, :, c:c + width] + got[:, there, :, c:c + width]
            at += rows


def pair(down, up, out, nodes, heads):
    chips = nodes // 2
    split = lambda a: a.reshape(heads, chips, 2, -1, a.shape[-1])
    down, up, out = split(down), split(up), split(out)
    width = out.shape[-1]
    rows = sum(a.shape[3] * a.shape[4] // width for a in (down, up, out))
    half = [pltpu.VMEM((heads, chips, *a.shape[3:]), f32) for a in (down, up, out)]
    dma = pltpu.SemaphoreType.DMA
    return pl.pallas_call(
        functools.partial(pair_kernel, nodes, heads),
        in_specs=[pl.BlockSpec(memory_space=pl.ANY)] * 3, out_specs=pl.BlockSpec(memory_space=pltpu.VMEM),
        out_shape=jax.ShapeDtypeStruct((chips, heads, rows, width), f32),
        scratch_shapes=half + half + [dma((3,))] * 3,
        compiler_params=pltpu.CompilerParams(collective_id=3, has_side_effects=True, vmem_limit_bytes=32 << 20),
        cost_estimate=pl.CostEstimate(flops=10**10, bytes_accessed=2 * 10**7, transcendentals=0),
        name="pair",
    )(down, up, out)


def send(src, dst, sems, slot, node, head):
    copy = pltpu.make_async_remote_copy(
        src_ref=src, dst_ref=dst, send_sem=sems[0].at[slot], recv_sem=sems[1].at[slot], device_id=(node, head), device_id_type=MESH)
    copy.start()
    return copy


def greet(nodes, heads, node, head):
    barrier = pltpu.get_barrier_semaphore()
    for s in range(1, nodes):
        pl.semaphore_signal(barrier, inc=1, device_id=(lax.rem(node + s, nodes), head), device_id_type=MESH)
    for s in range(1, heads):
        pl.semaphore_signal(barrier, inc=1, device_id=(node, lax.rem(head + s, heads)), device_id_type=MESH)
    pl.semaphore_wait(barrier, nodes + heads - 2)


def finish_kernel(nodes, heads, *refs):
    (qkv, enc, vec, *bulk), refs = refs[:4], refs[4:]
    (out_q, out_e, out_v, *out_b), refs = refs[:4], refs[4:]
    (q_half, q_one, q_two, q_part, q_sum, q_own, e_half, e_one, e_two, e_sum, e_three, e_own, v_half, v_two, v_three, v_one, v_sum), refs = refs[:17], refs[17:]
    s_one, r_one, s_two, r_two, s_three, r_three, s_four, r_four, s_bulk, r_bulk, s_pass, r_pass, l_sem = refs
    node, head = lax.axis_index("nodes"), lax.axis_index("heads")
    chips = nodes // 2
    chip, side = lax.div(node, 2), lax.rem(node, 2)
    twin = chip * 2 + 1 - side
    greet(nodes, heads, node, head)
    first = [send(ref.at[:, :, 1 - side], dst, (s_one, r_one), i, twin, head) for i, (ref, dst) in enumerate(((qkv, q_half), (enc, e_half)))]
    first.append(send(vec, v_half, (s_one, r_one), 2, twin, head))
    keep = [pltpu.make_async_copy(src, dst.at[node], l_sem.at[i]) for i, (src, dst) in enumerate(zip(bulk, out_b))]
    for copy in keep:
        copy.start()
    spread = []
    for s in range(chips):
        other = lax.rem(chip + s, chips) * 2 + side if s else twin
        spread.append([send(src, dst.at[node], (s_bulk, r_bulk), s + i, other, head) for i, (src, dst) in enumerate(zip(bulk, out_b))])
    for copy in first:
        copy.wait()
    q_one[...] = qkv[:, :, side] + q_half[...]
    e_one[...] = enc[:, :, side] + e_half[...]
    v_one[...] = vec[...] + v_half[...]
    second = []
    for s in range(1, chips):
        there = lax.rem(chip + s, chips)
        target = there * 2 + side
        i = (s - 1) * 3
        second.append(send(q_one.at[:, there], q_two.at[s - 1], (s_two, r_two), i, target, head))
        second.append(send(e_one.at[:, there], e_two.at[s - 1], (s_two, r_two), i + 1, target, head))
        second.append(send(v_one, v_two.at[s - 1], (s_two, r_two), i + 2, target, head))
    for copy in second:
        copy.wait()
    q_part[...] = functools.reduce(jnp.add, [q_two[s] for s in range(chips - 1)], q_one[:, chip])
    e_sum[...] = functools.reduce(jnp.add, [e_two[s] for s in range(chips - 1)], e_one[:, chip])
    v_sum[...] = functools.reduce(jnp.add, [v_two[s] for s in range(chips - 1)], v_one[...])
    third = []
    for s in range(1, heads):
        there = lax.rem(head + s, heads)
        i = (s - 1) * 3
        third.append(send(q_part.at[there], q_sum.at[head], (s_three, r_three), i, node, there))
        third.append(send(e_sum.at[there], e_three.at[s - 1], (s_three, r_three), i + 1, node, there))
        third.append(send(v_sum, v_three.at[s - 1], (s_three, r_three), i + 2, node, there))
    for copy in third:
        copy.wait()
    q_sum[pl.ds(head, 1)] = q_part[pl.ds(head, 1)]
    e_own[...] = functools.reduce(jnp.add, [e_three[s] for s in range(heads - 1)], e_sum[head])
    out_v[...] = functools.reduce(jnp.add, [v_three[s] for s in range(heads - 1)], v_sum[...])
    fourth = []
    for s in range(1, nodes):
        there = lax.rem(node + s, nodes)
        fourth.append(send(q_sum, out_q.at[node], (s_four, r_four), (s - 1) * 2, there, head))
        fourth.append(send(e_own, out_e.at[node], (s_four, r_four), (s - 1) * 2 + 1, there, head))
    out_q[node] = q_sum[...]
    out_e[node] = e_own[...]
    for copy in keep:
        copy.wait()
    passed = []
    for s in range(chips):
        for copy in spread[s]:
            copy.wait()
        if s:
            origin = lax.rem(chip + chips - s, chips) * 2 + side
            passed += [send(dst.at[origin], dst.at[origin], (s_pass, r_pass), (s - 1) + i, twin, head) for i, dst in enumerate(out_b)]
    for copy in passed:
        copy.wait()
    for copy in fourth:
        copy.wait()


def finish(qkv, enc, vec, bulk, nodes, heads):
    chips = nodes // 2
    split = lambda a: a.reshape(heads, chips, 2, -1, a.shape[-1])
    qkv, enc = split(qkv), split(enc)
    vm = lambda *s: pltpu.VMEM(s, f32)
    rq, wq, re, we = *qkv.shape[3:], *enc.shape[3:]
    dma = pltpu.SemaphoreType.DMA
    wv = vec.shape
    scratch = [vm(heads, chips, rq, wq), vm(heads, chips, rq, wq), vm(chips - 1, heads, rq, wq), vm(heads, rq, wq), vm(heads, rq, wq), vm(8, 128),
               vm(heads, chips, re, we), vm(heads, chips, re, we), vm(chips - 1, heads, re, we), vm(heads, re, we), vm(heads - 1, re, we), vm(re, we),
               vm(*wv), vm(chips - 1, *wv), vm(heads - 1, *wv), vm(*wv), vm(*wv)]
    counts = (3, 3, 3 * chips - 3, 3 * chips - 3, 3 * heads - 3, 3 * heads - 3, 2 * nodes - 2, 2 * nodes - 2, chips, chips, chips - 1, chips - 1, 1)
    out_shape = [jax.ShapeDtypeStruct(s, f32) for s in [(nodes, heads, rq, wq), (nodes, re, we), wv] + [(nodes, *b.shape) for b in bulk]]
    spec = pl.BlockSpec(memory_space=pltpu.VMEM)
    return pl.pallas_call(
        functools.partial(finish_kernel, nodes, heads),
        in_specs=[spec] * 4, out_specs=[spec] * 4, out_shape=out_shape,
        scratch_shapes=scratch + [dma((n,)) for n in counts],
        compiler_params=pltpu.CompilerParams(collective_id=1, has_side_effects=True, vmem_limit_bytes=48 << 20),
        name="finish",
    )(qkv, enc, vec, *bulk)
D = 512
HEADS = 8
NBR = 8
ADAM_STEP = 3
highest = lax.Precision.HIGHEST
beta_one = 0.5
beta_two = 0.5
learn_rate = 0.02
weight_decay = 0.1
adam_eps = 1e-08


def adamw(weight, first_moment, second, gradient):
    first_new = beta_one * first_moment + (1.0 - beta_one) * gradient
    second_new = beta_two * second + (1.0 - beta_two) * gradient * gradient
    first_hat = first_new / (1.0 - beta_one**ADAM_STEP)
    second_hat = second_new / (1.0 - beta_two**ADAM_STEP)
    weight_new = weight - learn_rate * (
        first_hat / (jnp.sqrt(second_hat) + adam_eps) + weight_decay * weight
    )
    return (weight_new, first_new, second_new)


def local(
    features, target, counts, neighbours, edge_kinds,
    enc_weight, enc_first, enc_second, qkv_weight, qkv_first, qkv_second,
    out_weight, out_first, out_second, up_weight, up_first, up_second,
    down_weight, down_first, down_second, vec_weight, vec_first, vec_second,
):
    heads_count = lax.axis_size("heads")
    nodes_count = lax.axis_size("nodes")
    head_index = lax.axis_index("heads")
    node_index = lax.axis_index("nodes")
    row_count = features.shape[0]
    own_blocks = row_count // BLOCK
    group_blocks = own_blocks * heads_count
    group_rows = group_blocks * BLOCK
    hl = HEADS // heads_count
    hs = D // HEADS
    cols = hl * hs
    cp = -(-cols // 128) * 128
    ka = -(-(cols + 1) // 128) * 128
    kinds = D // HEADS
    slots = NBR + 1
    low = lambda a: a.astype(bf16)
    gather = lambda a, axis: lax.all_gather(low(a), "heads", axis=axis, tiled=True)

    qkv_parts = jnp.transpose(low(qkv_weight).reshape(-1, heads_count, hl, 3, hs), (1, 0, 3, 2, 4)).reshape(heads_count, -1, 3, cols)
    qkv_parts = jnp.pad(qkv_parts, ((0, 0), (0, 0), (0, 0), (0, cp - cols))).reshape(heads_count, -1, 3 * cp)
    vec_part = jnp.pad(low(vec_weight).astype(f32), ((0, 2), (0, 0)))
    feats, enc_b, qkv_cols, vectors = front(features, low(enc_weight), qkv_parts, vec_part, nodes_count, heads_count)
    feats = feats.reshape(3 * group_rows, -1)
    enc_b = enc_b.reshape(-1, D)
    qkv_cols = qkv_cols.reshape(D, 3 * cp)
    vectors = jnp.transpose(vectors, (1, 0, 2)).reshape(8, D)
    up_low, out_low, down_low, enc_b = lax.optimization_barrier((low(up_weight), low(out_weight), low(down_weight), enc_b))
    wide_b = lax.all_gather(jnp.concatenate([up_low, out_low], axis=1), "heads", axis=0, tiled=True)
    down_b = lax.all_gather(down_low, "heads", axis=0, tiled=True)

    enc_bias, gain_one, gain_two, gain_three, head_vec = (vectors[r] for r in range(5))
    edge_local = lax.dynamic_slice_in_dim(vectors[5].reshape(kinds, HEADS), head_index * hl, hl, 1)
    own_counts = lax.dynamic_slice_in_dim(counts, (node_index * heads_count + head_index) * own_blocks, own_blocks)
    row_live = (jnp.arange(BLOCK, dtype=jnp.int32)[None, :] < own_counts[:, None]).reshape(row_count).astype(f32)
    live_total = jnp.sum(counts).astype(f32)

    def group_counts(offset):
        return lax.dynamic_slice_in_dim(counts, (node_index + offset) % nodes_count * group_blocks, group_blocks)

    pool_counts = jnp.concatenate([group_counts(nodes_count - 1), group_counts(0), group_counts(1)])
    relative = (neighbours // group_blocks - node_index + 1) % nodes_count
    nbr_pos = relative * group_blocks + neighbours % group_blocks
    self_pos = group_blocks + jnp.arange(group_blocks, dtype=jnp.int32)
    key_pos = jnp.concatenate([self_pos[:, None], nbr_pos], axis=1).reshape(-1)
    kind_hot = jax.nn.one_hot(edge_kinds, kinds, dtype=f32)
    slot_bias = jnp.einsum("bst,th->bsh", kind_hot, edge_local, precision=highest)
    bias_rows = jnp.repeat(slot_bias, BLOCK, axis=2)

    kaug, kt, value, vt, query = encode(
        pool_counts, feats, enc_b, enc_bias[None], gain_one[None], qkv_cols, cp, ka, cols, hs**-0.5)
    side = jnp.stack([target, row_live], axis=1)
    dense_vec = jnp.stack([enc_bias, gain_two, gain_three, head_vec])
    half = lambda a: a.reshape(heads_count, 2, row_count // 2, -1)
    exchange = lambda a: lax.all_to_all(a, "heads", split_axis=0, concat_axis=0, tiled=True)
    attn_parts, lse_parts, grad_parts, totals = [], [], [], None
    for part in range(2):
        attn_part, lse_part = attend(part, own_blocks, key_pos, query, bias_rows, kaug, vt, hl, hs)
        attn_parts.append(attn_part)
        lse_parts.append(lse_part)
    wide_b, down_b, attn_parts[1] = lax.optimization_barrier((wide_b, down_b, attn_parts[1]))
    up_b, out_b = wide_b[:, :up_weight.shape[1]], wide_b[:, up_weight.shape[1]:]
    for part in range(2):
        attn_rows = exchange(attn_parts[part].reshape(heads_count, row_count // 2, cp)[..., :cols])
        grad_part, *totals = dense(part, live_total[None], attn_rows, features, side, dense_vec, enc_b, out_b, up_b, down_b, totals)
        grad_parts.append(exchange(grad_part))
    grad_down, grad_up, grad_out, denc_own, dense_sums = totals
    grad_parts[0], grad_down = lax.optimization_barrier((grad_parts[0], grad_down))
    slab = pair(grad_down, grad_up, grad_out, nodes_count, heads_count)
    moved = [slab[0]] + [
        lax.ppermute(slab[s], "nodes", [(i, (i + 2 * s) % nodes_count) for i in range(nodes_count)]) for s in range(1, nodes_count // 2)]
    grad_heads = jnp.concatenate([g[:, None] for g in grad_parts], axis=1).reshape(group_rows, cols)
    grad_heads = jnp.pad(grad_heads, ((0, 0), (0, cp - cols)))
    dq, dkv, edge_sums = attend_back(own_blocks, key_pos, query, grad_heads, attn_parts, lse_parts, bias_rows, kaug, value, kt, hl, hs)
    moved, dkv = lax.optimization_barrier((moved, dkv))
    planes = exchange(functools.reduce(jnp.add, moved))
    slot_sums = jnp.sum(edge_sums.reshape(group_blocks, slots, hl, BLOCK), axis=3)
    edge_grad = jnp.einsum("bst,bsh->th", kind_hot, slot_sums, precision=highest)
    columns = lambda a: jnp.broadcast_to(a[:, None], (D, 128))
    dw, denc_t, dgain, dbias = encode_back(
        feats, dkv, dq, enc_b.T, columns(enc_bias), columns(gain_one), qkv_cols[:, :cp], qkv_cols[:, cp:])

    grad_gain_one = jnp.sum(dgain, axis=1)
    grad_enc_bias = jnp.sum(dbias, axis=1) + dense_sums[0]
    grad_enc = denc_t.T + denc_own
    edge_full = lax.dynamic_update_slice(jnp.zeros((kinds, HEADS), f32), edge_grad, (jnp.int32(0), head_index * hl))
    grad_vec = jnp.concatenate([grad_enc_bias[None], grad_gain_one[None], dense_sums[1:5], edge_full.reshape(1, D), jnp.zeros((1, D), f32)])
    planes, dw = lax.optimization_barrier((planes, dw))
    dw_sum, enc_sum, vec_total, bulk = finish(dw, grad_enc, grad_vec, [jnp.sum(planes, axis=0)], nodes_count, heads_count)
    total_loss = vec_total[5, 0]
    vec_sum = lax.dynamic_slice_in_dim(jnp.concatenate([vec_total[:5], vec_total[6:7]]), head_index * (D // heads_count), D // heads_count, 1)
    qkv_sum = jnp.transpose(dw_sum, (0, 2, 1, 3)).reshape(-1, heads_count, 3, cp)[..., :cols].reshape(-1, heads_count, 3, hl, hs)
    qkv_sum = jnp.transpose(qkv_sum, (0, 1, 3, 2, 4)).reshape(qkv_weight.shape)
    flat = lambda a: a.reshape(-1, a.shape[-1])
    rows_down, rows_out = down_weight.shape[0] // nodes_count, out_weight.shape[0] // nodes_count
    up_sum = bulk[:, rows_down:-rows_out].reshape(nodes_count, -1, rows_out, D)
    up_sum = jnp.transpose(up_sum, (0, 2, 1, 3)).reshape(up_weight.shape)
    summed = (flat(enc_sum), qkv_sum, flat(bulk[:, -rows_out:]), up_sum, flat(bulk[:, :rows_down]), vec_sum)
    enc_res = adamw(enc_weight, enc_first, enc_second, summed[0])
    qkv_res = adamw(qkv_weight, qkv_first, qkv_second, summed[1])
    out_res = adamw(out_weight, out_first, out_second, summed[2])
    up_res = adamw(up_weight, up_first, up_second, summed[3])
    down_res = adamw(down_weight, down_first, down_second, summed[4])
    vec_res = adamw(vec_weight, vec_first, vec_second, summed[5])
    loss_value = (total_loss / live_total).reshape(1)
    return (
        loss_value, *enc_res, *qkv_res, *out_res, *up_res, *down_res, *vec_res,
        low(enc_res[0]), low(qkv_res[0]), low(out_res[0]), low(up_res[0]), low(down_res[0]),
    )


def solution(mesh):
    rows = P("heads", None)
    both = P(("nodes", "heads"))
    lanes = P(None, "heads")
    in_specs = (P(("nodes", "heads"), None), both, P(), P("nodes", None), P("nodes", None)) + (rows,) * 15 + (lanes,) * 3
    out_specs = (P(),) + (rows,) * 15 + (lanes,) * 3 + (rows,) * 5
    return jax.shard_map(local, mesh=mesh, in_specs=in_specs, out_specs=out_specs, check_vma=False)
```

```python
import functools

import jax
import jax.numpy as jnp
from jax import lax
from jax.experimental import pallas as pl
from jax.experimental.pallas import tpu as pltpu
from jax.sharding import PartitionSpec as P

BLOCK = 128
NT = (((1,), (1,)), ((), ()))
NN = (((1,), (0,)), ((), ()))
f32 = jnp.float32
bf16 = jnp.bfloat16


def dotf(a, b, dims):
    return lax.dot_general(a, b, dims, preferred_element_type=f32)


def head_rows(x, hl, hs, cp):
    if hl == 1:
        return x
    lane = lax.broadcasted_iota(jnp.int32, (BLOCK, cp), 1)
    zero = jnp.zeros_like(x)
    return jnp.concatenate([jnp.where(lane // hs == h, x, zero) for h in range(hl)], axis=0)


def ones_lane(hl, cp, ka):
    rows = hl * BLOCK
    lane = lax.broadcasted_iota(jnp.int32, (rows, ka - cp), 1)
    return jnp.where(lane == 0, 1.0, 0.0).astype(bf16)


def attend_kernel(hl, hs, cp, ka, slots, unit, unit_of, pos_ref, q_ref, brow_ref, kaug_ref, vt_ref, o_ref, lse_ref, *scratch):
    first = unit_of(pl.program_id(0)) * unit
    rows = hl * BLOCK

    def spot(u, s):
        return pos_ref[(first + u) * slots + s]

    def score(u):
        s_ref = scratch[2 * (u % 2)]
        q2 = head_rows(q_ref[u * BLOCK:(u + 1) * BLOCK, :], hl, hs, cp)
        qa = jnp.concatenate([q2, ones_lane(hl, cp, ka)], axis=1) if ka > cp else q2
        keys = [kaug_ref[pl.ds(pl.multiple_of(spot(u, s) * BLOCK, BLOCK), BLOCK), :] for s in range(slots)]
        scores = dotf(jnp.concatenate(keys, axis=0), qa, NT)
        top = None
        for s in range(slots):
            sc = scores[s * BLOCK:(s + 1) * BLOCK]
            s_ref[s] = sc
            t = jnp.max(sc, axis=0, keepdims=True) + brow_ref[u, s:s + 1, :]
            top = t if top is None else jnp.maximum(top, t)
        return top

    def weigh(u, top):
        s_ref, p_ref = scratch[2 * (u % 2):2 * (u % 2) + 2]
        tot = jnp.zeros((1, rows), f32)
        for s in range(slots):
            e = jnp.exp(s_ref[s] - (top - brow_ref[u, s:s + 1, :]))
            s_ref[s] = e
            tot = tot + jnp.sum(e, axis=0, keepdims=True)
        lse_ref[u] = top + jnp.log(tot)
        inv = 1.0 / tot
        for s in range(slots):
            p_ref[s * BLOCK:(s + 1) * BLOCK, :] = (s_ref[s] * inv).astype(bf16)

    def total(u):
        p_ref = scratch[2 * (u % 2) + 1]
        ot = dotf(jnp.concatenate([vt_ref[spot(u, s)] for s in range(slots)], axis=1), p_ref[...], NN)
        parts = [ot[h * hs:(h + 1) * hs, h * BLOCK:(h + 1) * BLOCK] for h in range(hl)]
        if hl * hs < cp:
            parts.append(jnp.zeros((cp - hl * hs, BLOCK), f32))
        o_ref[u * BLOCK:(u + 1) * BLOCK, :] = jnp.concatenate(parts, axis=0).T.astype(bf16)

    top = score(0)
    for u in range(unit):
        following = score(u + 1) if u + 1 < unit else None
        weigh(u, top)
        total(u)
        top = following


def attend(part, own, pos, q, brow, kaug, vt, hl, hs, unit=4):
    cp, ka = q.shape[1], kaug.shape[1]
    nb = q.shape[0] // BLOCK // 2
    half, own = own // 2 // unit, own // unit
    unit_of = lambda i: lax.div(i, half) * own + part * half + lax.rem(i, half)
    slots = brow.shape[1]
    rows = hl * BLOCK
    whole = lambda a: pl.BlockSpec(a.shape, lambda i, *_: (0,) * a.ndim, pipeline_mode=pl.Buffered(1))
    return pl.pallas_call(
        functools.partial(attend_kernel, hl, hs, cp, ka, slots, unit, unit_of),
        grid_spec=pltpu.PrefetchScalarGridSpec(
            num_scalar_prefetch=1, grid=(nb // unit,),
            in_specs=[pl.BlockSpec((unit * BLOCK, cp), lambda i, *_: (unit_of(i), 0)),
                      pl.BlockSpec((unit, slots, rows), lambda i, *_: (unit_of(i), 0, 0)),
                      whole(kaug), whole(vt)],
            out_specs=[pl.BlockSpec((unit * BLOCK, cp), lambda i, *_: (i, 0)),
                       pl.BlockSpec((unit, 1, rows), lambda i, *_: (i, 0, 0))],
            scratch_shapes=[pltpu.VMEM((slots, BLOCK, rows), f32), pltpu.VMEM((slots * BLOCK, rows), bf16)] * 2),
        out_shape=[jax.ShapeDtypeStruct((nb * BLOCK, cp), bf16), jax.ShapeDtypeStruct((nb, 1, rows), f32)],
        cost_estimate=pl.CostEstimate(flops=nb * 10**9, bytes_accessed=3 * 10**7, transcendentals=0),
        compiler_params=pltpu.CompilerParams(vmem_limit_bytes=67043328),
        name="attend",
    )(pos, q, brow, kaug, vt)


def attend_back_kernel(hl, hs, cp, ka, slots, scale, unit, unit_of, pos_ref, q_ref, do_ref, oa_ref, ob_ref, la_ref, lb_ref, brow_ref, kaug_ref, v_ref,
                       kt_ref, dq_ref, dkv_ref, edge_ref, *scratch):
    i = pl.program_id(0)
    first = unit_of(i) * unit
    late = i >= pl.num_programs(0) // 2

    @pl.when(i == 0)
    def _():
        @pl.loop(0, dkv_ref.shape[0] // BLOCK)
        def _(n):
            dkv_ref[pl.ds(pl.multiple_of(n * BLOCK, BLOCK), BLOCK), :] = jnp.zeros((BLOCK, dkv_ref.shape[1]), f32)

    for u in range(unit):
        p_ref, d_ref = scratch[2 * (u % 2):2 * (u % 2) + 2]
        own = slice(u * BLOCK, (u + 1) * BLOCK)
        q2 = head_rows(q_ref[own, :], hl, hs, cp)
        qa = jnp.concatenate([q2, ones_lane(hl, cp, ka)], axis=1) if ka > cp else q2
        do = do_ref[own, :]
        do2 = head_rows(do, hl, hs, cp)
        prod = (do.astype(f32) * jnp.where(late, ob_ref[own, :], oa_ref[own, :]).astype(f32)).T
        dd = jnp.concatenate([jnp.sum(prod[h * hs:(h + 1) * hs], axis=0, keepdims=True) for h in range(hl)], axis=1)
        lse = jnp.where(late, lb_ref[u], la_ref[u])
        blocks = [pos_ref[(first + u) * slots + s] for s in range(slots)]
        spots = [pl.ds(pl.multiple_of(p * BLOCK, BLOCK), BLOCK) for p in blocks]
        scores = dotf(jnp.concatenate([kaug_ref[at, :] for at in spots], axis=0), qa, NT)
        grads = dotf(jnp.concatenate([v_ref[at, :] for at in spots], axis=0), do2, NT)
        for s in range(slots):
            here = slice(s * BLOCK, (s + 1) * BLOCK)
            pr = jnp.exp(scores[here] - (lse - brow_ref[u, s:s + 1, :]))
            ds = pr * (grads[here] - dd)
            edge_ref[u, s:s + 1, :] = jnp.sum(ds, axis=0, keepdims=True)
            p_ref[here, :] = pr.astype(bf16)
            d_ref[here, :] = ds.astype(bf16)
        dv = dotf(p_ref[...], do2, NN)
        dk = dotf(d_ref[...], q2, NN)
        dqt = dotf(jnp.concatenate([kt_ref[p] for p in blocks], axis=1), d_ref[...], NN)
        for s, at in enumerate(spots):
            here = slice(s * BLOCK, (s + 1) * BLOCK)
            dkv_ref[at, 0:cp] += dk[here]
            dkv_ref[at, cp:2 * cp] += dv[here]
        parts = [dqt[h * hs:(h + 1) * hs, h * BLOCK:(h + 1) * BLOCK] for h in range(hl)]
        if hl * hs < cp:
            parts.append(jnp.zeros((cp - hl * hs, BLOCK), f32))
        dq_ref[own, :] = (jnp.concatenate(parts, axis=0).T * scale).astype(bf16)


def attend_back(own, pos, q, do, outs, lses, brow, kaug, v, kt, hl, hs, unit=4):
    cp, ka = q.shape[1], kaug.shape[1]
    nb = q.shape[0] // BLOCK
    slots = brow.shape[1]
    rows = hl * BLOCK
    half, mid, own = own // 2 // unit, nb // 2 // unit, own // unit
    unit_of = lambda i: lax.div(lax.rem(i, mid), half) * own + lax.div(i, mid) * half + lax.rem(i, half)
    whole = lambda a: pl.BlockSpec(a.shape, lambda i, *_: (0,) * a.ndim, pipeline_mode=pl.Buffered(1))
    tile = pl.BlockSpec((unit * BLOCK, cp), lambda i, *_: (unit_of(i), 0))
    early = lambda i: jnp.minimum(i, mid - 1)
    late = lambda i: jnp.maximum(i - mid, 0)
    return pl.pallas_call(
        functools.partial(attend_back_kernel, hl, hs, cp, ka, slots, hs ** -0.5, unit, unit_of),
        grid_spec=pltpu.PrefetchScalarGridSpec(
            num_scalar_prefetch=1, grid=(nb // unit,),
            in_specs=[tile, tile,
                      pl.BlockSpec((unit * BLOCK, cp), lambda i, *_: (early(i), 0)), pl.BlockSpec((unit * BLOCK, cp), lambda i, *_: (late(i), 0)),
                      pl.BlockSpec((unit, 1, rows), lambda i, *_: (early(i), 0, 0)), pl.BlockSpec((unit, 1, rows), lambda i, *_: (late(i), 0, 0)),
                      pl.BlockSpec((unit, slots, rows), lambda i, *_: (unit_of(i), 0, 0)),
                      whole(kaug), whole(v), whole(kt)],
            out_specs=[tile, pl.BlockSpec((v.shape[0], 2 * cp), lambda i, *_: (0, 0), pipeline_mode=pl.Buffered(1)),
                       pl.BlockSpec((unit, slots, rows), lambda i, *_: (unit_of(i), 0, 0))],
            scratch_shapes=[pltpu.VMEM((slots * BLOCK, rows), bf16)] * 4),
        out_shape=[jax.ShapeDtypeStruct(q.shape, bf16), jax.ShapeDtypeStruct((v.shape[0], 2 * cp), f32),
                   jax.ShapeDtypeStruct((nb, slots, rows), f32)],
        cost_estimate=pl.CostEstimate(flops=nb * 2 * 10**9, bytes_accessed=6 * 10**7, transcendentals=0),
        compiler_params=pltpu.CompilerParams(vmem_limit_bytes=67043328),
        name="attend_back",
    )(pos, q, do, *outs, *lses, brow, kaug, v, kt)
norm_eps = 1e-05


def encode_kernel(cp, ka, cols, scale, per_group, cnt_ref, x_ref, enc_ref, bias_ref, gain_ref, w_ref,
                  kaug_ref, kt_ref, v_ref, vt_ref, q_ref):
    i = pl.program_id(0)
    group = i // per_group
    tile = x_ref.shape[0]
    resid = dotf(x_ref[...], enc_ref[...], NN) + bias_ref[...]
    centred = resid - jnp.mean(resid, axis=-1, keepdims=True)
    variance = jnp.mean(centred * centred, axis=-1, keepdims=True)
    act = (centred * lax.rsqrt(variance + norm_eps) * gain_ref[...]).astype(bf16)
    kv = dotf(act, w_ref[:, cp:], NN).astype(bf16)
    key, value = kv[:, :cp], kv[:, cp:]
    row = lax.broadcasted_iota(jnp.int32, (BLOCK, 128), 0)
    lane = lax.broadcasted_iota(jnp.int32, (BLOCK, 128), 1)
    first = i * (tile // BLOCK)
    dead = jnp.concatenate(
        [jnp.where((row >= cnt_ref[first + j]) & (lane == cols % 128), -1e30, 0.0) for j in range(tile // BLOCK)], axis=0).astype(bf16)
    if ka > cp:
        kaug_ref[:, :cp] = key
        kaug_ref[:, cp:] = dead
    else:
        kaug_ref[...] = key + dead
    v_ref[...] = value
    for j in range(tile // BLOCK):
        kt_ref[j] = key[j * BLOCK:(j + 1) * BLOCK].T
        vt_ref[j] = value[j * BLOCK:(j + 1) * BLOCK].T

    @pl.when(group == 1)
    def _():
        q = (dotf(act, w_ref[:, :cp], NN) * scale).astype(bf16)
        if ka == cp:
            lanes = lax.broadcasted_iota(jnp.int32, q.shape, 1)
            q = jnp.where(lanes == cols, jnp.ones_like(q), q)
        q_ref[...] = q


def encode(counts, feats, enc, bias, gain, w, cp, ka, cols, scale, tile=2048):
    rows, feat = feats.shape[0] // 3, feats.shape[1]
    width = enc.shape[1]
    per = rows // tile
    blocks = tile // BLOCK
    whole = lambda a: pl.BlockSpec(a.shape, lambda i, *_: (0,) * a.ndim, pipeline_mode=pl.Buffered(1))
    return pl.pallas_call(
        functools.partial(encode_kernel, cp, ka, cols, scale, per),
        grid_spec=pltpu.PrefetchScalarGridSpec(
            num_scalar_prefetch=1, grid=(3 * per,),
            in_specs=[pl.BlockSpec((tile, feat), lambda i, *_: (i, 0)), whole(enc), whole(bias), whole(gain), whole(w)],
            out_specs=[pl.BlockSpec((tile, ka), lambda i, *_: (i, 0)),
                       pl.BlockSpec((blocks, cp, BLOCK), lambda i, *_: (i, 0, 0)),
                       pl.BlockSpec((tile, cp), lambda i, *_: (i, 0)),
                       pl.BlockSpec((blocks, cp, BLOCK), lambda i, *_: (i, 0, 0)),
                       pl.BlockSpec((tile, cp), lambda i, *_: (jnp.clip(i - per, 0, per - 1), 0))]),
        out_shape=[jax.ShapeDtypeStruct((3 * rows, ka), bf16),
                   jax.ShapeDtypeStruct((3 * rows // BLOCK, cp, BLOCK), bf16),
                   jax.ShapeDtypeStruct((3 * rows, cp), bf16),
                   jax.ShapeDtypeStruct((3 * rows // BLOCK, cp, BLOCK), bf16),
                   jax.ShapeDtypeStruct((rows, cp), bf16)],
        compiler_params=pltpu.CompilerParams(vmem_limit_bytes=67043328),
        cost_estimate=pl.CostEstimate(flops=rows * 6 * 10**6, bytes_accessed=3 * 10**7, transcendentals=0),
        name="encode",
    )(counts, feats, enc, bias, gain, w)


def encode_back_kernel(cp, per_group, x_ref, dkv_ref, dq_ref, enct_ref, bias_ref, gain_ref, wq_ref, wkv_ref,
                       dw_ref, denc_ref, dgain_ref, dbias_ref, g_ref):
    i = pl.program_id(0)
    group = i // per_group
    tile = x_ref.shape[0]
    width = enct_ref.shape[0]
    reps = tile // 128

    @pl.when(i == 0)
    def _():
        for ref in (dw_ref, denc_ref, dgain_ref, dbias_ref):
            ref[...] = jnp.zeros_like(ref)

    x = x_ref[...]
    wide = lambda c: jnp.concatenate([c] * reps, axis=1)
    fold = lambda a: functools.reduce(jnp.add, [a[:, r * 128:(r + 1) * 128] for r in range(reps)])
    resid = dotf(enct_ref[...], x, NT) + wide(bias_ref[...])
    centred = resid - jnp.sum(resid, axis=0, keepdims=True) * (1.0 / width)
    variance = jnp.sum(centred * centred, axis=0, keepdims=True) * (1.0 / width)
    inv = lax.rsqrt(variance + norm_eps)
    norm = centred * inv
    gain = wide(gain_ref[...])
    act = (norm * gain).astype(bf16)
    dkv = dkv_ref[...].astype(bf16)
    g_ref[...] = dotf(wkv_ref[...], dkv, NT)
    dw_ref[:, cp:] += dotf(act, dkv, NN)

    @pl.when(group == 1)
    def _():
        dq = dq_ref[...]
        g_ref[...] += dotf(wq_ref[...], dq, NT)
        dw_ref[:, :cp] += dotf(act, dq, NN)

    grad = g_ref[...]
    dgain_ref[...] += fold(grad * norm)
    back = grad * gain
    mean_one = jnp.sum(back, axis=0, keepdims=True) * (1.0 / width)
    mean_two = jnp.sum(back * norm, axis=0, keepdims=True) * (1.0 / width)
    din = inv * (back - mean_one - norm * mean_two)
    dbias_ref[...] += fold(din)
    denc_ref[...] += dotf(din.astype(bf16), x, NN)


def encode_back(feats, dkv, dq, enct, bias, gain, wq, wkv, tile=2048):
    rows, feat = feats.shape[0] // 3, feats.shape[1]
    width = enct.shape[0]
    cp = dq.shape[1]
    per = rows // tile
    whole = lambda a: pl.BlockSpec(a.shape, lambda i: (0,) * a.ndim, pipeline_mode=pl.Buffered(1))
    keep = lambda s: pl.BlockSpec(s, lambda i: (0,) * len(s), pipeline_mode=pl.Buffered(1))
    shapes = [(width, 3 * cp), (width, feat), (width, 128), (width, 128)]
    return pl.pallas_call(
        functools.partial(encode_back_kernel, cp, per),
        grid=(3 * per,),
        in_specs=[pl.BlockSpec((tile, feat), lambda i: (i, 0)), pl.BlockSpec((tile, 2 * cp), lambda i: (i, 0)),
                  pl.BlockSpec((tile, cp), lambda i: (jnp.clip(i - per, 0, per - 1), 0)),
                  whole(enct), whole(bias), whole(gain), whole(wq), whole(wkv)],
        out_specs=[keep(s) for s in shapes],
        out_shape=[jax.ShapeDtypeStruct(s, f32) for s in shapes],
        scratch_shapes=[pltpu.VMEM((width, tile), f32)],
        compiler_params=pltpu.CompilerParams(vmem_limit_bytes=67043328),
        cost_estimate=pl.CostEstimate(flops=rows * 10**7, bytes_accessed=4 * 10**7, transcendentals=0),
        name="encode_back",
    )(feats, dkv, dq, enct, bias, gain, wq, wkv)


def row_norm(values):
    centred = values - jnp.mean(values, axis=-1, keepdims=True)
    inv = lax.rsqrt(jnp.mean(centred * centred, axis=-1, keepdims=True) + norm_eps)
    return centred * inv, inv


def norm_back(grad, norm, inv):
    return inv * (grad - jnp.mean(grad, axis=-1, keepdims=True) - norm * jnp.mean(grad * norm, axis=-1, keepdims=True))


def packed_dense_kernel(split, first, chunk, *refs):
    rows_down, rows_out = split
    packed, out_ref, up_ref, down_ref = refs[6], *refs[-3:]
    width = packed.shape[-1]

    @pl.when(pl.program_id(0) == 0)
    def _():
        for h in range(packed.shape[0]):
            for j in range(packed.shape[1]):
                k = h * packed.shape[1] + j
                down_ref[k * rows_down:(k + 1) * rows_down, :] = packed[h, j, :rows_down]
                for c in range(up_ref.shape[1] // width):
                    at = rows_down + c * rows_out
                    up_ref[k * rows_out:(k + 1) * rows_out, c * width:(c + 1) * width] = packed[h, j, at:at + rows_out]
                out_ref[k * rows_out:(k + 1) * rows_out, :] = packed[h, j, packed.shape[2] - rows_out:]

    dense_kernel(first, chunk, *refs[:6], out_ref, up_ref, down_ref, *refs[7:-3])


def dense_kernel(first, chunk, total_ref, attn_ref, feat_ref, side_ref, vec_ref, enc_ref, *refs):
    out_ref, up_ref, down_ref = refs[:3]
    refs = refs[3:]
    if not first:
        olds, refs = refs[:5], refs[5:]
    gattn_ref, ddown_ref, dup_ref, dout_ref, denc_ref, dvec_ref, u_ref, g_ref = refs
    i = pl.program_id(0)

    @pl.when(i == 0)
    def _():
        for n, ref in enumerate((ddown_ref, dup_ref, dout_ref, denc_ref, dvec_ref)):
            ref[...] = jnp.zeros_like(ref) if first else olds[n][...]

    heads = attn_ref.shape[0]
    ff = up_ref.shape[1]
    bias, gain_two, gain_three, head_vec = (vec_ref[r:r + 1, :] for r in range(4))
    target, live = side_ref[:, 0:1], side_ref[:, 1:2]
    attn = jnp.concatenate([attn_ref[h] for h in range(heads)], axis=1)
    feat = feat_ref[...]
    hidden_one = dotf(feat, enc_ref[...], NN) + bias + dotf(attn, out_ref[...], NN)
    norm_two, inv_two = row_norm(hidden_one)
    act_two = (norm_two * gain_two).astype(bf16)
    root = 0.7978845608028654
    acts = []
    for c in range(0, ff, chunk):
        u = dotf(act_two, up_ref[:, c:c + chunk], NN)
        square = u * u
        half = 0.5 * (1.0 + jnp.tanh(root * (u + 0.044715 * (u * square))))
        act = (u * half).astype(bf16)
        u_ref[:, c:c + chunk] = half + 2.0 * u * half * (1.0 - half) * (root * (1.0 + 0.134145 * square))
        g_ref[:, c:c + chunk] = act
    hidden_two = hidden_one + dotf(g_ref[...], down_ref[...], NN)
    norm_three, inv_three = row_norm(hidden_two)
    scaled = norm_three * gain_three
    error = jnp.sum(scaled * head_vec, axis=-1, keepdims=True) - target
    weighed = live * error
    grad_pred = 2.0 * weighed / total_ref[0]
    grad_two = norm_back(grad_pred * (head_vec * gain_three), norm_three, inv_three)
    low_two = grad_two.astype(bf16)
    act_two_t = act_two.T
    for c in range(0, ff, chunk):
        ddown_ref[c:c + chunk, :] += dotf(g_ref[:, c:c + chunk].T, low_two, NN)
        grad_up = (u_ref[:, c:c + chunk] * dotf(low_two, down_ref[c:c + chunk, :], NT)).astype(bf16)
        dup_ref[:, c:c + chunk] += dotf(act_two_t, grad_up, NN)
        g_ref[:, c:c + chunk] = grad_up
    grad_act_two = dotf(g_ref[...], up_ref[...], NT)
    grad_one = grad_two + norm_back(grad_act_two * gain_two, norm_two, inv_two)
    low_one = grad_one.astype(bf16)
    dout_ref[...] += dotf(attn.T, low_one, NN)
    denc_ref[...] += dotf(feat.T, low_one, NN)
    gattn = dotf(low_one, out_ref[...], NT).astype(bf16)
    width = gattn.shape[1] // heads
    for h in range(heads):
        gattn_ref[h] = gattn[:, h * width:(h + 1) * width]
    down = lambda a: jnp.sum(a, axis=0, keepdims=True)
    loss = jnp.broadcast_to(jnp.sum(weighed * error, axis=0, keepdims=True), (1, bias.shape[1]))
    dvec_ref[...] += jnp.concatenate(
        [down(grad_one), down(grad_act_two * norm_two), down(grad_pred * head_vec * norm_three), down(grad_pred * scaled), loss,
         jnp.zeros((3, bias.shape[1]), f32)], axis=0)


def dense(part, total, attn, feat, side, vec, enc, weights, ff, olds=None, tile=512, chunk=1024):
    heads, rows, cols = attn.shape
    width = enc.shape[1]
    per = rows // tile
    first = olds is None
    whole = lambda a: pl.BlockSpec(a.shape, lambda i: (0,) * a.ndim, pipeline_mode=pl.Buffered(1))
    keep = lambda s: pl.BlockSpec(s, lambda i: (0,) * len(s), pipeline_mode=pl.Buffered(1))
    shapes = [(ff, width), (width, ff), (width, width), (feat.shape[1], width), (8, width)]
    olds = () if first else tuple(olds)
    kernel, extra = dense_kernel, []
    if len(weights) == 1:
        pieces = weights[0].shape[0] * weights[0].shape[1]
        kernel = functools.partial(packed_dense_kernel, (ff // pieces, width // pieces))
        extra = [pltpu.VMEM((width, width), bf16), pltpu.VMEM((width, ff), bf16), pltpu.VMEM((ff, width), bf16)]
    return pl.pallas_call(
        functools.partial(kernel, first, chunk),
        grid=(per,),
        in_specs=[pl.BlockSpec(memory_space=pltpu.SMEM),
                  pl.BlockSpec((heads, tile, cols), lambda i: (0, i, 0)),
                  pl.BlockSpec((tile, feat.shape[1]), lambda i: (part * per + i, 0)),
                  pl.BlockSpec((tile, side.shape[1]), lambda i: (part * per + i, 0)),
                  whole(vec), whole(enc)] + [whole(w) for w in weights] + [whole(o) for o in olds],
        out_specs=[pl.BlockSpec((heads, tile, cols), lambda i: (0, i, 0))] + [keep(s) for s in shapes],
        out_shape=[jax.ShapeDtypeStruct((heads, rows, cols), bf16)] + [jax.ShapeDtypeStruct(s, f32) for s in shapes],
        scratch_shapes=[pltpu.VMEM((tile, ff), f32), pltpu.VMEM((tile, ff), bf16)] + extra,
        compiler_params=pltpu.CompilerParams(vmem_limit_bytes=67043328),
        cost_estimate=pl.CostEstimate(flops=rows * 5 * 10**7, bytes_accessed=3 * 10**7, transcendentals=0),
        name="dense",
    )(total, attn, feat, side, vec, enc, *weights, *olds)
MESH = pl.DeviceIdType.MESH


def front_kernel(nodes, heads, feat, enc, qkv, vec, out_f, out_e, out_q, out_v, up_s, up_r, down_s, down_r, halo_s, halo_r, w_s, w_r, l_sem):
    node, head = lax.axis_index("nodes"), lax.axis_index("heads")
    after, before = lax.rem(node + 1, nodes), lax.rem(node + nodes - 1, nodes)
    barrier = pltpu.get_barrier_semaphore()
    for other in (after, before):
        pl.semaphore_signal(barrier, inc=1, device_id=(other, head), device_id_type=MESH)
    for s in range(1, heads):
        pl.semaphore_signal(barrier, inc=1, device_id=(node, lax.rem(head + s, heads)), device_id_type=MESH)
    pl.semaphore_wait(barrier, heads + 1)

    own = [pltpu.make_async_copy(feat, out_f.at[1, head], l_sem.at[0]),
           pltpu.make_async_copy(enc, out_e.at[head], l_sem.at[1]),
           pltpu.make_async_copy(qkv.at[head], out_q.at[head], l_sem.at[2]),
           pltpu.make_async_copy(vec, out_v.at[head], l_sem.at[3])]

    def relay(step, upward):
        shard = head - step if upward else head + step
        shard = jnp.clip(shard, 0, heads - 1)
        target = jnp.clip(head + 1 if upward else head - 1, 0, heads - 1)
        sems = (up_s, up_r) if upward else (down_s, down_r)
        src = feat if step == 0 else out_f.at[1, shard]
        return pltpu.make_async_remote_copy(
            src_ref=src, dst_ref=out_f.at[1, shard], send_sem=sems[0].at[step], recv_sem=sems[1].at[step],
            device_id=(node, target), device_id_type=MESH)

    def halo(shard, src, way):
        return pltpu.make_async_remote_copy(
            src_ref=src, dst_ref=out_f.at[0 if way == 0 else 2, shard], send_sem=halo_s.at[way, shard], recv_sem=halo_r.at[way, shard],
            device_id=(after if way == 0 else before, head), device_id_type=MESH)

    def sends(step, upward):
        return (head - step >= 0) & (head + 1 <= heads - 1) if upward else (head + step <= heads - 1) & (head - 1 >= 0)

    def gets(step, upward):
        return head - 1 - step >= 0 if upward else head + 1 + step <= heads - 1

    for step in range(heads - 1):
        for upward in (True, False):
            @pl.when(sends(step, upward))
            def _(step=step, upward=upward):
                relay(step, upward).start()
        if step == 0:
            for way in range(2):
                halo(head, feat, way).start()
            for copy in own:
                copy.start()
        if step == heads - 2:
            weights = []
            for s in range(1, heads):
                there = lax.rem(head + s, heads)
                for i, (src, dst) in enumerate(((enc, out_e.at[head]), (qkv.at[there], out_q.at[head]), (vec, out_v.at[head]))):
                    slot = (s - 1) * 3 + i
                    weights.append(pltpu.make_async_remote_copy(
                        src_ref=src, dst_ref=dst, send_sem=w_s.at[slot], recv_sem=w_r.at[slot], device_id=(node, there), device_id_type=MESH))
                    weights[-1].start()
        for upward in (True, False):
            @pl.when(gets(step, upward))
            def _(step=step, upward=upward):
                relay(step, upward).wait_recv()
                shard = head - 1 - step if upward else head + 1 + step
                for way in range(2):
                    halo(shard, out_f.at[1, shard], way).start()
    for step in range(heads - 1):
        for upward in (True, False):
            @pl.when(sends(step, upward))
            def _(step=step, upward=upward):
                relay(step, upward).wait_send()
    for copy in own + weights:
        copy.wait()
    for shard in range(heads):
        for way in range(2):
            halo(shard, feat, way).wait()


def front(feat, enc, qkv, vec, nodes, heads):
    dma = pltpu.SemaphoreType.DMA
    vmem, anywhere = pl.BlockSpec(memory_space=pltpu.VMEM), pl.BlockSpec(memory_space=pl.ANY)
    n = 3 * (heads - 1)
    return pl.pallas_call(
        functools.partial(front_kernel, nodes, heads),
        in_specs=[vmem] * 4, out_specs=[anywhere] + [vmem] * 3,
        out_shape=[jax.ShapeDtypeStruct((3, heads, *feat.shape), feat.dtype), jax.ShapeDtypeStruct((heads, *enc.shape), enc.dtype),
                   jax.ShapeDtypeStruct(qkv.shape, qkv.dtype), jax.ShapeDtypeStruct((heads, *vec.shape), vec.dtype)],
        scratch_shapes=[dma((heads - 1,))] * 4 + [dma((2, heads))] * 2 + [dma((n,))] * 2 + [dma((4,))],
        compiler_params=pltpu.CompilerParams(collective_id=2, has_side_effects=True, vmem_limit_bytes=67043328),
        name="front",
    )(feat, enc, qkv, vec)


def pair_kernel(nodes, heads, down, up, out, slab, got_d, got_u, got_o, own_d, own_u, own_o, s_sem, r_sem, l_sem):
    node, head = lax.axis_index("nodes"), lax.axis_index("heads")
    chips = nodes // 2
    chip, side = lax.div(node, 2), lax.rem(node, 2)
    twin = chip * 2 + 1 - side
    barrier = pltpu.get_barrier_semaphore()
    pl.semaphore_signal(barrier, inc=1, device_id=(twin, head), device_id_type=MESH)
    pl.semaphore_wait(barrier, 1)
    moves = []
    for i, (src, got, own) in enumerate(((down, got_d, own_d), (up, got_u, own_u), (out, got_o, own_o))):
        local = pltpu.make_async_copy(src.at[:, :, side], own, l_sem.at[i])
        remote = pltpu.make_async_remote_copy(
            src_ref=src.at[:, :, 1 - side], dst_ref=got, send_sem=s_sem.at[i], recv_sem=r_sem.at[i], device_id=(twin, head), device_id_type=MESH)
        local.start()
        remote.start()
        moves.append((local, remote))
    width = out.shape[-1]
    at = 0
    for (local, remote), got, own in zip(moves, (got_d, got_u, got_o), (own_d, own_u, own_o)):
        local.wait()
        remote.wait()
        rows = own.shape[2]
        for c in range(0, own.shape[3], width):
            for s in range(chips):
                there = lax.rem(chip + s, chips)
                slab[s, :, at:at + rows, :] = own[:, there, :, c:c + width] + got[:, there, :, c:c + width]
            at += rows


def pair(down, up, out, nodes, heads):
    chips = nodes // 2
    split = lambda a: a.reshape(heads, chips, 2, -1, a.shape[-1])
    down, up, out = split(down), split(up), split(out)
    width = out.shape[-1]
    rows = sum(a.shape[3] * a.shape[4] // width for a in (down, up, out))
    half = [pltpu.VMEM((heads, chips, *a.shape[3:]), f32) for a in (down, up, out)]
    dma = pltpu.SemaphoreType.DMA
    return pl.pallas_call(
        functools.partial(pair_kernel, nodes, heads),
        in_specs=[pl.BlockSpec(memory_space=pl.ANY)] * 3, out_specs=pl.BlockSpec(memory_space=pltpu.VMEM),
        out_shape=jax.ShapeDtypeStruct((chips, heads, rows, width), f32),
        scratch_shapes=half + half + [dma((3,))] * 3,
        compiler_params=pltpu.CompilerParams(collective_id=3, has_side_effects=True, vmem_limit_bytes=67043328),
        cost_estimate=pl.CostEstimate(flops=10**10, bytes_accessed=2 * 10**7, transcendentals=0),
        name="pair",
    )(down, up, out)


def send(src, dst, sems, slot, node, head):
    copy = pltpu.make_async_remote_copy(
        src_ref=src, dst_ref=dst, send_sem=sems[0].at[slot], recv_sem=sems[1].at[slot], device_id=(node, head), device_id_type=MESH)
    copy.start()
    return copy


def greet(nodes, heads, node, head):
    barrier = pltpu.get_barrier_semaphore()
    for s in range(1, nodes):
        pl.semaphore_signal(barrier, inc=1, device_id=(lax.rem(node + s, nodes), head), device_id_type=MESH)
    for s in range(1, heads):
        pl.semaphore_signal(barrier, inc=1, device_id=(node, lax.rem(head + s, heads)), device_id_type=MESH)
    pl.semaphore_wait(barrier, nodes + heads - 2)


def finish_kernel(nodes, heads, *refs):
    (qkv, enc, vec, *bulk), refs = refs[:4], refs[4:]
    (out_q, out_e, out_v, *out_b), refs = refs[:4], refs[4:]
    (q_half, q_one, q_two, q_part, q_sum, q_own, e_half, e_one, e_two, e_sum, e_three, e_own, v_half, v_two, v_three, v_one, v_sum), refs = refs[:17], refs[17:]
    s_one, r_one, s_two, r_two, s_three, r_three, s_four, r_four, s_bulk, r_bulk, s_pass, r_pass, l_sem = refs
    node, head = lax.axis_index("nodes"), lax.axis_index("heads")
    chips = nodes // 2
    chip, side = lax.div(node, 2), lax.rem(node, 2)
    twin = chip * 2 + 1 - side
    greet(nodes, heads, node, head)
    first = [send(ref.at[:, :, 1 - side], dst, (s_one, r_one), i, twin, head) for i, (ref, dst) in enumerate(((qkv, q_half), (enc, e_half)))]
    first.append(send(vec, v_half, (s_one, r_one), 2, twin, head))
    keep = [pltpu.make_async_copy(src, dst.at[node], l_sem.at[i]) for i, (src, dst) in enumerate(zip(bulk, out_b))]
    for copy in keep:
        copy.start()
    for copy in first:
        copy.wait()
    q_one[...] = qkv[:, :, side] + q_half[...]
    e_one[...] = enc[:, :, side] + e_half[...]
    v_one[...] = vec[...] + v_half[...]
    second = []
    for s in range(1, chips):
        there = lax.rem(chip + s, chips)
        target = there * 2 + side
        i = (s - 1) * 3
        second.append(send(q_one.at[:, there], q_two.at[s - 1], (s_two, r_two), i, target, head))
        second.append(send(e_one.at[:, there], e_two.at[s - 1], (s_two, r_two), i + 1, target, head))
        second.append(send(v_one, v_two.at[s - 1], (s_two, r_two), i + 2, target, head))
    spread = []
    for s in range(chips):
        other = lax.rem(chip + s, chips) * 2 + side if s else twin
        spread.append([send(src, dst.at[node], (s_bulk, r_bulk), s + i, other, head) for i, (src, dst) in enumerate(zip(bulk, out_b))])
    for copy in second:
        copy.wait()
    q_part[...] = functools.reduce(jnp.add, [q_two[s] for s in range(chips - 1)], q_one[:, chip])
    e_sum[...] = functools.reduce(jnp.add, [e_two[s] for s in range(chips - 1)], e_one[:, chip])
    v_sum[...] = functools.reduce(jnp.add, [v_two[s] for s in range(chips - 1)], v_one[...])
    third = []
    for s in range(1, heads):
        there = lax.rem(head + s, heads)
        i = (s - 1) * 3
        third.append(send(q_part.at[there], q_sum.at[head], (s_three, r_three), i, node, there))
        third.append(send(e_sum.at[there], e_three.at[s - 1], (s_three, r_three), i + 1, node, there))
        third.append(send(v_sum, v_three.at[s - 1], (s_three, r_three), i + 2, node, there))
    for copy in third:
        copy.wait()
    q_sum[pl.ds(head, 1)] = q_part[pl.ds(head, 1)]
    e_own[...] = functools.reduce(jnp.add, [e_three[s] for s in range(heads - 1)], e_sum[head])
    out_v[...] = functools.reduce(jnp.add, [v_three[s] for s in range(heads - 1)], v_sum[...])
    fourth = []
    for s in range(1, nodes):
        there = lax.rem(node + s, nodes)
        fourth.append(send(q_sum, out_q.at[node], (s_four, r_four), (s - 1) * 2, there, head))
        fourth.append(send(e_own, out_e.at[node], (s_four, r_four), (s - 1) * 2 + 1, there, head))
    out_q[node] = q_sum[...]
    out_e[node] = e_own[...]
    for copy in keep:
        copy.wait()
    passed = []
    for s in range(chips):
        for copy in spread[s]:
            copy.wait()
        if s:
            origin = lax.rem(chip + chips - s, chips) * 2 + side
            passed += [send(dst.at[origin], dst.at[origin], (s_pass, r_pass), (s - 1) + i, twin, head) for i, dst in enumerate(out_b)]
    for copy in passed:
        copy.wait()
    for copy in fourth:
        copy.wait()


def finish(qkv, enc, vec, bulk, nodes, heads):
    chips = nodes // 2
    split = lambda a: a.reshape(heads, chips, 2, -1, a.shape[-1])
    qkv, enc = split(qkv), split(enc)
    vm = lambda *s: pltpu.VMEM(s, f32)
    rq, wq, re, we = *qkv.shape[3:], *enc.shape[3:]
    dma = pltpu.SemaphoreType.DMA
    wv = vec.shape
    scratch = [vm(heads, chips, rq, wq), vm(heads, chips, rq, wq), vm(chips - 1, heads, rq, wq), vm(heads, rq, wq), vm(heads, rq, wq), vm(8, 128),
               vm(heads, chips, re, we), vm(heads, chips, re, we), vm(chips - 1, heads, re, we), vm(heads, re, we), vm(heads - 1, re, we), vm(re, we),
               vm(*wv), vm(chips - 1, *wv), vm(heads - 1, *wv), vm(*wv), vm(*wv)]
    counts = (3, 3, 3 * chips - 3, 3 * chips - 3, 3 * heads - 3, 3 * heads - 3, 2 * nodes - 2, 2 * nodes - 2, chips, chips, chips - 1, chips - 1, 1)
    out_shape = [jax.ShapeDtypeStruct(s, f32) for s in [(nodes, heads, rq, wq), (nodes, re, we), wv] + [(nodes, *b.shape) for b in bulk]]
    spec = pl.BlockSpec(memory_space=pltpu.VMEM)
    return pl.pallas_call(
        functools.partial(finish_kernel, nodes, heads),
        in_specs=[spec] * 4, out_specs=[spec] * 4, out_shape=out_shape,
        scratch_shapes=scratch + [dma((n,)) for n in counts],
        compiler_params=pltpu.CompilerParams(collective_id=1, has_side_effects=True, vmem_limit_bytes=48 << 20),
        name="finish",
    )(qkv, enc, vec, *bulk)
D = 512
HEADS = 8
NBR = 8
ADAM_STEP = 3
highest = lax.Precision.HIGHEST
beta_one = 0.5
beta_two = 0.5
learn_rate = 0.02
weight_decay = 0.1
adam_eps = 1e-08


def adamw(weight, first_moment, second, gradient):
    first_new = beta_one * first_moment + (1.0 - beta_one) * gradient
    second_new = beta_two * second + (1.0 - beta_two) * gradient * gradient
    first_hat = first_new / (1.0 - beta_one**ADAM_STEP)
    second_hat = second_new / (1.0 - beta_two**ADAM_STEP)
    weight_new = weight - learn_rate * (
        first_hat / (jnp.sqrt(second_hat) + adam_eps) + weight_decay * weight
    )
    return (weight_new, first_new, second_new)


def local(
    features, target, counts, neighbours, edge_kinds,
    enc_weight, enc_first, enc_second, qkv_weight, qkv_first, qkv_second,
    out_weight, out_first, out_second, up_weight, up_first, up_second,
    down_weight, down_first, down_second, vec_weight, vec_first, vec_second,
):
    heads_count = lax.axis_size("heads")
    nodes_count = lax.axis_size("nodes")
    head_index = lax.axis_index("heads")
    node_index = lax.axis_index("nodes")
    row_count = features.shape[0]
    own_blocks = row_count // BLOCK
    group_blocks = own_blocks * heads_count
    group_rows = group_blocks * BLOCK
    hl = HEADS // heads_count
    hs = D // HEADS
    cols = hl * hs
    cp = -(-cols // 128) * 128
    ka = -(-(cols + 1) // 128) * 128
    kinds = D // HEADS
    slots = NBR + 1
    low = lambda a: a.astype(bf16)
    gather = lambda a, axis: lax.all_gather(low(a), "heads", axis=axis, tiled=True)

    qkv_parts = jnp.transpose(low(qkv_weight).reshape(-1, heads_count, hl, 3, hs), (1, 0, 3, 2, 4)).reshape(heads_count, -1, 3, cols)
    qkv_parts = jnp.pad(qkv_parts, ((0, 0), (0, 0), (0, 0), (0, cp - cols))).reshape(heads_count, -1, 3 * cp)
    vec_part = jnp.pad(low(vec_weight).astype(f32), ((0, 2), (0, 0)))
    feats, enc_b, qkv_cols, vectors = front(features, low(enc_weight), qkv_parts, vec_part, nodes_count, heads_count)
    feats = feats.reshape(3 * group_rows, -1)
    enc_b = enc_b.reshape(-1, D)
    qkv_cols = qkv_cols.reshape(D, 3 * cp)
    vectors = jnp.transpose(vectors, (1, 0, 2)).reshape(8, D)
    up_low, out_low, down_low, enc_b = lax.optimization_barrier((low(up_weight), low(out_weight), low(down_weight), enc_b))
    ff = up_weight.shape[1]
    pieces = heads_count * nodes_count
    rows_down, rows_out = ff // pieces, D // pieces
    mine = lambda a, rows: lax.dynamic_slice_in_dim(a, node_index * rows, rows, 0)
    up_mine = mine(up_low, rows_out)
    packed = jnp.concatenate([mine(down_low, rows_down)] + [up_mine[:, c:c + D] for c in range(0, ff, D)] + [mine(out_low, rows_out)], axis=0)
    packed = lax.all_gather(packed, ("heads", "nodes"), axis=0, tiled=False).reshape(heads_count, nodes_count, -1, D)

    enc_bias, gain_one, gain_two, gain_three, head_vec = (vectors[r] for r in range(5))
    edge_local = lax.dynamic_slice_in_dim(vectors[5].reshape(kinds, HEADS), head_index * hl, hl, 1)
    own_counts = lax.dynamic_slice_in_dim(counts, (node_index * heads_count + head_index) * own_blocks, own_blocks)
    row_live = (jnp.arange(BLOCK, dtype=jnp.int32)[None, :] < own_counts[:, None]).reshape(row_count).astype(f32)
    live_total = jnp.sum(counts).astype(f32)

    def group_counts(offset):
        return lax.dynamic_slice_in_dim(counts, (node_index + offset) % nodes_count * group_blocks, group_blocks)

    pool_counts = jnp.concatenate([group_counts(nodes_count - 1), group_counts(0), group_counts(1)])
    relative = (neighbours // group_blocks - node_index + 1) % nodes_count
    nbr_pos = relative * group_blocks + neighbours % group_blocks
    self_pos = group_blocks + jnp.arange(group_blocks, dtype=jnp.int32)
    key_pos = jnp.concatenate([self_pos[:, None], nbr_pos], axis=1).reshape(-1)
    kind_hot = jax.nn.one_hot(edge_kinds, kinds, dtype=f32)
    slot_bias = jnp.einsum("bst,th->bsh", kind_hot, edge_local, precision=highest)
    bias_rows = jnp.repeat(slot_bias, BLOCK, axis=2)

    kaug, kt, value, vt, query = encode(
        pool_counts, feats, enc_b, enc_bias[None], gain_one[None], qkv_cols, cp, ka, cols, hs**-0.5)
    side = jnp.stack([target, row_live], axis=1)
    dense_vec = jnp.stack([enc_bias, gain_two, gain_three, head_vec])
    half = lambda a: a.reshape(heads_count, 2, row_count // 2, -1)
    exchange = lambda a: lax.all_to_all(a, "heads", split_axis=0, concat_axis=0, tiled=True)
    attn_parts, lse_parts, grad_parts, totals = [], [], [], None
    for part in range(2):
        attn_part, lse_part = attend(part, own_blocks, key_pos, query, bias_rows, kaug, vt, hl, hs)
        attn_parts.append(attn_part)
        lse_parts.append(lse_part)
    packed, attn_parts[1] = lax.optimization_barrier((packed, attn_parts[1]))
    weights = (packed,)
    if rows_out % 16:
        up_rows = packed[:, :, rows_down:-rows_out].reshape(pieces, -1, rows_out, D)
        weights = (packed[:, :, -rows_out:].reshape(D, D), jnp.transpose(up_rows, (0, 2, 1, 3)).reshape(D, ff), packed[:, :, :rows_down].reshape(ff, D))
    for part in range(2):
        attn_rows = exchange(attn_parts[part].reshape(heads_count, row_count // 2, cp)[..., :cols])
        grad_part, *totals = dense(part, live_total[None], attn_rows, features, side, dense_vec, enc_b, weights, ff, totals)
        grad_parts.append(exchange(grad_part))
    grad_down, grad_up, grad_out, denc_own, dense_sums = totals
    grad_parts[0], grad_down = lax.optimization_barrier((grad_parts[0], grad_down))
    slab = pair(grad_down, grad_up, grad_out, nodes_count, heads_count)
    moved = [slab[0]] + [
        lax.ppermute(slab[s], "nodes", [(i, (i + 2 * s) % nodes_count) for i in range(nodes_count)]) for s in range(1, nodes_count // 2)]
    grad_heads = jnp.concatenate([g[:, None] for g in grad_parts], axis=1).reshape(group_rows, cols)
    grad_heads = jnp.pad(grad_heads, ((0, 0), (0, cp - cols)))
    dq, dkv, edge_sums = attend_back(own_blocks, key_pos, query, grad_heads, attn_parts, lse_parts, bias_rows, kaug, value, kt, hl, hs)
    moved, dkv = lax.optimization_barrier((moved, dkv))
    planes = exchange(functools.reduce(jnp.add, moved))
    slot_sums = jnp.sum(edge_sums.reshape(group_blocks, slots, hl, BLOCK), axis=3)
    edge_grad = jnp.einsum("bst,bsh->th", kind_hot, slot_sums, precision=highest)
    columns = lambda a: jnp.broadcast_to(a[:, None], (D, 128))
    dw, denc_t, dgain, dbias = encode_back(
        feats, dkv, dq, enc_b.T, columns(enc_bias), columns(gain_one), qkv_cols[:, :cp], qkv_cols[:, cp:])

    grad_gain_one = jnp.sum(dgain, axis=1)
    grad_enc_bias = jnp.sum(dbias, axis=1) + dense_sums[0]
    grad_enc = denc_t.T + denc_own
    edge_full = lax.dynamic_update_slice(jnp.zeros((kinds, HEADS), f32), edge_grad, (jnp.int32(0), head_index * hl))
    grad_vec = jnp.concatenate([grad_enc_bias[None], grad_gain_one[None], dense_sums[1:5], edge_full.reshape(1, D), jnp.zeros((1, D), f32)])
    planes, dw = lax.optimization_barrier((planes, dw))
    dw_sum, enc_sum, vec_total, bulk = finish(dw, grad_enc, grad_vec, [jnp.sum(planes, axis=0)], nodes_count, heads_count)
    total_loss = vec_total[5, 0]
    vec_sum = lax.dynamic_slice_in_dim(jnp.concatenate([vec_total[:5], vec_total[6:7]]), head_index * (D // heads_count), D // heads_count, 1)
    states = (enc_weight, enc_first, enc_second, qkv_weight, qkv_first, qkv_second, out_weight, out_first, out_second,
              up_weight, up_first, up_second, down_weight, down_first, down_second)
    vec_res = adamw(vec_weight, vec_first, vec_second, vec_sum)
    if rows_out % 16:
        qkv_sum = jnp.transpose(dw_sum, (0, 2, 1, 3)).reshape(-1, heads_count, 3, cp)[..., :cols].reshape(-1, heads_count, 3, hl, hs)
        qkv_sum = jnp.transpose(qkv_sum, (0, 1, 3, 2, 4)).reshape(qkv_weight.shape)
        flat = lambda a: a.reshape(-1, a.shape[-1])
        up_sum = bulk[:, rows_down:-rows_out].reshape(nodes_count, -1, rows_out, D)
        up_sum = jnp.transpose(up_sum, (0, 2, 1, 3)).reshape(up_weight.shape)
        summed = (flat(enc_sum), qkv_sum, flat(bulk[:, -rows_out:]), up_sum, flat(bulk[:, :rows_down]))
        results = []
        for n, grad in enumerate(summed):
            results += adamw(*states[3 * n:3 * n + 3], grad)
        results += [low(r) for r in results[::3]]
    else:
        results = adam(enc_sum, dw_sum, bulk, states, hl, hs, cp)
    loss_value = (total_loss / live_total).reshape(1)
    return (loss_value, *results[:15], *vec_res, *results[15:])


def solution(mesh):
    rows = P("heads", None)
    both = P(("nodes", "heads"))
    lanes = P(None, "heads")
    in_specs = (P(("nodes", "heads"), None), both, P(), P("nodes", None), P("nodes", None)) + (rows,) * 15 + (lanes,) * 3
    out_specs = (P(),) + (rows,) * 15 + (lanes,) * 3 + (rows,) * 5
    return jax.shard_map(local, mesh=mesh, in_specs=in_specs, out_specs=out_specs, check_vma=False)


def adam_kernel(hl, hs, cp, *refs):
    g_enc, g_qkv, g_bulk = refs[:3]
    ins, outs = refs[3:18], refs[18:]
    rows_down, rows_out = ins[12].shape[0], ins[6].shape[0]
    heads = g_qkv.shape[1]
    bulk = g_bulk[0]
    parts = []
    for h in range(heads):
        part = g_qkv[0, h]
        for k in range(hl):
            parts += [part[:, j * cp + k * hs:j * cp + (k + 1) * hs] for j in range(3)]
    up_at = lambda c: rows_down + c * rows_out
    grads = [g_enc[0], jnp.concatenate(parts, axis=1), bulk[-rows_out:],
             jnp.concatenate([bulk[up_at(c):up_at(c) + rows_out] for c in range(ins[9].shape[1] // bulk.shape[1])], axis=1), bulk[:rows_down]]
    for n, grad in enumerate(grads):
        new = adamw(*(ref[...] for ref in ins[3 * n:3 * n + 3]), grad)
        for ref, value in zip(outs[3 * n:3 * n + 3], new):
            ref[...] = value
        outs[15 + n][...] = new[0].astype(bf16)


def adam(g_enc, g_qkv, g_bulk, states, hl, hs, cp):
    nodes = g_enc.shape[0]
    rows = lambda a: pl.BlockSpec((a.shape[0] // nodes, a.shape[1]), lambda i: (i, 0))
    lead = lambda a: pl.BlockSpec((1, *a.shape[1:]), lambda i: (i,) + (0,) * (a.ndim - 1))
    shapes = [jax.ShapeDtypeStruct(a.shape, f32) for a in states] + [jax.ShapeDtypeStruct(a.shape, bf16) for a in states[::3]]
    return pl.pallas_call(
        functools.partial(adam_kernel, hl, hs, cp),
        grid=(nodes,),
        in_specs=[lead(g_enc), lead(g_qkv), lead(g_bulk)] + [rows(a) for a in states],
        out_specs=[rows(a) for a in shapes], out_shape=shapes,
        compiler_params=pltpu.CompilerParams(vmem_limit_bytes=67043328),
        name="adam",
    )(g_enc, g_qkv, g_bulk, *states)
```

```python
import functools

import jax
import jax.numpy as jnp
from jax import lax
from jax.experimental import pallas as pl
from jax.experimental.pallas import tpu as pltpu
from jax.sharding import PartitionSpec as P

BLOCK = 128
NT = (((1,), (1,)), ((), ()))
NN = (((1,), (0,)), ((), ()))
f32 = jnp.float32
bf16 = jnp.bfloat16


def dotf(a, b, dims):
    return lax.dot_general(a, b, dims, preferred_element_type=f32)


def head_rows(x, hl, hs, cp):
    if hl == 1:
        return x
    lane = lax.broadcasted_iota(jnp.int32, (BLOCK, cp), 1)
    zero = jnp.zeros_like(x)
    return jnp.concatenate([jnp.where(lane // hs == h, x, zero) for h in range(hl)], axis=0)


def ones_lane(hl, cp, ka):
    rows = hl * BLOCK
    lane = lax.broadcasted_iota(jnp.int32, (rows, ka - cp), 1)
    return jnp.where(lane == 0, 1.0, 0.0).astype(bf16)


def attend_kernel(hl, hs, cp, ka, slots, unit, unit_of, pos_ref, q_ref, brow_ref, kaug_ref, vt_ref, o_ref, lse_ref, *scratch):
    first = unit_of(pl.program_id(0)) * unit
    rows = hl * BLOCK

    def spot(u, s):
        return pos_ref[(first + u) * slots + s]

    def score(u):
        s_ref = scratch[2 * (u % 2)]
        q2 = head_rows(q_ref[u * BLOCK:(u + 1) * BLOCK, :], hl, hs, cp)
        qa = jnp.concatenate([q2, ones_lane(hl, cp, ka)], axis=1) if ka > cp else q2
        keys = [kaug_ref[pl.ds(pl.multiple_of(spot(u, s) * BLOCK, BLOCK), BLOCK), :] for s in range(slots)]
        scores = dotf(jnp.concatenate(keys, axis=0), qa, NT)
        top = None
        for s in range(slots):
            sc = scores[s * BLOCK:(s + 1) * BLOCK]
            s_ref[s] = sc
            t = jnp.max(sc, axis=0, keepdims=True) + brow_ref[u, s:s + 1, :]
            top = t if top is None else jnp.maximum(top, t)
        return top

    def weigh(u, top):
        s_ref, p_ref = scratch[2 * (u % 2):2 * (u % 2) + 2]
        tot = jnp.zeros((1, rows), f32)
        for s in range(slots):
            e = jnp.exp(s_ref[s] - (top - brow_ref[u, s:s + 1, :]))
            s_ref[s] = e
            tot = tot + jnp.sum(e, axis=0, keepdims=True)
        lse_ref[u] = top + jnp.log(tot)
        inv = 1.0 / tot
        for s in range(slots):
            p_ref[s * BLOCK:(s + 1) * BLOCK, :] = (s_ref[s] * inv).astype(bf16)

    def total(u):
        p_ref = scratch[2 * (u % 2) + 1]
        ot = dotf(jnp.concatenate([vt_ref[spot(u, s)] for s in range(slots)], axis=1), p_ref[...], NN)
        parts = [ot[h * hs:(h + 1) * hs, h * BLOCK:(h + 1) * BLOCK] for h in range(hl)]
        if hl * hs < cp:
            parts.append(jnp.zeros((cp - hl * hs, BLOCK), f32))
        o_ref[u * BLOCK:(u + 1) * BLOCK, :] = jnp.concatenate(parts, axis=0).T.astype(bf16)

    top = score(0)
    for u in range(unit):
        following = score(u + 1) if u + 1 < unit else None
        weigh(u, top)
        total(u)
        top = following


def attend(part, own, pos, q, brow, kaug, vt, hl, hs, unit=4):
    cp, ka = q.shape[1], kaug.shape[1]
    nb = q.shape[0] // BLOCK // 2
    half, own = own // 2 // unit, own // unit
    unit_of = lambda i: lax.div(i, half) * own + part * half + lax.rem(i, half)
    slots = brow.shape[1]
    rows = hl * BLOCK
    whole = lambda a: pl.BlockSpec(a.shape, lambda i, *_: (0,) * a.ndim, pipeline_mode=pl.Buffered(1))
    return pl.pallas_call(
        functools.partial(attend_kernel, hl, hs, cp, ka, slots, unit, unit_of),
        grid_spec=pltpu.PrefetchScalarGridSpec(
            num_scalar_prefetch=1, grid=(nb // unit,),
            in_specs=[pl.BlockSpec((unit * BLOCK, cp), lambda i, *_: (unit_of(i), 0)),
                      pl.BlockSpec((unit, slots, rows), lambda i, *_: (unit_of(i), 0, 0)),
                      whole(kaug), whole(vt)],
            out_specs=[pl.BlockSpec((unit * BLOCK, cp), lambda i, *_: (i, 0)),
                       pl.BlockSpec((unit, 1, rows), lambda i, *_: (i, 0, 0))],
            scratch_shapes=[pltpu.VMEM((slots, BLOCK, rows), f32), pltpu.VMEM((slots * BLOCK, rows), bf16)] * 2),
        out_shape=[jax.ShapeDtypeStruct((nb * BLOCK, cp), bf16), jax.ShapeDtypeStruct((nb, 1, rows), f32)],
        cost_estimate=pl.CostEstimate(flops=nb * 10**9, bytes_accessed=3 * 10**7, transcendentals=0),
        compiler_params=pltpu.CompilerParams(vmem_limit_bytes=67043328),
        name="attend",
    )(pos, q, brow, kaug, vt)


def attend_back_kernel(hl, hs, cp, ka, slots, scale, unit, unit_of, pos_ref, q_ref, da_ref, db_ref, oa_ref, ob_ref, la_ref, lb_ref, brow_ref, kaug_ref, v_ref,
                       kt_ref, dq_ref, dkv_ref, edge_ref, *scratch):
    i = pl.program_id(0)
    first = unit_of(i) * unit
    late = i >= pl.num_programs(0) // 2

    @pl.when(i == 0)
    def _():
        @pl.loop(0, dkv_ref.shape[0] // BLOCK)
        def _(n):
            dkv_ref[pl.ds(pl.multiple_of(n * BLOCK, BLOCK), BLOCK), :] = jnp.zeros((BLOCK, dkv_ref.shape[1]), f32)

    for u in range(unit):
        p_ref, d_ref = scratch[2 * (u % 2):2 * (u % 2) + 2]
        own = slice(u * BLOCK, (u + 1) * BLOCK)
        q2 = head_rows(q_ref[own, :], hl, hs, cp)
        qa = jnp.concatenate([q2, ones_lane(hl, cp, ka)], axis=1) if ka > cp else q2
        do = jnp.where(late, db_ref[own, :], da_ref[own, :])
        do2 = head_rows(do, hl, hs, cp)
        prod = (do.astype(f32) * jnp.where(late, ob_ref[own, :], oa_ref[own, :]).astype(f32)).T
        dd = jnp.concatenate([jnp.sum(prod[h * hs:(h + 1) * hs], axis=0, keepdims=True) for h in range(hl)], axis=1)
        lse = jnp.where(late, lb_ref[u], la_ref[u])
        blocks = [pos_ref[(first + u) * slots + s] for s in range(slots)]
        spots = [pl.ds(pl.multiple_of(p * BLOCK, BLOCK), BLOCK) for p in blocks]
        scores = dotf(jnp.concatenate([kaug_ref[at, :] for at in spots], axis=0), qa, NT)
        grads = dotf(jnp.concatenate([v_ref[at, :] for at in spots], axis=0), do2, NT)
        for s in range(slots):
            here = slice(s * BLOCK, (s + 1) * BLOCK)
            pr = jnp.exp(scores[here] - (lse - brow_ref[u, s:s + 1, :]))
            ds = pr * (grads[here] - dd)
            edge_ref[u, s:s + 1, :] = jnp.sum(ds, axis=0, keepdims=True)
            p_ref[here, :] = pr.astype(bf16)
            d_ref[here, :] = ds.astype(bf16)
        dv = dotf(p_ref[...], do2, NN)
        dk = dotf(d_ref[...], q2, NN)
        dqt = dotf(jnp.concatenate([kt_ref[p] for p in blocks], axis=1), d_ref[...], NN)
        for s, at in enumerate(spots):
            here = slice(s * BLOCK, (s + 1) * BLOCK)
            dkv_ref[at, 0:cp] += dk[here]
            dkv_ref[at, cp:2 * cp] += dv[here]
        parts = [dqt[h * hs:(h + 1) * hs, h * BLOCK:(h + 1) * BLOCK] for h in range(hl)]
        if hl * hs < cp:
            parts.append(jnp.zeros((cp - hl * hs, BLOCK), f32))
        dq_ref[own, :] = (jnp.concatenate(parts, axis=0).T * scale).astype(bf16)


def attend_back(own, pos, q, dos, outs, lses, brow, kaug, v, kt, hl, hs, unit=4):
    cp, ka = q.shape[1], kaug.shape[1]
    nb = q.shape[0] // BLOCK
    slots = brow.shape[1]
    rows = hl * BLOCK
    half, mid, own = own // 2 // unit, nb // 2 // unit, own // unit
    unit_of = lambda i: lax.div(lax.rem(i, mid), half) * own + lax.div(i, mid) * half + lax.rem(i, half)
    whole = lambda a: pl.BlockSpec(a.shape, lambda i, *_: (0,) * a.ndim, pipeline_mode=pl.Buffered(1))
    tile = pl.BlockSpec((unit * BLOCK, cp), lambda i, *_: (unit_of(i), 0))
    early = lambda i: jnp.minimum(i, mid - 1)
    late = lambda i: jnp.maximum(i - mid, 0)
    return pl.pallas_call(
        functools.partial(attend_back_kernel, hl, hs, cp, ka, slots, hs ** -0.5, unit, unit_of),
        grid_spec=pltpu.PrefetchScalarGridSpec(
            num_scalar_prefetch=1, grid=(nb // unit,),
            in_specs=[tile] + [pl.BlockSpec((unit * BLOCK, cp), lambda i, *_: (early(i), 0)), pl.BlockSpec((unit * BLOCK, cp), lambda i, *_: (late(i), 0))] * 2 + [
                      pl.BlockSpec((unit, 1, rows), lambda i, *_: (early(i), 0, 0)), pl.BlockSpec((unit, 1, rows), lambda i, *_: (late(i), 0, 0)),
                      pl.BlockSpec((unit, slots, rows), lambda i, *_: (unit_of(i), 0, 0)),
                      whole(kaug), whole(v), whole(kt)],
            out_specs=[tile, pl.BlockSpec((v.shape[0], 2 * cp), lambda i, *_: (0, 0), pipeline_mode=pl.Buffered(1)),
                       pl.BlockSpec((unit, slots, rows), lambda i, *_: (unit_of(i), 0, 0))],
            scratch_shapes=[pltpu.VMEM((slots * BLOCK, rows), bf16)] * 4),
        out_shape=[jax.ShapeDtypeStruct(q.shape, bf16), jax.ShapeDtypeStruct((v.shape[0], 2 * cp), f32),
                   jax.ShapeDtypeStruct((nb, slots, rows), f32)],
        cost_estimate=pl.CostEstimate(flops=nb * 2 * 10**9, bytes_accessed=6 * 10**7, transcendentals=0),
        compiler_params=pltpu.CompilerParams(vmem_limit_bytes=67043328),
        name="attend_back",
    )(pos, q, *dos, *outs, *lses, brow, kaug, v, kt)
norm_eps = 1e-05


def encode_kernel(cp, ka, cols, scale, per_group, inner, cnt_ref, x_all, enc_ref, bias_ref, gain_ref, w_ref,
                  kaug_all, kt_all, v_all, vt_all, q_all):
    @pl.loop(0, x_all.shape[0] // inner)
    def _(n):
        rows = pl.ds(pl.multiple_of(n * inner, inner), inner)
        blocks = pl.ds(n * (inner // BLOCK), inner // BLOCK)
        encode_rows(cp, ka, cols, scale, per_group, pl.program_id(0), n, x_all.shape[0] // inner, cnt_ref, x_all.at[rows], enc_ref, bias_ref, gain_ref,
                    w_ref, kaug_all.at[rows], kt_all.at[blocks], v_all.at[rows], vt_all.at[blocks], q_all.at[rows])


def encode_rows(cp, ka, cols, scale, per_group, i, n, count, cnt_ref, x_ref, enc_ref, bias_ref, gain_ref, w_ref,
                kaug_ref, kt_ref, v_ref, vt_ref, q_ref):
    group = i // per_group
    tile = x_ref.shape[0]
    resid = dotf(x_ref[...], enc_ref[...], NN) + bias_ref[...]
    centred = resid - jnp.mean(resid, axis=-1, keepdims=True)
    variance = jnp.mean(centred * centred, axis=-1, keepdims=True)
    act = (centred * lax.rsqrt(variance + norm_eps) * gain_ref[...]).astype(bf16)
    kv = dotf(act, w_ref[:, cp:], NN).astype(bf16)
    key, value = kv[:, :cp], kv[:, cp:]
    row = lax.broadcasted_iota(jnp.int32, (BLOCK, 128), 0)
    lane = lax.broadcasted_iota(jnp.int32, (BLOCK, 128), 1)
    first = (i * count + n) * (tile // BLOCK)
    dead = jnp.concatenate(
        [jnp.where((row >= cnt_ref[first + j]) & (lane == cols % 128), -1e30, 0.0) for j in range(tile // BLOCK)], axis=0).astype(bf16)
    if ka > cp:
        kaug_ref[:, :cp] = key
        kaug_ref[:, cp:] = dead
    else:
        kaug_ref[...] = key + dead
    v_ref[...] = value
    for j in range(tile // BLOCK):
        kt_ref[j] = key[j * BLOCK:(j + 1) * BLOCK].T
        vt_ref[j] = value[j * BLOCK:(j + 1) * BLOCK].T

    @pl.when(group == 1)
    def _():
        q = (dotf(act, w_ref[:, :cp], NN) * scale).astype(bf16)
        if ka == cp:
            lanes = lax.broadcasted_iota(jnp.int32, q.shape, 1)
            q = jnp.where(lanes == cols, jnp.ones_like(q), q)
        q_ref[...] = q


def encode(counts, feats, enc, bias, gain, w, cp, ka, cols, scale, tile=2048):
    rows, feat = feats.shape[0] // 3, feats.shape[1]
    width = enc.shape[1]
    per = rows // tile
    blocks = tile // BLOCK
    whole = lambda a: pl.BlockSpec(a.shape, lambda i, *_: (0,) * a.ndim, pipeline_mode=pl.Buffered(1))
    return pl.pallas_call(
        functools.partial(encode_kernel, cp, ka, cols, scale, per, 1024),
        grid_spec=pltpu.PrefetchScalarGridSpec(
            num_scalar_prefetch=1, grid=(3 * per,),
            in_specs=[pl.BlockSpec((tile, feat), lambda i, *_: (i, 0)), whole(enc), whole(bias), whole(gain), whole(w)],
            out_specs=[pl.BlockSpec((tile, ka), lambda i, *_: (i, 0)),
                       pl.BlockSpec((blocks, cp, BLOCK), lambda i, *_: (i, 0, 0)),
                       pl.BlockSpec((tile, cp), lambda i, *_: (i, 0)),
                       pl.BlockSpec((blocks, cp, BLOCK), lambda i, *_: (i, 0, 0)),
                       pl.BlockSpec((tile, cp), lambda i, *_: (jnp.clip(i - per, 0, per - 1), 0))]),
        out_shape=[jax.ShapeDtypeStruct((3 * rows, ka), bf16),
                   jax.ShapeDtypeStruct((3 * rows // BLOCK, cp, BLOCK), bf16),
                   jax.ShapeDtypeStruct((3 * rows, cp), bf16),
                   jax.ShapeDtypeStruct((3 * rows // BLOCK, cp, BLOCK), bf16),
                   jax.ShapeDtypeStruct((rows, cp), bf16)],
        compiler_params=pltpu.CompilerParams(vmem_limit_bytes=67043328),
        cost_estimate=pl.CostEstimate(flops=rows * 6 * 10**6, bytes_accessed=3 * 10**7, transcendentals=0),
        name="encode",
    )(counts, feats, enc, bias, gain, w)


def encode_back_kernel(cp, per_group, inner, x_all, dkv_all, dq_all, enct_ref, bias_ref, gain_ref, wq_ref, wkv_ref,
                       dw_ref, denc_ref, dgain_ref, dbias_ref, g_ref):
    i = pl.program_id(0)

    @pl.when(i == 0)
    def _():
        for ref in (dw_ref, denc_ref, dgain_ref, dbias_ref):
            ref[...] = jnp.zeros_like(ref)

    @pl.loop(0, x_all.shape[0] // inner)
    def _(n):
        rows = pl.ds(pl.multiple_of(n * inner, inner), inner)
        encode_back_rows(cp, i // per_group, x_all.at[rows], dkv_all.at[rows], dq_all.at[rows], enct_ref, bias_ref, gain_ref, wq_ref, wkv_ref,
                         dw_ref, denc_ref, dgain_ref, dbias_ref, g_ref)


def encode_back_rows(cp, group, x_ref, dkv_ref, dq_ref, enct_ref, bias_ref, gain_ref, wq_ref, wkv_ref,
                     dw_ref, denc_ref, dgain_ref, dbias_ref, g_ref):
    tile = x_ref.shape[0]
    width = enct_ref.shape[0]
    reps = tile // 128

    x = x_ref[...]
    wide = lambda c: jnp.concatenate([c] * reps, axis=1)
    fold = lambda a: functools.reduce(jnp.add, [a[:, r * 128:(r + 1) * 128] for r in range(reps)])
    resid = dotf(enct_ref[...], x, NT) + wide(bias_ref[...])
    centred = resid - jnp.sum(resid, axis=0, keepdims=True) * (1.0 / width)
    variance = jnp.sum(centred * centred, axis=0, keepdims=True) * (1.0 / width)
    inv = lax.rsqrt(variance + norm_eps)
    norm = centred * inv
    gain = wide(gain_ref[...])
    act = (norm * gain).astype(bf16)
    dkv = dkv_ref[...].astype(bf16)
    g_ref[...] = dotf(wkv_ref[...], dkv, NT)
    dw_ref[:, cp:] += dotf(act, dkv, NN)

    @pl.when(group == 1)
    def _():
        dq = dq_ref[...]
        g_ref[...] += dotf(wq_ref[...], dq, NT)
        dw_ref[:, :cp] += dotf(act, dq, NN)

    grad = g_ref[...]
    dgain_ref[...] += fold(grad * norm)
    back = grad * gain
    mean_one = jnp.sum(back, axis=0, keepdims=True) * (1.0 / width)
    mean_two = jnp.sum(back * norm, axis=0, keepdims=True) * (1.0 / width)
    din = inv * (back - mean_one - norm * mean_two)
    dbias_ref[...] += fold(din)
    denc_ref[...] += dotf(din.astype(bf16), x, NN)


def encode_back(feats, dkv, dq, enct, bias, gain, wq, wkv, tile=2048, inner=1024):
    rows, feat = feats.shape[0] // 3, feats.shape[1]
    width = enct.shape[0]
    cp = dq.shape[1]
    per = rows // tile
    whole = lambda a: pl.BlockSpec(a.shape, lambda i: (0,) * a.ndim, pipeline_mode=pl.Buffered(1))
    keep = lambda s: pl.BlockSpec(s, lambda i: (0,) * len(s), pipeline_mode=pl.Buffered(1))
    shapes = [(width, 3 * cp), (width, feat), (width, 128), (width, 128)]
    return pl.pallas_call(
        functools.partial(encode_back_kernel, cp, per, inner),
        grid=(3 * per,),
        in_specs=[pl.BlockSpec((tile, feat), lambda i: (i, 0)), pl.BlockSpec((tile, 2 * cp), lambda i: (i, 0)),
                  pl.BlockSpec((tile, cp), lambda i: (jnp.clip(i - per, 0, per - 1), 0)),
                  whole(enct), whole(bias), whole(gain), whole(wq), whole(wkv)],
        out_specs=[keep(s) for s in shapes],
        out_shape=[jax.ShapeDtypeStruct(s, f32) for s in shapes],
        scratch_shapes=[pltpu.VMEM((width, inner), f32)],
        compiler_params=pltpu.CompilerParams(vmem_limit_bytes=67043328),
        cost_estimate=pl.CostEstimate(flops=rows * 10**7, bytes_accessed=4 * 10**7, transcendentals=0),
        name="encode_back",
    )(feats, dkv, dq, enct, bias, gain, wq, wkv)


def row_norm(values):
    centred = values - jnp.mean(values, axis=-1, keepdims=True)
    inv = lax.rsqrt(jnp.mean(centred * centred, axis=-1, keepdims=True) + norm_eps)
    return centred * inv, inv


def norm_back(grad, norm, inv):
    return inv * (grad - jnp.mean(grad, axis=-1, keepdims=True) - norm * jnp.mean(grad * norm, axis=-1, keepdims=True))


def packed_dense_kernel(split, first, chunk, *refs):
    rows_down, rows_out = split
    packed, out_ref, up_ref, down_ref = refs[6], *refs[-3:]
    width = packed.shape[-1]

    @pl.when(pl.program_id(0) == 0)
    def _():
        for h in range(packed.shape[0]):
            for j in range(packed.shape[1]):
                k = h * packed.shape[1] + j
                down_ref[k * rows_down:(k + 1) * rows_down, :] = packed[h, j, :rows_down]
                for c in range(up_ref.shape[1] // width):
                    at = rows_down + c * rows_out
                    up_ref[k * rows_out:(k + 1) * rows_out, c * width:(c + 1) * width] = packed[h, j, at:at + rows_out]
                out_ref[k * rows_out:(k + 1) * rows_out, :] = packed[h, j, packed.shape[2] - rows_out:]

    dense_kernel(first, chunk, *refs[:6], out_ref, up_ref, down_ref, *refs[7:-3])


def dense_kernel(first, chunk, total_ref, attn_ref, feat_ref, side_ref, vec_ref, enc_ref, *refs):
    out_ref, up_ref, down_ref = refs[:3]
    refs = refs[3:]
    if not first:
        olds, refs = refs[:5], refs[5:]
    gattn_ref, ddown_ref, dup_ref, dout_ref, denc_ref, dvec_ref, u_ref, g_ref = refs
    i = pl.program_id(0)

    @pl.when(i == 0)
    def _():
        for n, ref in enumerate((ddown_ref, dup_ref, dout_ref, denc_ref, dvec_ref)):
            ref[...] = jnp.zeros_like(ref) if first else olds[n][...]

    heads = attn_ref.shape[0]
    ff = up_ref.shape[1]
    bias, gain_two, gain_three, head_vec = (vec_ref[r:r + 1, :] for r in range(4))
    target, live = side_ref[:, 0:1], side_ref[:, 1:2]
    attn = jnp.concatenate([attn_ref[h] for h in range(heads)], axis=1)
    feat = feat_ref[...]
    hidden_one = dotf(feat, enc_ref[...], NN) + bias + dotf(attn, out_ref[...], NN)
    norm_two, inv_two = row_norm(hidden_one)
    act_two = (norm_two * gain_two).astype(bf16)
    root = 0.7978845608028654
    acts = []
    for c in range(0, ff, chunk):
        u = dotf(act_two, up_ref[:, c:c + chunk], NN)
        square = u * u
        half = 0.5 * (1.0 + jnp.tanh(root * (u + 0.044715 * (u * square))))
        act = (u * half).astype(bf16)
        u_ref[:, c:c + chunk] = half + 2.0 * u * half * (1.0 - half) * (root * (1.0 + 0.134145 * square))
        g_ref[:, c:c + chunk] = act
    hidden_two = hidden_one + dotf(g_ref[...], down_ref[...], NN)
    norm_three, inv_three = row_norm(hidden_two)
    scaled = norm_three * gain_three
    error = jnp.sum(scaled * head_vec, axis=-1, keepdims=True) - target
    weighed = live * error
    grad_pred = 2.0 * weighed / total_ref[0]
    grad_two = norm_back(grad_pred * (head_vec * gain_three), norm_three, inv_three)
    low_two = grad_two.astype(bf16)
    act_two_t = act_two.T
    for c in range(0, ff, chunk):
        ddown_ref[c:c + chunk, :] += dotf(g_ref[:, c:c + chunk].T, low_two, NN)
        grad_up = (u_ref[:, c:c + chunk] * dotf(low_two, down_ref[c:c + chunk, :], NT)).astype(bf16)
        dup_ref[:, c:c + chunk] += dotf(act_two_t, grad_up, NN)
        g_ref[:, c:c + chunk] = grad_up
    grad_act_two = dotf(g_ref[...], up_ref[...], NT)
    grad_one = grad_two + norm_back(grad_act_two * gain_two, norm_two, inv_two)
    low_one = grad_one.astype(bf16)
    dout_ref[...] += dotf(attn.T, low_one, NN)
    denc_ref[...] += dotf(feat.T, low_one, NN)
    gattn = dotf(low_one, out_ref[...], NT).astype(bf16)
    width = gattn.shape[1] // heads
    for h in range(heads):
        gattn_ref[h] = gattn[:, h * width:(h + 1) * width]
    down = lambda a: jnp.sum(a, axis=0, keepdims=True)
    loss = jnp.broadcast_to(jnp.sum(weighed * error, axis=0, keepdims=True), (1, bias.shape[1]))
    dvec_ref[...] += jnp.concatenate(
        [down(grad_one), down(grad_act_two * norm_two), down(grad_pred * head_vec * norm_three), down(grad_pred * scaled), loss,
         jnp.zeros((3, bias.shape[1]), f32)], axis=0)


def dense(part, total, attn, feat, side, vec, enc, weights, ff, olds=None, tile=512, chunk=1024):
    heads, rows, cols = attn.shape
    width = enc.shape[1]
    per = rows // tile
    first = olds is None
    whole = lambda a: pl.BlockSpec(a.shape, lambda i: (0,) * a.ndim, pipeline_mode=pl.Buffered(1))
    keep = lambda s: pl.BlockSpec(s, lambda i: (0,) * len(s), pipeline_mode=pl.Buffered(1))
    shapes = [(ff, width), (width, ff), (width, width), (feat.shape[1], width), (8, width)]
    olds = () if first else tuple(olds)
    kernel, extra = dense_kernel, []
    if len(weights) == 1:
        pieces = weights[0].shape[0] * weights[0].shape[1]
        kernel = functools.partial(packed_dense_kernel, (ff // pieces, width // pieces))
        extra = [pltpu.VMEM((width, width), bf16), pltpu.VMEM((width, ff), bf16), pltpu.VMEM((ff, width), bf16)]
    return pl.pallas_call(
        functools.partial(kernel, first, chunk),
        grid=(per,),
        in_specs=[pl.BlockSpec(memory_space=pltpu.SMEM),
                  pl.BlockSpec((heads, tile, cols), lambda i: (0, i, 0)),
                  pl.BlockSpec((tile, feat.shape[1]), lambda i: (part * per + i, 0)),
                  pl.BlockSpec((tile, side.shape[1]), lambda i: (part * per + i, 0)),
                  whole(vec), whole(enc)] + [whole(w) for w in weights] + [whole(o) for o in olds],
        out_specs=[pl.BlockSpec((heads, tile, cols), lambda i: (0, i, 0))] + [keep(s) for s in shapes],
        out_shape=[jax.ShapeDtypeStruct((heads, rows, cols), bf16)] + [jax.ShapeDtypeStruct(s, f32) for s in shapes],
        scratch_shapes=[pltpu.VMEM((tile, ff), f32), pltpu.VMEM((tile, ff), bf16)] + extra,
        compiler_params=pltpu.CompilerParams(vmem_limit_bytes=67043328),
        cost_estimate=pl.CostEstimate(flops=rows * 5 * 10**7, bytes_accessed=3 * 10**7, transcendentals=0),
        name="dense",
    )(total, attn, feat, side, vec, enc, *weights, *olds)
MESH = pl.DeviceIdType.MESH


def front_kernel(nodes, heads, parts, feat, enc, qkv, vec, down, up, out, out_f, out_e, out_q, out_v, packed, up_s, up_r, down_s, down_r, halo_s, halo_r,
                 w_s, w_r, l_sem, down_v, up_v, out_v2):
    node, head = lax.axis_index("nodes"), lax.axis_index("heads")
    after, before = lax.rem(node + 1, nodes), lax.rem(node + nodes - 1, nodes)
    barrier = pltpu.get_barrier_semaphore()
    for other in (after, before):
        pl.semaphore_signal(barrier, inc=1, device_id=(other, head), device_id_type=MESH)
    for s in range(1, heads):
        pl.semaphore_signal(barrier, inc=1, device_id=(node, lax.rem(head + s, heads)), device_id_type=MESH)
    pl.semaphore_wait(barrier, heads + 1)

    rows = feat.shape[0] // parts
    cut = lambda k: pl.ds(k * rows, rows)

    def relay(step, k, upward):
        shard = jnp.clip(head - step if upward else head + step, 0, heads - 1)
        target = jnp.clip(head + 1 if upward else head - 1, 0, heads - 1)
        sems = (up_s, up_r) if upward else (down_s, down_r)
        src = feat.at[cut(k)] if step == 0 else out_f.at[1, shard, cut(k)]
        return pltpu.make_async_remote_copy(
            src_ref=src, dst_ref=out_f.at[1, shard, cut(k)], send_sem=sems[0].at[step, k], recv_sem=sems[1].at[step, k],
            device_id=(node, target), device_id_type=MESH)

    def halo(shard, k, src, way):
        return pltpu.make_async_remote_copy(
            src_ref=src, dst_ref=out_f.at[0 if way == 0 else 2, shard, cut(k)], send_sem=halo_s.at[way, shard, k], recv_sem=halo_r.at[way, shard, k],
            device_id=(after if way == 0 else before, head), device_id_type=MESH)

    def sends(step, upward):
        return (head - step >= 0) & (head + 1 <= heads - 1) if upward else (head + step <= heads - 1) & (head - 1 >= 0)

    def gets(step, upward):
        return head - 1 - step >= 0 if upward else head + 1 + step <= heads - 1

    for k in range(parts):
        for upward in (True, False):
            @pl.when(sends(0, upward))
            def _(k=k, upward=upward):
                relay(0, k, upward).start()
        for way in range(2):
            halo(head, k, feat.at[cut(k)], way).start()
    own = [pltpu.make_async_copy(feat, out_f.at[1, head], l_sem.at[0]),
           pltpu.make_async_copy(enc, out_e.at[head], l_sem.at[1]),
           pltpu.make_async_copy(qkv.at[head], out_q.at[head], l_sem.at[2]),
           pltpu.make_async_copy(vec, out_v.at[head], l_sem.at[3])]
    own += [pltpu.make_async_copy(src.at[node], dst, l_sem.at[4 + i]) for i, (src, dst) in enumerate(((down, down_v), (up, up_v), (out, out_v2)))]
    for copy in own:
        copy.start()
    for copy in own:
        copy.wait()
    width = out_v2.shape[1]
    rows_down, rows_out = down_v.shape[0], out_v2.shape[0]
    packed[:rows_down, :] = down_v[...].astype(bf16)
    at = rows_down
    for c in range(0, up_v.shape[1], width):
        packed[at:at + rows_out, :] = up_v[:, c:c + width].astype(bf16)
        at += rows_out
    packed[at:at + rows_out, :] = out_v2[...].astype(bf16)

    weights = []
    for step in range(heads - 1):
        if step == heads - 2:
            for s in range(1, heads):
                there = lax.rem(head + s, heads)
                for i, (src, dst) in enumerate(((enc, out_e.at[head]), (qkv.at[there], out_q.at[head]), (vec, out_v.at[head]))):
                    slot = (s - 1) * 3 + i
                    weights.append(pltpu.make_async_remote_copy(
                        src_ref=src, dst_ref=dst, send_sem=w_s.at[slot], recv_sem=w_r.at[slot], device_id=(node, there), device_id_type=MESH))
                    weights[-1].start()
        for k in range(parts):
            for upward in (True, False):
                @pl.when(gets(step, upward))
                def _(step=step, k=k, upward=upward):
                    relay(step, k, upward).wait_recv()
                    if step + 1 < heads - 1:
                        @pl.when(sends(step + 1, upward))
                        def _():
                            relay(step + 1, k, upward).start()
                    shard = head - 1 - step if upward else head + 1 + step
                    for way in range(2):
                        halo(shard, k, out_f.at[1, shard, cut(k)], way).start()
    for step in range(heads - 1):
        for k in range(parts):
            for upward in (True, False):
                @pl.when(sends(step, upward))
                def _(step=step, k=k, upward=upward):
                    relay(step, k, upward).wait_send()
    for copy in weights:
        copy.wait()
    for shard in range(heads):
        for k in range(parts):
            for way in range(2):
                halo(shard, k, feat.at[cut(k)], way).wait()


def front(feat, enc, qkv, vec, down, up, out, nodes, heads, parts=2):
    dma = pltpu.SemaphoreType.DMA
    vmem, anywhere = pl.BlockSpec(memory_space=pltpu.VMEM), pl.BlockSpec(memory_space=pl.ANY)
    n = 3 * (heads - 1)
    width = out.shape[2]
    rows = down.shape[1] + up.shape[1] * up.shape[2] // width + out.shape[1]
    return pl.pallas_call(
        functools.partial(front_kernel, nodes, heads, parts),
        in_specs=[vmem] * 4 + [anywhere] * 3, out_specs=[anywhere] + [vmem] * 4,
        out_shape=[jax.ShapeDtypeStruct((3, heads, *feat.shape), feat.dtype), jax.ShapeDtypeStruct((heads, *enc.shape), enc.dtype),
                   jax.ShapeDtypeStruct(qkv.shape, qkv.dtype), jax.ShapeDtypeStruct((heads, *vec.shape), vec.dtype),
                   jax.ShapeDtypeStruct((rows, width), bf16)],
        scratch_shapes=[dma((heads - 1, parts))] * 4 + [dma((2, heads, parts))] * 2 + [dma((n,))] * 2 + [dma((7,))]
        + [pltpu.VMEM(a.shape[1:], f32) for a in (down, up, out)],
        compiler_params=pltpu.CompilerParams(collective_id=2, has_side_effects=True, vmem_limit_bytes=67043328),
        name="front",
    )(feat, enc, qkv, vec, down, up, out)


def pair_kernel(nodes, heads, down, up, out, *refs):
    slabs, (got_d, got_u, got_o, own_d, own_u, own_o, s_sem, r_sem, l_sem) = refs[:nodes // 2], refs[nodes // 2:]
    node, head = lax.axis_index("nodes"), lax.axis_index("heads")
    chips = nodes // 2
    chip, side = lax.div(node, 2), lax.rem(node, 2)
    twin = chip * 2 + 1 - side
    barrier = pltpu.get_barrier_semaphore()
    pl.semaphore_signal(barrier, inc=1, device_id=(twin, head), device_id_type=MESH)
    pl.semaphore_wait(barrier, 1)
    moves = []
    for i, (src, got, own) in enumerate(((down, got_d, own_d), (up, got_u, own_u), (out, got_o, own_o))):
        local = pltpu.make_async_copy(src.at[:, :, side], own, l_sem.at[i])
        remote = pltpu.make_async_remote_copy(
            src_ref=src.at[:, :, 1 - side], dst_ref=got, send_sem=s_sem.at[i], recv_sem=r_sem.at[i], device_id=(twin, head), device_id_type=MESH)
        local.start()
        remote.start()
        moves.append((local, remote))
    width = out.shape[-1]
    at = 0
    for (local, remote), got, own in zip(moves, (got_d, got_u, got_o), (own_d, own_u, own_o)):
        local.wait()
        remote.wait()
        rows = own.shape[2]
        for c in range(0, own.shape[3], width):
            for s in range(chips):
                there = lax.rem(chip + s, chips)
                slabs[s][:, at:at + rows, :] = own[:, there, :, c:c + width] + got[:, there, :, c:c + width]
            at += rows


def pair(down, up, out, nodes, heads):
    chips = nodes // 2
    split = lambda a: a.reshape(heads, chips, 2, -1, a.shape[-1])
    down, up, out = split(down), split(up), split(out)
    width = out.shape[-1]
    rows = sum(a.shape[3] * a.shape[4] // width for a in (down, up, out))
    half = [pltpu.VMEM((heads, chips, *a.shape[3:]), f32) for a in (down, up, out)]
    dma = pltpu.SemaphoreType.DMA
    return pl.pallas_call(
        functools.partial(pair_kernel, nodes, heads),
        in_specs=[pl.BlockSpec(memory_space=pl.ANY)] * 3, out_specs=[pl.BlockSpec(memory_space=pltpu.VMEM)] * chips,
        out_shape=[jax.ShapeDtypeStruct((heads, rows, width), f32)] * chips,
        scratch_shapes=half + half + [dma((3,))] * 3,
        compiler_params=pltpu.CompilerParams(collective_id=3, has_side_effects=True, vmem_limit_bytes=67043328),
        cost_estimate=pl.CostEstimate(flops=10**10, bytes_accessed=2 * 10**7, transcendentals=0),
        name="pair",
    )(down, up, out)


def send(src, dst, sems, slot, node, head):
    copy = pltpu.make_async_remote_copy(
        src_ref=src, dst_ref=dst, send_sem=sems[0].at[slot], recv_sem=sems[1].at[slot], device_id=(node, head), device_id_type=MESH)
    copy.start()
    return copy


def greet(nodes, heads, node, head):
    barrier = pltpu.get_barrier_semaphore()
    for s in range(1, nodes):
        pl.semaphore_signal(barrier, inc=1, device_id=(lax.rem(node + s, nodes), head), device_id_type=MESH)
    for s in range(1, heads):
        pl.semaphore_signal(barrier, inc=1, device_id=(node, lax.rem(head + s, heads)), device_id_type=MESH)
    pl.semaphore_wait(barrier, nodes + heads - 2)


def finish_kernel(nodes, heads, *refs):
    (qkv, enc, vec, *bulk), refs = refs[:4], refs[4:]
    (out_q, out_e, out_v, *out_b), refs = refs[:4], refs[4:]
    (q_half, q_one, q_two, q_part, q_sum, q_own, e_half, e_one, e_two, e_sum, e_three, e_own, v_half, v_two, v_three, v_one, v_sum), refs = refs[:17], refs[17:]
    s_one, r_one, s_two, r_two, s_three, r_three, s_four, r_four, s_bulk, r_bulk, s_pass, r_pass, l_sem = refs
    node, head = lax.axis_index("nodes"), lax.axis_index("heads")
    chips = nodes // 2
    chip, side = lax.div(node, 2), lax.rem(node, 2)
    twin = chip * 2 + 1 - side
    cuts = 3 if bulk[0].shape[0] % 24 == 0 else 1
    step = bulk[0].shape[0] // cuts
    greet(nodes, heads, node, head)
    first = [send(ref.at[:, :, 1 - side], dst, (s_one, r_one), i, twin, head) for i, (ref, dst) in enumerate(((qkv, q_half), (enc, e_half)))]
    first.append(send(vec, v_half, (s_one, r_one), 2, twin, head))
    keep = [pltpu.make_async_copy(src, dst.at[node], l_sem.at[i]) for i, (src, dst) in enumerate(zip(bulk, out_b))]
    for copy in keep:
        copy.start()
    spread = {}

    def bulk_out(which):
        for k in which:
            for s in range(chips):
                other = lax.rem(chip + s, chips) * 2 + side if s else twin
                at = pl.ds(k * step, step)
                spread[k, s] = send(bulk[0].at[at], out_b[0].at[node, at], (s_bulk, r_bulk), k * chips + s, other, head)

    bulk_out(range(1))
    for copy in first:
        copy.wait()
    q_one[...] = qkv[:, :, side] + q_half[...]
    e_one[...] = enc[:, :, side] + e_half[...]
    v_one[...] = vec[...] + v_half[...]
    second = []
    for s in range(1, chips):
        there = lax.rem(chip + s, chips)
        target = there * 2 + side
        i = (s - 1) * 3
        second.append(send(q_one.at[:, there], q_two.at[s - 1], (s_two, r_two), i, target, head))
        second.append(send(e_one.at[:, there], e_two.at[s - 1], (s_two, r_two), i + 1, target, head))
        second.append(send(v_one, v_two.at[s - 1], (s_two, r_two), i + 2, target, head))
    bulk_out(range(1, cuts))
    for copy in second:
        copy.wait()
    q_part[...] = functools.reduce(jnp.add, [q_two[s] for s in range(chips - 1)], q_one[:, chip])
    e_sum[...] = functools.reduce(jnp.add, [e_two[s] for s in range(chips - 1)], e_one[:, chip])
    v_sum[...] = functools.reduce(jnp.add, [v_two[s] for s in range(chips - 1)], v_one[...])
    third = []
    for s in range(1, heads):
        there = lax.rem(head + s, heads)
        i = (s - 1) * 3
        third.append(send(q_part.at[there], q_sum.at[head], (s_three, r_three), i, node, there))
        third.append(send(e_sum.at[there], e_three.at[s - 1], (s_three, r_three), i + 1, node, there))
        third.append(send(v_sum, v_three.at[s - 1], (s_three, r_three), i + 2, node, there))
    for copy in third:
        copy.wait()
    q_sum[pl.ds(head, 1)] = q_part[pl.ds(head, 1)]
    e_own[...] = functools.reduce(jnp.add, [e_three[s] for s in range(heads - 1)], e_sum[head])
    out_v[...] = functools.reduce(jnp.add, [v_three[s] for s in range(heads - 1)], v_sum[...])
    fourth = []
    for s in range(1, nodes):
        there = lax.rem(node + s, nodes)
        fourth.append(send(q_sum, out_q.at[node], (s_four, r_four), (s - 1) * 2, there, head))
        fourth.append(send(e_own, out_e.at[node], (s_four, r_four), (s - 1) * 2 + 1, there, head))
    out_q[node] = q_sum[...]
    out_e[node] = e_own[...]
    for copy in keep:
        copy.wait()
    passed = []
    for k in range(cuts):
        for s in range(chips):
            spread[k, s].wait()
            if s:
                origin = lax.rem(chip + chips - s, chips) * 2 + side
                here = out_b[0].at[origin, pl.ds(k * step, step)]
                passed.append(send(here, here, (s_pass, r_pass), k * (chips - 1) + s - 1, twin, head))
    for copy in passed:
        copy.wait()
    for copy in fourth:
        copy.wait()


def finish(qkv, enc, vec, bulk, nodes, heads):
    chips = nodes // 2
    split = lambda a: a.reshape(heads, chips, 2, -1, a.shape[-1])
    qkv, enc = split(qkv), split(enc)
    vm = lambda *s: pltpu.VMEM(s, f32)
    rq, wq, re, we = *qkv.shape[3:], *enc.shape[3:]
    dma = pltpu.SemaphoreType.DMA
    wv = vec.shape
    scratch = [vm(heads, chips, rq, wq), vm(heads, chips, rq, wq), vm(chips - 1, heads, rq, wq), vm(heads, rq, wq), vm(heads, rq, wq), vm(8, 128),
               vm(heads, chips, re, we), vm(heads, chips, re, we), vm(chips - 1, heads, re, we), vm(heads, re, we), vm(heads - 1, re, we), vm(re, we),
               vm(*wv), vm(chips - 1, *wv), vm(heads - 1, *wv), vm(*wv), vm(*wv)]
    counts = (3, 3, 3 * chips - 3, 3 * chips - 3, 3 * heads - 3, 3 * heads - 3, 2 * nodes - 2, 2 * nodes - 2, 3 * chips, 3 * chips, 3 * chips - 3, 3 * chips - 3, 1)
    out_shape = [jax.ShapeDtypeStruct(s, f32) for s in [(nodes, heads, rq, wq), (nodes, re, we), wv] + [(nodes, *b.shape) for b in bulk]]
    spec = pl.BlockSpec(memory_space=pltpu.VMEM)
    return pl.pallas_call(
        functools.partial(finish_kernel, nodes, heads),
        in_specs=[spec] * 4, out_specs=[spec] * 4, out_shape=out_shape,
        scratch_shapes=scratch + [dma((n,)) for n in counts],
        compiler_params=pltpu.CompilerParams(collective_id=1, has_side_effects=True, vmem_limit_bytes=48 << 20),
        name="finish",
    )(qkv, enc, vec, *bulk)
D = 512
HEADS = 8
NBR = 8
ADAM_STEP = 3
highest = lax.Precision.HIGHEST
beta_one = 0.5
beta_two = 0.5
learn_rate = 0.02
weight_decay = 0.1
adam_eps = 1e-08


def adamw(weight, first_moment, second, gradient):
    first_new = beta_one * first_moment + (1.0 - beta_one) * gradient
    second_new = beta_two * second + (1.0 - beta_two) * gradient * gradient
    first_hat = first_new / (1.0 - beta_one**ADAM_STEP)
    second_hat = second_new / (1.0 - beta_two**ADAM_STEP)
    weight_new = weight - learn_rate * (
        first_hat / (jnp.sqrt(second_hat) + adam_eps) + weight_decay * weight
    )
    return (weight_new, first_new, second_new)


def local(
    features, target, counts, neighbours, edge_kinds,
    enc_weight, enc_first, enc_second, qkv_weight, qkv_first, qkv_second,
    out_weight, out_first, out_second, up_weight, up_first, up_second,
    down_weight, down_first, down_second, vec_weight, vec_first, vec_second,
):
    heads_count = lax.axis_size("heads")
    nodes_count = lax.axis_size("nodes")
    head_index = lax.axis_index("heads")
    node_index = lax.axis_index("nodes")
    row_count = features.shape[0]
    own_blocks = row_count // BLOCK
    group_blocks = own_blocks * heads_count
    group_rows = group_blocks * BLOCK
    hl = HEADS // heads_count
    hs = D // HEADS
    cols = hl * hs
    cp = -(-cols // 128) * 128
    ka = -(-(cols + 1) // 128) * 128
    kinds = D // HEADS
    slots = NBR + 1
    low = lambda a: a.astype(bf16)
    gather = lambda a, axis: lax.all_gather(low(a), "heads", axis=axis, tiled=True)

    qkv_parts = jnp.transpose(low(qkv_weight).reshape(-1, heads_count, hl, 3, hs), (1, 0, 3, 2, 4)).reshape(heads_count, -1, 3, cols)
    qkv_parts = jnp.pad(qkv_parts, ((0, 0), (0, 0), (0, 0), (0, cp - cols))).reshape(heads_count, -1, 3 * cp)
    vec_part = jnp.pad(low(vec_weight).astype(f32), ((0, 2), (0, 0)))
    ff = up_weight.shape[1]
    pieces = heads_count * nodes_count
    rows_down, rows_out = ff // pieces, D // pieces
    by_node = lambda a: a.reshape(nodes_count, -1, a.shape[1])
    feats, enc_b, qkv_cols, vectors, packed = front(
        features, low(enc_weight), qkv_parts, vec_part, by_node(down_weight), by_node(up_weight), by_node(out_weight), nodes_count, heads_count)
    feats = feats.reshape(3 * group_rows, -1)
    enc_b = enc_b.reshape(-1, D)
    qkv_cols = qkv_cols.reshape(D, 3 * cp)
    vectors = jnp.transpose(vectors, (1, 0, 2)).reshape(8, D)
    packed = lax.all_gather(packed, ("heads", "nodes"), axis=0, tiled=False).reshape(heads_count, nodes_count, -1, D)

    enc_bias, gain_one, gain_two, gain_three, head_vec = (vectors[r] for r in range(5))
    edge_local = lax.dynamic_slice_in_dim(vectors[5].reshape(kinds, HEADS), head_index * hl, hl, 1)
    own_counts = lax.dynamic_slice_in_dim(counts, (node_index * heads_count + head_index) * own_blocks, own_blocks)
    row_live = (jnp.arange(BLOCK, dtype=jnp.int32)[None, :] < own_counts[:, None]).reshape(row_count).astype(f32)
    live_total = jnp.sum(counts).astype(f32)

    def group_counts(offset):
        return lax.dynamic_slice_in_dim(counts, (node_index + offset) % nodes_count * group_blocks, group_blocks)

    pool_counts = jnp.concatenate([group_counts(nodes_count - 1), group_counts(0), group_counts(1)])
    relative = (neighbours // group_blocks - node_index + 1) % nodes_count
    nbr_pos = relative * group_blocks + neighbours % group_blocks
    self_pos = group_blocks + jnp.arange(group_blocks, dtype=jnp.int32)
    key_pos = jnp.concatenate([self_pos[:, None], nbr_pos], axis=1).reshape(-1)
    kind_hot = jax.nn.one_hot(edge_kinds, kinds, dtype=f32)
    slot_bias = jnp.einsum("bst,th->bsh", kind_hot, edge_local, precision=highest)
    bias_rows = jnp.repeat(slot_bias, BLOCK, axis=2)

    kaug, kt, value, vt, query = encode(
        pool_counts, feats, enc_b, enc_bias[None], gain_one[None], qkv_cols, cp, ka, cols, hs**-0.5)
    side = jnp.stack([target, row_live], axis=1)
    dense_vec = jnp.stack([enc_bias, gain_two, gain_three, head_vec])
    half = lambda a: a.reshape(heads_count, 2, row_count // 2, -1)
    exchange = lambda a: lax.all_to_all(a, "heads", split_axis=0, concat_axis=0, tiled=True)
    attn_parts, lse_parts, grad_parts, totals = [], [], [], None
    for part in range(2):
        attn_part, lse_part = attend(part, own_blocks, key_pos, query, bias_rows, kaug, vt, hl, hs)
        attn_parts.append(attn_part)
        lse_parts.append(lse_part)
    packed, attn_parts[1] = lax.optimization_barrier((packed, attn_parts[1]))
    weights = (packed,)
    if rows_out % 16:
        up_rows = packed[:, :, rows_down:-rows_out].reshape(pieces, -1, rows_out, D)
        weights = (packed[:, :, -rows_out:].reshape(D, D), jnp.transpose(up_rows, (0, 2, 1, 3)).reshape(D, ff), packed[:, :, :rows_down].reshape(ff, D))
    for part in range(2):
        attn_rows = exchange(attn_parts[part].reshape(heads_count, row_count // 2, cp)[..., :cols])
        grad_part, *totals = dense(part, live_total[None], attn_rows, features, side, dense_vec, enc_b, weights, ff, totals)
        grad_parts.append(exchange(grad_part))
    grad_down, grad_up, grad_out, denc_own, dense_sums = totals
    grad_parts[0], grad_down = lax.optimization_barrier((grad_parts[0], grad_down))
    slab = pair(grad_down, grad_up, grad_out, nodes_count, heads_count)
    moved = [slab[0]] + [
        lax.ppermute(slab[s], "nodes", [(i, (i + 2 * s) % nodes_count) for i in range(nodes_count)]) for s in range(1, nodes_count // 2)]
    grad_heads = [jnp.pad(g.reshape(group_rows // 2, cols), ((0, 0), (0, cp - cols))) for g in grad_parts]
    dq, dkv, edge_sums = attend_back(own_blocks, key_pos, query, grad_heads, attn_parts, lse_parts, bias_rows, kaug, value, kt, hl, hs)
    moved, dkv = lax.optimization_barrier((moved, dkv))
    planes = exchange(functools.reduce(jnp.add, moved))
    slot_sums = jnp.sum(edge_sums.reshape(group_blocks, slots, hl, BLOCK), axis=3)
    edge_grad = jnp.einsum("bst,bsh->th", kind_hot, slot_sums, precision=highest)
    columns = lambda a: jnp.broadcast_to(a[:, None], (D, 128))
    dw, denc_t, dgain, dbias = encode_back(
        feats, dkv, dq, enc_b.T, columns(enc_bias), columns(gain_one), qkv_cols[:, :cp], qkv_cols[:, cp:])

    grad_gain_one = jnp.sum(dgain, axis=1)
    grad_enc_bias = jnp.sum(dbias, axis=1) + dense_sums[0]
    grad_enc = denc_t.T + denc_own
    edge_full = lax.dynamic_update_slice(jnp.zeros((kinds, HEADS), f32), edge_grad, (jnp.int32(0), head_index * hl))
    grad_vec = jnp.concatenate([grad_enc_bias[None], grad_gain_one[None], dense_sums[1:5], edge_full.reshape(1, D), jnp.zeros((1, D), f32)])
    planes, dw = lax.optimization_barrier((planes, dw))
    dw_sum, enc_sum, vec_total, bulk = finish(dw, grad_enc, grad_vec, [jnp.sum(planes, axis=0)], nodes_count, heads_count)
    total_loss = vec_total[5, 0]
    vec_sum = lax.dynamic_slice_in_dim(jnp.concatenate([vec_total[:5], vec_total[6:7]]), head_index * (D // heads_count), D // heads_count, 1)
    states = (enc_weight, enc_first, enc_second, qkv_weight, qkv_first, qkv_second, out_weight, out_first, out_second,
              up_weight, up_first, up_second, down_weight, down_first, down_second)
    vec_res = adamw(vec_weight, vec_first, vec_second, vec_sum)
    if rows_out % 16:
        qkv_sum = jnp.transpose(dw_sum, (0, 2, 1, 3)).reshape(-1, heads_count, 3, cp)[..., :cols].reshape(-1, heads_count, 3, hl, hs)
        qkv_sum = jnp.transpose(qkv_sum, (0, 1, 3, 2, 4)).reshape(qkv_weight.shape)
        flat = lambda a: a.reshape(-1, a.shape[-1])
        up_sum = bulk[:, rows_down:-rows_out].reshape(nodes_count, -1, rows_out, D)
        up_sum = jnp.transpose(up_sum, (0, 2, 1, 3)).reshape(up_weight.shape)
        summed = (flat(enc_sum), qkv_sum, flat(bulk[:, -rows_out:]), up_sum, flat(bulk[:, :rows_down]))
        results = []
        for n, grad in enumerate(summed):
            results += adamw(*states[3 * n:3 * n + 3], grad)
        results += [low(r) for r in results[::3]]
    else:
        results = adam(enc_sum, dw_sum, bulk, states, hl, hs, cp)
    loss_value = (total_loss / live_total).reshape(1)
    return (loss_value, *results[:15], *vec_res, *results[15:])


def solution(mesh):
    rows = P("heads", None)
    both = P(("nodes", "heads"))
    lanes = P(None, "heads")
    in_specs = (P(("nodes", "heads"), None), both, P(), P("nodes", None), P("nodes", None)) + (rows,) * 15 + (lanes,) * 3
    out_specs = (P(),) + (rows,) * 15 + (lanes,) * 3 + (rows,) * 5
    return jax.shard_map(local, mesh=mesh, in_specs=in_specs, out_specs=out_specs, check_vma=False)


def adam_kernel(hl, hs, cp, *refs):
    g_enc, g_qkv, g_bulk = refs[:3]
    ins, outs = refs[3:18], refs[18:]
    rows_down, rows_out = ins[12].shape[0], ins[6].shape[0]
    heads = g_qkv.shape[1]
    bulk = g_bulk[0]
    parts = []
    for h in range(heads):
        part = g_qkv[0, h]
        for k in range(hl):
            parts += [part[:, j * cp + k * hs:j * cp + (k + 1) * hs] for j in range(3)]
    up_at = lambda c: rows_down + c * rows_out
    grads = [g_enc[0], jnp.concatenate(parts, axis=1), bulk[-rows_out:],
             jnp.concatenate([bulk[up_at(c):up_at(c) + rows_out] for c in range(ins[9].shape[1] // bulk.shape[1])], axis=1), bulk[:rows_down]]
    for n, grad in enumerate(grads):
        new = adamw(*(ref[...] for ref in ins[3 * n:3 * n + 3]), grad)
        for ref, value in zip(outs[3 * n:3 * n + 3], new):
            ref[...] = value
        outs[15 + n][...] = new[0].astype(bf16)


def adam(g_enc, g_qkv, g_bulk, states, hl, hs, cp):
    nodes = g_enc.shape[0]
    rows = lambda a: pl.BlockSpec((a.shape[0] // nodes, a.shape[1]), lambda i: (i, 0))
    lead = lambda a: pl.BlockSpec((1, *a.shape[1:]), lambda i: (i,) + (0,) * (a.ndim - 1))
    shapes = [jax.ShapeDtypeStruct(a.shape, f32) for a in states] + [jax.ShapeDtypeStruct(a.shape, bf16) for a in states[::3]]
    return pl.pallas_call(
        functools.partial(adam_kernel, hl, hs, cp),
        grid=(nodes,),
        in_specs=[lead(g_enc), lead(g_qkv), lead(g_bulk)] + [rows(a) for a in states],
        out_specs=[rows(a) for a in shapes], out_shape=shapes,
        compiler_params=pltpu.CompilerParams(vmem_limit_bytes=67043328),
        name="adam",
    )(g_enc, g_qkv, g_bulk, *states)
```

```python
import functools

import jax
import jax.numpy as jnp
from jax import lax
from jax.experimental import pallas as pl
from jax.experimental.pallas import tpu as pltpu
from jax.sharding import PartitionSpec as P

BLOCK = 128
NT = (((1,), (1,)), ((), ()))
NN = (((1,), (0,)), ((), ()))
f32 = jnp.float32
bf16 = jnp.bfloat16


def dotf(a, b, dims):
    return lax.dot_general(a, b, dims, preferred_element_type=f32)


def head_rows(x, hl, hs, cp):
    if hl == 1:
        return x
    lane = lax.broadcasted_iota(jnp.int32, (BLOCK, cp), 1)
    zero = jnp.zeros_like(x)
    return jnp.concatenate([jnp.where(lane // hs == h, x, zero) for h in range(hl)], axis=0)


def ones_lane(hl, cp, ka):
    rows = hl * BLOCK
    lane = lax.broadcasted_iota(jnp.int32, (rows, ka - cp), 1)
    return jnp.where(lane == 0, 1.0, 0.0).astype(bf16)


def attend_kernel(hl, hs, cp, ka, slots, unit, unit_of, pos_ref, q_ref, brow_ref, kaug_ref, vt_ref, o_ref, lse_ref, *scratch):
    first = unit_of(pl.program_id(0)) * unit
    rows = hl * BLOCK

    def spot(u, s):
        return pos_ref[(first + u) * slots + s]

    def score(u):
        s_ref = scratch[2 * (u % 2)]
        q2 = head_rows(q_ref[u * BLOCK:(u + 1) * BLOCK, :], hl, hs, cp)
        qa = jnp.concatenate([q2, ones_lane(hl, cp, ka)], axis=1) if ka > cp else q2
        keys = [kaug_ref[pl.ds(pl.multiple_of(spot(u, s) * BLOCK, BLOCK), BLOCK), :] for s in range(slots)]
        scores = dotf(jnp.concatenate(keys, axis=0), qa, NT)
        top = None
        for s in range(slots):
            sc = scores[s * BLOCK:(s + 1) * BLOCK]
            s_ref[s] = sc
            t = jnp.max(sc, axis=0, keepdims=True) + brow_ref[u, s:s + 1, :]
            top = t if top is None else jnp.maximum(top, t)
        return top

    def weigh(u, top):
        s_ref, p_ref = scratch[2 * (u % 2):2 * (u % 2) + 2]
        tot = jnp.zeros((1, rows), f32)
        for s in range(slots):
            e = jnp.exp(s_ref[s] - (top - brow_ref[u, s:s + 1, :]))
            s_ref[s] = e
            tot = tot + jnp.sum(e, axis=0, keepdims=True)
        lse_ref[u] = top + jnp.log(tot)
        inv = 1.0 / tot
        for s in range(slots):
            p_ref[s * BLOCK:(s + 1) * BLOCK, :] = (s_ref[s] * inv).astype(bf16)

    def total(u):
        p_ref = scratch[2 * (u % 2) + 1]
        ot = dotf(jnp.concatenate([vt_ref[spot(u, s)] for s in range(slots)], axis=1), p_ref[...], NN)
        parts = [ot[h * hs:(h + 1) * hs, h * BLOCK:(h + 1) * BLOCK] for h in range(hl)]
        if hl * hs < cp:
            parts.append(jnp.zeros((cp - hl * hs, BLOCK), f32))
        o_ref[u * BLOCK:(u + 1) * BLOCK, :] = jnp.concatenate(parts, axis=0).T.astype(bf16)

    top = score(0)
    for u in range(unit):
        following = score(u + 1) if u + 1 < unit else None
        weigh(u, top)
        total(u)
        top = following


def attend(part, own, pos, q, brow, kaug, vt, hl, hs, unit=4):
    cp, ka = q.shape[1], kaug.shape[1]
    nb = q.shape[0] // BLOCK // 2
    half, own = own // 2 // unit, own // unit
    unit_of = lambda i: lax.div(i, half) * own + part * half + lax.rem(i, half)
    slots = brow.shape[1]
    rows = hl * BLOCK
    whole = lambda a: pl.BlockSpec(a.shape, lambda i, *_: (0,) * a.ndim, pipeline_mode=pl.Buffered(1))
    return pl.pallas_call(
        functools.partial(attend_kernel, hl, hs, cp, ka, slots, unit, unit_of),
        grid_spec=pltpu.PrefetchScalarGridSpec(
            num_scalar_prefetch=1, grid=(nb // unit,),
            in_specs=[pl.BlockSpec((unit * BLOCK, cp), lambda i, *_: (unit_of(i), 0)),
                      pl.BlockSpec((unit, slots, rows), lambda i, *_: (unit_of(i), 0, 0)),
                      whole(kaug), whole(vt)],
            out_specs=[pl.BlockSpec((unit * BLOCK, cp), lambda i, *_: (i, 0)),
                       pl.BlockSpec((unit, 1, rows), lambda i, *_: (i, 0, 0))],
            scratch_shapes=[pltpu.VMEM((slots, BLOCK, rows), f32), pltpu.VMEM((slots * BLOCK, rows), bf16)] * 2),
        out_shape=[jax.ShapeDtypeStruct((nb * BLOCK, cp), bf16), jax.ShapeDtypeStruct((nb, 1, rows), f32)],
        cost_estimate=pl.CostEstimate(flops=nb * 10**9, bytes_accessed=3 * 10**7, transcendentals=0),
        compiler_params=pltpu.CompilerParams(vmem_limit_bytes=67043328),
        name="attend",
    )(pos, q, brow, kaug, vt)


def attend_back_kernel(hl, hs, cp, ka, slots, scale, unit, unit_of, pos_ref, q_ref, da_ref, db_ref, oa_ref, ob_ref, la_ref, lb_ref, brow_ref, kaug_ref, v_ref,
                       kt_ref, dq_ref, dkv_ref, edge_ref, *scratch):
    i = pl.program_id(0)
    first = unit_of(i) * unit
    late = i >= pl.num_programs(0) // 2

    @pl.when(i == 0)
    def _():
        @pl.loop(0, dkv_ref.shape[0] // BLOCK)
        def _(n):
            dkv_ref[pl.ds(pl.multiple_of(n * BLOCK, BLOCK), BLOCK), :] = jnp.zeros((BLOCK, dkv_ref.shape[1]), f32)

    for u in range(unit):
        p_ref, d_ref = scratch[2 * (u % 2):2 * (u % 2) + 2]
        own = slice(u * BLOCK, (u + 1) * BLOCK)
        q2 = head_rows(q_ref[own, :], hl, hs, cp)
        qa = jnp.concatenate([q2, ones_lane(hl, cp, ka)], axis=1) if ka > cp else q2
        do = jnp.where(late, db_ref[own, :], da_ref[own, :])
        do2 = head_rows(do, hl, hs, cp)
        prod = (do.astype(f32) * jnp.where(late, ob_ref[own, :], oa_ref[own, :]).astype(f32)).T
        dd = jnp.concatenate([jnp.sum(prod[h * hs:(h + 1) * hs], axis=0, keepdims=True) for h in range(hl)], axis=1)
        lse = jnp.where(late, lb_ref[u], la_ref[u])
        blocks = [pos_ref[(first + u) * slots + s] for s in range(slots)]
        spots = [pl.ds(pl.multiple_of(p * BLOCK, BLOCK), BLOCK) for p in blocks]
        scores = dotf(jnp.concatenate([kaug_ref[at, :] for at in spots], axis=0), qa, NT)
        grads = dotf(jnp.concatenate([v_ref[at, :] for at in spots], axis=0), do2, NT)
        for s in range(slots):
            here = slice(s * BLOCK, (s + 1) * BLOCK)
            pr = jnp.exp(scores[here] - (lse - brow_ref[u, s:s + 1, :]))
            ds = pr * (grads[here] - dd)
            edge_ref[u, s:s + 1, :] = jnp.sum(ds, axis=0, keepdims=True)
            p_ref[here, :] = pr.astype(bf16)
            d_ref[here, :] = ds.astype(bf16)
        dv = dotf(p_ref[...], do2, NN)
        dk = dotf(d_ref[...], q2, NN)
        dqt = dotf(jnp.concatenate([kt_ref[p] for p in blocks], axis=1), d_ref[...], NN)
        for s, at in enumerate(spots):
            here = slice(s * BLOCK, (s + 1) * BLOCK)
            dkv_ref[at, 0:cp] += dk[here]
            dkv_ref[at, cp:2 * cp] += dv[here]
        parts = [dqt[h * hs:(h + 1) * hs, h * BLOCK:(h + 1) * BLOCK] for h in range(hl)]
        if hl * hs < cp:
            parts.append(jnp.zeros((cp - hl * hs, BLOCK), f32))
        dq_ref[own, :] = (jnp.concatenate(parts, axis=0).T * scale).astype(bf16)


def attend_back(own, pos, q, dos, outs, lses, brow, kaug, v, kt, hl, hs, unit=4):
    cp, ka = q.shape[1], kaug.shape[1]
    nb = q.shape[0] // BLOCK
    slots = brow.shape[1]
    rows = hl * BLOCK
    half, mid, own = own // 2 // unit, nb // 2 // unit, own // unit
    unit_of = lambda i: lax.div(lax.rem(i, mid), half) * own + lax.div(i, mid) * half + lax.rem(i, half)
    whole = lambda a: pl.BlockSpec(a.shape, lambda i, *_: (0,) * a.ndim, pipeline_mode=pl.Buffered(1))
    tile = pl.BlockSpec((unit * BLOCK, cp), lambda i, *_: (unit_of(i), 0))
    early = lambda i: jnp.minimum(i, mid - 1)
    late = lambda i: jnp.maximum(i - mid, 0)
    return pl.pallas_call(
        functools.partial(attend_back_kernel, hl, hs, cp, ka, slots, hs ** -0.5, unit, unit_of),
        grid_spec=pltpu.PrefetchScalarGridSpec(
            num_scalar_prefetch=1, grid=(nb // unit,),
            in_specs=[tile] + [pl.BlockSpec((unit * BLOCK, cp), lambda i, *_: (early(i), 0)), pl.BlockSpec((unit * BLOCK, cp), lambda i, *_: (late(i), 0))] * 2 + [
                      pl.BlockSpec((unit, 1, rows), lambda i, *_: (early(i), 0, 0)), pl.BlockSpec((unit, 1, rows), lambda i, *_: (late(i), 0, 0)),
                      pl.BlockSpec((unit, slots, rows), lambda i, *_: (unit_of(i), 0, 0)),
                      whole(kaug), whole(v), whole(kt)],
            out_specs=[tile, pl.BlockSpec((v.shape[0], 2 * cp), lambda i, *_: (0, 0), pipeline_mode=pl.Buffered(1)),
                       pl.BlockSpec((unit, slots, rows), lambda i, *_: (unit_of(i), 0, 0))],
            scratch_shapes=[pltpu.VMEM((slots * BLOCK, rows), bf16)] * 4),
        out_shape=[jax.ShapeDtypeStruct(q.shape, bf16), jax.ShapeDtypeStruct((v.shape[0], 2 * cp), f32),
                   jax.ShapeDtypeStruct((nb, slots, rows), f32)],
        cost_estimate=pl.CostEstimate(flops=nb * 2 * 10**9, bytes_accessed=6 * 10**7, transcendentals=0),
        compiler_params=pltpu.CompilerParams(vmem_limit_bytes=67043328),
        name="attend_back",
    )(pos, q, *dos, *outs, *lses, brow, kaug, v, kt)
norm_eps = 1e-05


def encode_kernel(cp, ka, cols, scale, per_group, inner, cnt_ref, x_all, enc_ref, bias_ref, gain_ref, w_ref,
                  kaug_all, kt_all, v_all, vt_all, q_all):
    @pl.loop(0, x_all.shape[0] // inner)
    def _(n):
        rows = pl.ds(pl.multiple_of(n * inner, inner), inner)
        blocks = pl.ds(n * (inner // BLOCK), inner // BLOCK)
        encode_rows(cp, ka, cols, scale, per_group, pl.program_id(0), n, x_all.shape[0] // inner, cnt_ref, x_all.at[rows], enc_ref, bias_ref, gain_ref,
                    w_ref, kaug_all.at[rows], kt_all.at[blocks], v_all.at[rows], vt_all.at[blocks], q_all.at[rows])


def encode_rows(cp, ka, cols, scale, per_group, i, n, count, cnt_ref, x_ref, enc_ref, bias_ref, gain_ref, w_ref,
                kaug_ref, kt_ref, v_ref, vt_ref, q_ref):
    group = i // per_group
    tile = x_ref.shape[0]
    resid = dotf(x_ref[...], enc_ref[...], NN) + bias_ref[...]
    centred = resid - jnp.mean(resid, axis=-1, keepdims=True)
    variance = jnp.mean(centred * centred, axis=-1, keepdims=True)
    act = (centred * lax.rsqrt(variance + norm_eps) * gain_ref[...]).astype(bf16)
    kv = dotf(act, w_ref[:, cp:], NN).astype(bf16)
    key, value = kv[:, :cp], kv[:, cp:]
    row = lax.broadcasted_iota(jnp.int32, (BLOCK, 128), 0)
    lane = lax.broadcasted_iota(jnp.int32, (BLOCK, 128), 1)
    first = (i * count + n) * (tile // BLOCK)
    dead = jnp.concatenate(
        [jnp.where((row >= cnt_ref[first + j]) & (lane == cols % 128), -1e30, 0.0) for j in range(tile // BLOCK)], axis=0).astype(bf16)
    if ka > cp:
        kaug_ref[:, :cp] = key
        kaug_ref[:, cp:] = dead
    else:
        kaug_ref[...] = key + dead
    v_ref[...] = value
    for j in range(tile // BLOCK):
        kt_ref[j] = key[j * BLOCK:(j + 1) * BLOCK].T
        vt_ref[j] = value[j * BLOCK:(j + 1) * BLOCK].T

    @pl.when(group == 1)
    def _():
        q = (dotf(act, w_ref[:, :cp], NN) * scale).astype(bf16)
        if ka == cp:
            lanes = lax.broadcasted_iota(jnp.int32, q.shape, 1)
            q = jnp.where(lanes == cols, jnp.ones_like(q), q)
        q_ref[...] = q


def encode(counts, feats, enc, bias, gain, w, cp, ka, cols, scale, tile=2048):
    rows, feat = feats.shape[0] // 3, feats.shape[1]
    width = enc.shape[1]
    per = rows // tile
    blocks = tile // BLOCK
    whole = lambda a: pl.BlockSpec(a.shape, lambda i, *_: (0,) * a.ndim, pipeline_mode=pl.Buffered(1))
    return pl.pallas_call(
        functools.partial(encode_kernel, cp, ka, cols, scale, per, 1024),
        grid_spec=pltpu.PrefetchScalarGridSpec(
            num_scalar_prefetch=1, grid=(3 * per,),
            in_specs=[pl.BlockSpec((tile, feat), lambda i, *_: (i, 0)), whole(enc), whole(bias), whole(gain), whole(w)],
            out_specs=[pl.BlockSpec((tile, ka), lambda i, *_: (i, 0)),
                       pl.BlockSpec((blocks, cp, BLOCK), lambda i, *_: (i, 0, 0)),
                       pl.BlockSpec((tile, cp), lambda i, *_: (i, 0)),
                       pl.BlockSpec((blocks, cp, BLOCK), lambda i, *_: (i, 0, 0)),
                       pl.BlockSpec((tile, cp), lambda i, *_: (jnp.clip(i - per, 0, per - 1), 0))]),
        out_shape=[jax.ShapeDtypeStruct((3 * rows, ka), bf16),
                   jax.ShapeDtypeStruct((3 * rows // BLOCK, cp, BLOCK), bf16),
                   jax.ShapeDtypeStruct((3 * rows, cp), bf16),
                   jax.ShapeDtypeStruct((3 * rows // BLOCK, cp, BLOCK), bf16),
                   jax.ShapeDtypeStruct((rows, cp), bf16)],
        compiler_params=pltpu.CompilerParams(vmem_limit_bytes=67043328),
        cost_estimate=pl.CostEstimate(flops=rows * 6 * 10**6, bytes_accessed=3 * 10**7, transcendentals=0),
        name="encode",
    )(counts, feats, enc, bias, gain, w)


def encode_back_kernel(cp, per_group, inner, x_all, dkv_all, dq_all, enc_ref, vec_ref, w_ref, own_ref, sums_ref, edge_ref,
                       dw_ref, denc_ref, dvec_ref, g_ref, enct_ref, bias_ref, gain_ref, denct_ref, dgain_ref, dbias_ref):
    i = pl.program_id(0)

    @pl.when(i == 0)
    def _():
        for ref in (dw_ref, denct_ref, dgain_ref, dbias_ref):
            ref[...] = jnp.zeros_like(ref)
        enct_ref[...] = enc_ref[...].T
        for r, ref in enumerate((bias_ref, gain_ref)):
            ref[...] = jnp.broadcast_to(vec_ref[r:r + 1, :], (128, vec_ref.shape[1])).T

    @pl.loop(0, x_all.shape[0] // inner)
    def _(n):
        rows = pl.ds(pl.multiple_of(n * inner, inner), inner)
        encode_back_rows(cp, i // per_group, x_all.at[rows], dkv_all.at[rows], dq_all.at[rows], enct_ref, bias_ref, gain_ref, w_ref,
                         dw_ref, denct_ref, dgain_ref, dbias_ref, g_ref)

    @pl.when(i == pl.num_programs(0) - 1)
    def _():
        denc_ref[...] = denct_ref[...].T + own_ref[...]
        line = lambda ref: jnp.sum(ref[...].T, axis=0, keepdims=True)
        dvec_ref[...] = jnp.concatenate(
            [line(dbias_ref) + sums_ref[0:1, :], line(dgain_ref), sums_ref[1:5, :], edge_ref[...], jnp.zeros_like(edge_ref[...])], axis=0)


def encode_back_rows(cp, group, x_ref, dkv_ref, dq_ref, enct_ref, bias_ref, gain_ref, w_ref,
                     dw_ref, denc_ref, dgain_ref, dbias_ref, g_ref):
    tile = x_ref.shape[0]
    width = enct_ref.shape[0]
    reps = tile // 128

    x = x_ref[...]
    wide = lambda c: jnp.concatenate([c] * reps, axis=1)
    fold = lambda a: functools.reduce(jnp.add, [a[:, r * 128:(r + 1) * 128] for r in range(reps)])
    resid = dotf(enct_ref[...], x, NT) + wide(bias_ref[...])
    centred = resid - jnp.sum(resid, axis=0, keepdims=True) * (1.0 / width)
    variance = jnp.sum(centred * centred, axis=0, keepdims=True) * (1.0 / width)
    inv = lax.rsqrt(variance + norm_eps)
    norm = centred * inv
    gain = wide(gain_ref[...])
    act = (norm * gain).astype(bf16)
    dkv = dkv_ref[...].astype(bf16)
    g_ref[...] = dotf(w_ref[:, cp:], dkv, NT)
    dw_ref[:, cp:] += dotf(act, dkv, NN)

    @pl.when(group == 1)
    def _():
        dq = dq_ref[...]
        g_ref[...] += dotf(w_ref[:, :cp], dq, NT)
        dw_ref[:, :cp] += dotf(act, dq, NN)

    grad = g_ref[...]
    dgain_ref[...] += fold(grad * norm)
    back = grad * gain
    mean_one = jnp.sum(back, axis=0, keepdims=True) * (1.0 / width)
    mean_two = jnp.sum(back * norm, axis=0, keepdims=True) * (1.0 / width)
    din = inv * (back - mean_one - norm * mean_two)
    dbias_ref[...] += fold(din)
    denc_ref[...] += dotf(din.astype(bf16), x, NN)


def encode_back(feats, dkv, dq, enc, vec, w, own, sums, edge, tile=2048, inner=1024):
    rows, feat = feats.shape[0] // 3, feats.shape[1]
    width = enc.shape[1]
    cp = dq.shape[1]
    per = rows // tile
    whole = lambda a: pl.BlockSpec(a.shape, lambda i: (0,) * a.ndim, pipeline_mode=pl.Buffered(1))
    keep = lambda s: pl.BlockSpec(s, lambda i: (0,) * len(s), pipeline_mode=pl.Buffered(1))
    shapes = [(width, 3 * cp), (feat, width), (8, width)]
    column = pltpu.VMEM((width, 128), f32)
    return pl.pallas_call(
        functools.partial(encode_back_kernel, cp, per, inner),
        grid=(3 * per,),
        in_specs=[pl.BlockSpec((tile, feat), lambda i: (i, 0)), pl.BlockSpec((tile, 2 * cp), lambda i: (i, 0)),
                  pl.BlockSpec((tile, cp), lambda i: (jnp.clip(i - per, 0, per - 1), 0))] + [whole(a) for a in (enc, vec, w, own, sums, edge)],
        out_specs=[keep(s) for s in shapes],
        out_shape=[jax.ShapeDtypeStruct(s, f32) for s in shapes],
        scratch_shapes=[pltpu.VMEM((width, inner), f32), pltpu.VMEM((width, feat), bf16), column, column, pltpu.VMEM((width, feat), f32), column, column],
        compiler_params=pltpu.CompilerParams(vmem_limit_bytes=67043328),
        cost_estimate=pl.CostEstimate(flops=rows * 10**7, bytes_accessed=4 * 10**7, transcendentals=0),
        name="encode_back",
    )(feats, dkv, dq, enc, vec, w, own, sums, edge)


def row_norm(values):
    centred = values - jnp.mean(values, axis=-1, keepdims=True)
    inv = lax.rsqrt(jnp.mean(centred * centred, axis=-1, keepdims=True) + norm_eps)
    return centred * inv, inv


def norm_back(grad, norm, inv):
    return inv * (grad - jnp.mean(grad, axis=-1, keepdims=True) - norm * jnp.mean(grad * norm, axis=-1, keepdims=True))


def packed_dense_kernel(split, first, chunk, *refs):
    rows_down, rows_out = split
    packed, out_ref, up_ref, down_ref = refs[6], *refs[-3:]
    width = packed.shape[-1]

    @pl.when(pl.program_id(0) == 0)
    def _():
        for h in range(packed.shape[0]):
            for j in range(packed.shape[1]):
                k = h * packed.shape[1] + j
                down_ref[k * rows_down:(k + 1) * rows_down, :] = packed[h, j, :rows_down]
                for c in range(up_ref.shape[1] // width):
                    at = rows_down + c * rows_out
                    up_ref[k * rows_out:(k + 1) * rows_out, c * width:(c + 1) * width] = packed[h, j, at:at + rows_out]
                out_ref[k * rows_out:(k + 1) * rows_out, :] = packed[h, j, packed.shape[2] - rows_out:]

    dense_kernel(first, chunk, *refs[:6], out_ref, up_ref, down_ref, *refs[7:-3])


def dense_kernel(first, chunk, total_ref, attn_ref, feat_ref, side_ref, vec_ref, enc_ref, *refs):
    out_ref, up_ref, down_ref = refs[:3]
    refs = refs[3:]
    if not first:
        olds, refs = refs[:5], refs[5:]
    gattn_ref, ddown_ref, dup_ref, dout_ref, denc_ref, dvec_ref, u_ref, g_ref = refs
    i = pl.program_id(0)

    @pl.when(i == 0)
    def _():
        for n, ref in enumerate((ddown_ref, dup_ref, dout_ref, denc_ref, dvec_ref)):
            ref[...] = jnp.zeros_like(ref) if first else olds[n][...]

    heads = attn_ref.shape[0]
    ff = up_ref.shape[1]
    bias, gain_two, gain_three, head_vec = (vec_ref[r:r + 1, :] for r in range(4))
    target, live = side_ref[:, 0:1], side_ref[:, 1:2]
    attn = jnp.concatenate([attn_ref[h] for h in range(heads)], axis=1)
    feat = feat_ref[...]
    hidden_one = dotf(feat, enc_ref[...], NN) + bias + dotf(attn, out_ref[...], NN)
    norm_two, inv_two = row_norm(hidden_one)
    act_two = (norm_two * gain_two).astype(bf16)
    root = 0.7978845608028654
    acts = []
    for c in range(0, ff, chunk):
        u = dotf(act_two, up_ref[:, c:c + chunk], NN)
        square = u * u
        half = 0.5 * (1.0 + jnp.tanh(root * (u + 0.044715 * (u * square))))
        act = (u * half).astype(bf16)
        u_ref[:, c:c + chunk] = half + 2.0 * u * half * (1.0 - half) * (root * (1.0 + 0.134145 * square))
        g_ref[:, c:c + chunk] = act
    hidden_two = hidden_one + dotf(g_ref[...], down_ref[...], NN)
    norm_three, inv_three = row_norm(hidden_two)
    scaled = norm_three * gain_three
    error = jnp.sum(scaled * head_vec, axis=-1, keepdims=True) - target
    weighed = live * error
    grad_pred = 2.0 * weighed / total_ref[0]
    grad_two = norm_back(grad_pred * (head_vec * gain_three), norm_three, inv_three)
    low_two = grad_two.astype(bf16)
    act_two_t = act_two.T
    for c in range(0, ff, chunk):
        ddown_ref[c:c + chunk, :] += dotf(g_ref[:, c:c + chunk].T, low_two, NN)
        grad_up = (u_ref[:, c:c + chunk] * dotf(low_two, down_ref[c:c + chunk, :], NT)).astype(bf16)
        dup_ref[:, c:c + chunk] += dotf(act_two_t, grad_up, NN)
        g_ref[:, c:c + chunk] = grad_up
    grad_act_two = dotf(g_ref[...], up_ref[...], NT)
    grad_one = grad_two + norm_back(grad_act_two * gain_two, norm_two, inv_two)
    low_one = grad_one.astype(bf16)
    dout_ref[...] += dotf(attn.T, low_one, NN)
    denc_ref[...] += dotf(feat.T, low_one, NN)
    gattn = dotf(low_one, out_ref[...], NT).astype(bf16)
    width = gattn.shape[1] // heads
    for h in range(heads):
        gattn_ref[h] = gattn[:, h * width:(h + 1) * width]
    down = lambda a: jnp.sum(a, axis=0, keepdims=True)
    loss = jnp.broadcast_to(jnp.sum(weighed * error, axis=0, keepdims=True), (1, bias.shape[1]))
    dvec_ref[...] += jnp.concatenate(
        [down(grad_one), down(grad_act_two * norm_two), down(grad_pred * head_vec * norm_three), down(grad_pred * scaled), loss,
         jnp.zeros((3, bias.shape[1]), f32)], axis=0)


def dense(part, total, attn, feat, side, vec, enc, weights, ff, olds=None, tile=512, chunk=1024):
    heads, rows, cols = attn.shape
    width = enc.shape[1]
    per = rows // tile
    first = olds is None
    whole = lambda a: pl.BlockSpec(a.shape, lambda i: (0,) * a.ndim, pipeline_mode=pl.Buffered(1))
    keep = lambda s: pl.BlockSpec(s, lambda i: (0,) * len(s), pipeline_mode=pl.Buffered(1))
    shapes = [(ff, width), (width, ff), (width, width), (feat.shape[1], width), (8, width)]
    olds = () if first else tuple(olds)
    kernel, extra = dense_kernel, []
    if len(weights) == 1:
        pieces = weights[0].shape[0] * weights[0].shape[1]
        kernel = functools.partial(packed_dense_kernel, (ff // pieces, width // pieces))
        extra = [pltpu.VMEM((width, width), bf16), pltpu.VMEM((width, ff), bf16), pltpu.VMEM((ff, width), bf16)]
    return pl.pallas_call(
        functools.partial(kernel, first, chunk),
        grid=(per,),
        in_specs=[pl.BlockSpec(memory_space=pltpu.SMEM),
                  pl.BlockSpec((heads, tile, cols), lambda i: (0, i, 0)),
                  pl.BlockSpec((tile, feat.shape[1]), lambda i: (part * per + i, 0)),
                  pl.BlockSpec((tile, side.shape[1]), lambda i: (part * per + i, 0)),
                  whole(vec), whole(enc)] + [whole(w) for w in weights] + [whole(o) for o in olds],
        out_specs=[pl.BlockSpec((heads, tile, cols), lambda i: (0, i, 0))] + [keep(s) for s in shapes],
        out_shape=[jax.ShapeDtypeStruct((heads, rows, cols), bf16)] + [jax.ShapeDtypeStruct(s, f32) for s in shapes],
        scratch_shapes=[pltpu.VMEM((tile, ff), f32), pltpu.VMEM((tile, ff), bf16)] + extra,
        compiler_params=pltpu.CompilerParams(vmem_limit_bytes=67043328),
        cost_estimate=pl.CostEstimate(flops=rows * 5 * 10**7, bytes_accessed=3 * 10**7, transcendentals=0),
        name="dense",
    )(total, attn, feat, side, vec, enc, *weights, *olds)
MESH = pl.DeviceIdType.MESH


def front_kernel(nodes, heads, parts, feat, enc, qkv, vec, down, up, out, out_f, out_e, out_q, out_v, packed, up_s, up_r, down_s, down_r, halo_s, halo_r,
                 w_s, w_r, l_sem, down_v, up_v, out_v2):
    node, head = lax.axis_index("nodes"), lax.axis_index("heads")
    after, before = lax.rem(node + 1, nodes), lax.rem(node + nodes - 1, nodes)
    barrier = pltpu.get_barrier_semaphore()
    for other in (after, before):
        pl.semaphore_signal(barrier, inc=1, device_id=(other, head), device_id_type=MESH)
    for s in range(1, heads):
        pl.semaphore_signal(barrier, inc=1, device_id=(node, lax.rem(head + s, heads)), device_id_type=MESH)
    pl.semaphore_wait(barrier, heads + 1)

    rows = feat.shape[0] // parts
    cut = lambda k: pl.ds(k * rows, rows)

    def relay(step, k, upward):
        shard = jnp.clip(head - step if upward else head + step, 0, heads - 1)
        target = jnp.clip(head + 1 if upward else head - 1, 0, heads - 1)
        sems = (up_s, up_r) if upward else (down_s, down_r)
        src = feat.at[cut(k)] if step == 0 else out_f.at[1, shard, cut(k)]
        return pltpu.make_async_remote_copy(
            src_ref=src, dst_ref=out_f.at[1, shard, cut(k)], send_sem=sems[0].at[step, k], recv_sem=sems[1].at[step, k],
            device_id=(node, target), device_id_type=MESH)

    def halo(shard, k, src, way):
        return pltpu.make_async_remote_copy(
            src_ref=src, dst_ref=out_f.at[0 if way == 0 else 2, shard, cut(k)], send_sem=halo_s.at[way, shard, k], recv_sem=halo_r.at[way, shard, k],
            device_id=(after if way == 0 else before, head), device_id_type=MESH)

    def sends(step, upward):
        return (head - step >= 0) & (head + 1 <= heads - 1) if upward else (head + step <= heads - 1) & (head - 1 >= 0)

    def gets(step, upward):
        return head - 1 - step >= 0 if upward else head + 1 + step <= heads - 1

    for k in range(parts):
        for upward in (True, False):
            @pl.when(sends(0, upward))
            def _(k=k, upward=upward):
                relay(0, k, upward).start()
        for way in range(2):
            halo(head, k, feat.at[cut(k)], way).start()
    own = [pltpu.make_async_copy(feat, out_f.at[1, head], l_sem.at[0]),
           pltpu.make_async_copy(enc, out_e.at[head], l_sem.at[1]),
           pltpu.make_async_copy(qkv.at[head], out_q.at[head], l_sem.at[2]),
           pltpu.make_async_copy(vec, out_v.at[head], l_sem.at[3])]
    own += [pltpu.make_async_copy(src.at[node], dst, l_sem.at[4 + i]) for i, (src, dst) in enumerate(((down, down_v), (up, up_v), (out, out_v2)))]
    for copy in own:
        copy.start()
    for copy in own:
        copy.wait()
    width = out_v2.shape[1]
    rows_down, rows_out = down_v.shape[0], out_v2.shape[0]
    packed[:rows_down, :] = down_v[...].astype(bf16)
    at = rows_down
    for c in range(0, up_v.shape[1], width):
        packed[at:at + rows_out, :] = up_v[:, c:c + width].astype(bf16)
        at += rows_out
    packed[at:at + rows_out, :] = out_v2[...].astype(bf16)

    weights = []
    for step in range(heads - 1):
        if step == heads - 2:
            for s in range(1, heads):
                there = lax.rem(head + s, heads)
                for i, (src, dst) in enumerate(((enc, out_e.at[head]), (qkv.at[there], out_q.at[head]), (vec, out_v.at[head]))):
                    slot = (s - 1) * 3 + i
                    weights.append(pltpu.make_async_remote_copy(
                        src_ref=src, dst_ref=dst, send_sem=w_s.at[slot], recv_sem=w_r.at[slot], device_id=(node, there), device_id_type=MESH))
                    weights[-1].start()
        for k in range(parts):
            for upward in (True, False):
                @pl.when(gets(step, upward))
                def _(step=step, k=k, upward=upward):
                    relay(step, k, upward).wait_recv()
                    if step + 1 < heads - 1:
                        @pl.when(sends(step + 1, upward))
                        def _():
                            relay(step + 1, k, upward).start()
                    shard = head - 1 - step if upward else head + 1 + step
                    for way in range(2):
                        halo(shard, k, out_f.at[1, shard, cut(k)], way).start()
    for step in range(heads - 1):
        for k in range(parts):
            for upward in (True, False):
                @pl.when(sends(step, upward))
                def _(step=step, k=k, upward=upward):
                    relay(step, k, upward).wait_send()
    for copy in weights:
        copy.wait()
    for shard in range(heads):
        for k in range(parts):
            for way in range(2):
                halo(shard, k, feat.at[cut(k)], way).wait()


def front(feat, enc, qkv, vec, down, up, out, nodes, heads, parts=4):
    dma = pltpu.SemaphoreType.DMA
    vmem, anywhere = pl.BlockSpec(memory_space=pltpu.VMEM), pl.BlockSpec(memory_space=pl.ANY)
    n = 3 * (heads - 1)
    width = out.shape[2]
    rows = down.shape[1] + up.shape[1] * up.shape[2] // width + out.shape[1]
    return pl.pallas_call(
        functools.partial(front_kernel, nodes, heads, parts),
        in_specs=[vmem] * 4 + [anywhere] * 3, out_specs=[anywhere] + [vmem] * 4,
        out_shape=[jax.ShapeDtypeStruct((3, heads, *feat.shape), feat.dtype), jax.ShapeDtypeStruct((heads, *enc.shape), enc.dtype),
                   jax.ShapeDtypeStruct(qkv.shape, qkv.dtype), jax.ShapeDtypeStruct((heads, *vec.shape), vec.dtype),
                   jax.ShapeDtypeStruct((rows, width), bf16)],
        scratch_shapes=[dma((heads - 1, parts))] * 4 + [dma((2, heads, parts))] * 2 + [dma((n,))] * 2 + [dma((7,))]
        + [pltpu.VMEM(a.shape[1:], f32) for a in (down, up, out)],
        compiler_params=pltpu.CompilerParams(collective_id=2, has_side_effects=True, vmem_limit_bytes=67043328),
        name="front",
    )(feat, enc, qkv, vec, down, up, out)


def pair_kernel(nodes, heads, down, up, out, *refs):
    slabs, (got_d, got_u, got_o, own_d, own_u, own_o, s_sem, r_sem, l_sem) = refs[:nodes // 2], refs[nodes // 2:]
    node, head = lax.axis_index("nodes"), lax.axis_index("heads")
    chips = nodes // 2
    chip, side = lax.div(node, 2), lax.rem(node, 2)
    twin = chip * 2 + 1 - side
    barrier = pltpu.get_barrier_semaphore()
    pl.semaphore_signal(barrier, inc=1, device_id=(twin, head), device_id_type=MESH)
    pl.semaphore_wait(barrier, 1)
    moves = []
    for i, (src, got, own) in enumerate(((down, got_d, own_d), (up, got_u, own_u), (out, got_o, own_o))):
        local = pltpu.make_async_copy(src.at[:, :, side], own, l_sem.at[i])
        remote = pltpu.make_async_remote_copy(
            src_ref=src.at[:, :, 1 - side], dst_ref=got, send_sem=s_sem.at[i], recv_sem=r_sem.at[i], device_id=(twin, head), device_id_type=MESH)
        local.start()
        remote.start()
        moves.append((local, remote))
    width = out.shape[-1]
    at = 0
    for (local, remote), got, own in zip(moves, (got_d, got_u, got_o), (own_d, own_u, own_o)):
        local.wait()
        remote.wait()
        rows = own.shape[2]
        for c in range(0, own.shape[3], width):
            for s in range(chips):
                there = lax.rem(chip + s, chips)
                slabs[s][:, at:at + rows, :] = (own[:, there, :, c:c + width] + got[:, there, :, c:c + width]).astype(slabs[s].dtype)
            at += rows


def pair(down, up, out, nodes, heads):
    chips = nodes // 2
    split = lambda a: a.reshape(heads, chips, 2, -1, a.shape[-1])
    down, up, out = split(down), split(up), split(out)
    width = out.shape[-1]
    rows = sum(a.shape[3] * a.shape[4] // width for a in (down, up, out))
    half = [pltpu.VMEM((heads, chips, *a.shape[3:]), f32) for a in (down, up, out)]
    dma = pltpu.SemaphoreType.DMA
    return pl.pallas_call(
        functools.partial(pair_kernel, nodes, heads),
        in_specs=[pl.BlockSpec(memory_space=pl.ANY)] * 3, out_specs=[pl.BlockSpec(memory_space=pltpu.VMEM)] * chips,
        out_shape=[jax.ShapeDtypeStruct((heads, rows, width), bf16 if s else f32) for s in range(chips)],
        scratch_shapes=half + half + [dma((3,))] * 3,
        compiler_params=pltpu.CompilerParams(collective_id=3, has_side_effects=True, vmem_limit_bytes=67043328),
        cost_estimate=pl.CostEstimate(flops=10**10, bytes_accessed=2 * 10**7, transcendentals=0),
        name="pair",
    )(down, up, out)


def send(src, dst, sems, slot, node, head):
    copy = pltpu.make_async_remote_copy(
        src_ref=src, dst_ref=dst, send_sem=sems[0].at[slot], recv_sem=sems[1].at[slot], device_id=(node, head), device_id_type=MESH)
    copy.start()
    return copy


def greet(nodes, heads, node, head):
    barrier = pltpu.get_barrier_semaphore()
    for s in range(1, nodes):
        pl.semaphore_signal(barrier, inc=1, device_id=(lax.rem(node + s, nodes), head), device_id_type=MESH)
    for s in range(1, heads):
        pl.semaphore_signal(barrier, inc=1, device_id=(node, lax.rem(head + s, heads)), device_id_type=MESH)
    pl.semaphore_wait(barrier, nodes + heads - 2)


def finish_kernel(nodes, heads, *refs):
    (qkv, enc, vec, *bulk), refs = refs[:4], refs[4:]
    (out_q, out_e, out_v, *out_b), refs = refs[:4], refs[4:]
    (q_half, q_one, q_two, q_part, q_sum, q_own, e_half, e_one, e_two, e_sum, e_three, e_own, v_half, v_two, v_three, v_one, v_sum), refs = refs[:17], refs[17:]
    s_one, r_one, s_two, r_two, s_three, r_three, s_four, r_four, s_bulk, r_bulk, s_pass, r_pass, l_sem, piece = refs
    node, head = lax.axis_index("nodes"), lax.axis_index("heads")
    chips = nodes // 2
    chip, side = lax.div(node, 2), lax.rem(node, 2)
    twin = chip * 2 + 1 - side
    cuts = 3 if piece.shape[0] % 24 == 0 else 1
    step = piece.shape[0] // cuts
    piece[...] = functools.reduce(jnp.add, [bulk[0][h] for h in range(heads)])
    greet(nodes, heads, node, head)
    first = [send(ref.at[:, :, 1 - side], dst, (s_one, r_one), i, twin, head) for i, (ref, dst) in enumerate(((qkv, q_half), (enc, e_half)))]
    first.append(send(vec, v_half, (s_one, r_one), 2, twin, head))
    keep = [pltpu.make_async_copy(src, dst.at[node], l_sem.at[i]) for i, (src, dst) in enumerate(zip((piece,), out_b))]
    for copy in keep:
        copy.start()
    spread = {}

    def bulk_out(which):
        for k in which:
            for s in range(chips):
                other = lax.rem(chip + s, chips) * 2 + side if s else twin
                at = pl.ds(k * step, step)
                spread[k, s] = send(piece.at[at], out_b[0].at[node, at], (s_bulk, r_bulk), k * chips + s, other, head)

    bulk_out(range(1))
    for copy in first:
        copy.wait()
    q_one[...] = qkv[:, :, side] + q_half[...]
    e_one[...] = enc[:, :, side] + e_half[...]
    v_one[...] = vec[...] + v_half[...]
    second = []
    for s in range(1, chips):
        there = lax.rem(chip + s, chips)
        target = there * 2 + side
        i = (s - 1) * 3
        second.append(send(q_one.at[:, there], q_two.at[s - 1], (s_two, r_two), i, target, head))
        second.append(send(e_one.at[:, there], e_two.at[s - 1], (s_two, r_two), i + 1, target, head))
        second.append(send(v_one, v_two.at[s - 1], (s_two, r_two), i + 2, target, head))
    bulk_out(range(1, cuts))
    for copy in second:
        copy.wait()
    q_part[...] = functools.reduce(jnp.add, [q_two[s] for s in range(chips - 1)], q_one[:, chip])
    e_sum[...] = functools.reduce(jnp.add, [e_two[s] for s in range(chips - 1)], e_one[:, chip])
    v_sum[...] = functools.reduce(jnp.add, [v_two[s] for s in range(chips - 1)], v_one[...])
    third = []
    for s in range(1, heads):
        there = lax.rem(head + s, heads)
        i = (s - 1) * 3
        third.append(send(q_part.at[there], q_sum.at[head], (s_three, r_three), i, node, there))
        third.append(send(e_sum.at[there], e_three.at[s - 1], (s_three, r_three), i + 1, node, there))
        third.append(send(v_sum, v_three.at[s - 1], (s_three, r_three), i + 2, node, there))
    for copy in third:
        copy.wait()
    q_sum[pl.ds(head, 1)] = q_part[pl.ds(head, 1)]
    e_own[...] = functools.reduce(jnp.add, [e_three[s] for s in range(heads - 1)], e_sum[head])
    out_v[...] = functools.reduce(jnp.add, [v_three[s] for s in range(heads - 1)], v_sum[...])
    fourth = []
    for s in range(1, nodes):
        there = lax.rem(node + s, nodes)
        fourth.append(send(q_sum, out_q.at[node], (s_four, r_four), (s - 1) * 2, there, head))
        fourth.append(send(e_own, out_e.at[node], (s_four, r_four), (s - 1) * 2 + 1, there, head))
    out_q[node] = q_sum[...]
    out_e[node] = e_own[...]
    for copy in keep:
        copy.wait()
    passed = []
    for k in range(cuts):
        for s in range(chips):
            spread[k, s].wait()
            if s:
                origin = lax.rem(chip + chips - s, chips) * 2 + side
                here = out_b[0].at[origin, pl.ds(k * step, step)]
                passed.append(send(here, here, (s_pass, r_pass), k * (chips - 1) + s - 1, twin, head))
    for copy in passed:
        copy.wait()
    for copy in fourth:
        copy.wait()


def finish(qkv, enc, vec, bulk, nodes, heads):
    chips = nodes // 2
    split = lambda a: a.reshape(heads, chips, 2, -1, a.shape[-1])
    qkv, enc = split(qkv), split(enc)
    vm = lambda *s: pltpu.VMEM(s, f32)
    rq, wq, re, we = *qkv.shape[3:], *enc.shape[3:]
    dma = pltpu.SemaphoreType.DMA
    wv = vec.shape
    scratch = [vm(heads, chips, rq, wq), vm(heads, chips, rq, wq), vm(chips - 1, heads, rq, wq), vm(heads, rq, wq), vm(heads, rq, wq), vm(8, 128),
               vm(heads, chips, re, we), vm(heads, chips, re, we), vm(chips - 1, heads, re, we), vm(heads, re, we), vm(heads - 1, re, we), vm(re, we),
               vm(*wv), vm(chips - 1, *wv), vm(heads - 1, *wv), vm(*wv), vm(*wv)]
    counts = (3, 3, 3 * chips - 3, 3 * chips - 3, 3 * heads - 3, 3 * heads - 3, 2 * nodes - 2, 2 * nodes - 2, 3 * chips, 3 * chips, 3 * chips - 3, 3 * chips - 3, 1)
    out_shape = [jax.ShapeDtypeStruct(s, f32) for s in [(nodes, heads, rq, wq), (nodes, re, we), wv] + [(nodes, *b.shape[1:]) for b in bulk]]
    spec = pl.BlockSpec(memory_space=pltpu.VMEM)
    return pl.pallas_call(
        functools.partial(finish_kernel, nodes, heads),
        in_specs=[spec] * 4, out_specs=[spec] * 4, out_shape=out_shape,
        scratch_shapes=scratch + [dma((n,)) for n in counts] + [vm(*bulk[0].shape[1:])],
        compiler_params=pltpu.CompilerParams(collective_id=1, has_side_effects=True, vmem_limit_bytes=48 << 20),
        name="finish",
    )(qkv, enc, vec, *bulk)
D = 512
HEADS = 8
NBR = 8
ADAM_STEP = 3
highest = lax.Precision.HIGHEST
beta_one = 0.5
beta_two = 0.5
learn_rate = 0.02
weight_decay = 0.1
adam_eps = 1e-08


def adamw(weight, first_moment, second, gradient):
    first_new = beta_one * first_moment + (1.0 - beta_one) * gradient
    second_new = beta_two * second + (1.0 - beta_two) * gradient * gradient
    first_hat = first_new / (1.0 - beta_one**ADAM_STEP)
    second_hat = second_new / (1.0 - beta_two**ADAM_STEP)
    weight_new = weight - learn_rate * (
        first_hat / (jnp.sqrt(second_hat) + adam_eps) + weight_decay * weight
    )
    return (weight_new, first_new, second_new)


def local(
    features, target, counts, neighbours, edge_kinds,
    enc_weight, enc_first, enc_second, qkv_weight, qkv_first, qkv_second,
    out_weight, out_first, out_second, up_weight, up_first, up_second,
    down_weight, down_first, down_second, vec_weight, vec_first, vec_second,
):
    heads_count = lax.axis_size("heads")
    nodes_count = lax.axis_size("nodes")
    head_index = lax.axis_index("heads")
    node_index = lax.axis_index("nodes")
    row_count = features.shape[0]
    own_blocks = row_count // BLOCK
    group_blocks = own_blocks * heads_count
    group_rows = group_blocks * BLOCK
    hl = HEADS // heads_count
    hs = D // HEADS
    cols = hl * hs
    cp = -(-cols // 128) * 128
    ka = -(-(cols + 1) // 128) * 128
    kinds = D // HEADS
    slots = NBR + 1
    low = lambda a: a.astype(bf16)
    gather = lambda a, axis: lax.all_gather(low(a), "heads", axis=axis, tiled=True)

    qkv_parts = jnp.transpose(low(qkv_weight).reshape(-1, heads_count, hl, 3, hs), (1, 0, 3, 2, 4)).reshape(heads_count, -1, 3, cols)
    qkv_parts = jnp.pad(qkv_parts, ((0, 0), (0, 0), (0, 0), (0, cp - cols))).reshape(heads_count, -1, 3 * cp)
    vec_part = jnp.pad(low(vec_weight).astype(f32), ((0, 2), (0, 0)))
    ff = up_weight.shape[1]
    pieces = heads_count * nodes_count
    rows_down, rows_out = ff // pieces, D // pieces
    by_node = lambda a: a.reshape(nodes_count, -1, a.shape[1])
    feats, enc_b, qkv_cols, vectors, packed = front(
        features, low(enc_weight), qkv_parts, vec_part, by_node(down_weight), by_node(up_weight), by_node(out_weight), nodes_count, heads_count)
    feats = feats.reshape(3 * group_rows, -1)
    enc_b = enc_b.reshape(-1, D)
    qkv_cols = qkv_cols.reshape(D, 3 * cp)
    vectors = jnp.transpose(vectors, (1, 0, 2)).reshape(8, D)
    packed = lax.all_gather(packed, ("heads", "nodes"), axis=0, tiled=False).reshape(heads_count, nodes_count, -1, D)

    enc_bias, gain_one, gain_two, gain_three, head_vec = (vectors[r] for r in range(5))
    edge_local = lax.dynamic_slice_in_dim(vectors[5].reshape(kinds, HEADS), head_index * hl, hl, 1)
    own_counts = lax.dynamic_slice_in_dim(counts, (node_index * heads_count + head_index) * own_blocks, own_blocks)
    row_live = (jnp.arange(BLOCK, dtype=jnp.int32)[None, :] < own_counts[:, None]).reshape(row_count).astype(f32)
    live_total = jnp.sum(counts).astype(f32)

    def group_counts(offset):
        return lax.dynamic_slice_in_dim(counts, (node_index + offset) % nodes_count * group_blocks, group_blocks)

    pool_counts = jnp.concatenate([group_counts(nodes_count - 1), group_counts(0), group_counts(1)])
    relative = (neighbours // group_blocks - node_index + 1) % nodes_count
    nbr_pos = relative * group_blocks + neighbours % group_blocks
    self_pos = group_blocks + jnp.arange(group_blocks, dtype=jnp.int32)
    key_pos = jnp.concatenate([self_pos[:, None], nbr_pos], axis=1).reshape(-1)
    kind_hot = jax.nn.one_hot(edge_kinds, kinds, dtype=f32)
    slot_bias = jnp.einsum("bst,th->bsh", kind_hot, edge_local, precision=highest)
    bias_rows = jnp.repeat(slot_bias, BLOCK, axis=2)

    kaug, kt, value, vt, query = encode(
        pool_counts, feats, enc_b, enc_bias[None], gain_one[None], qkv_cols, cp, ka, cols, hs**-0.5)
    side = jnp.stack([target, row_live], axis=1)
    dense_vec = jnp.stack([enc_bias, gain_two, gain_three, head_vec])
    half = lambda a: a.reshape(heads_count, 2, row_count // 2, -1)
    exchange = lambda a: lax.all_to_all(a, "heads", split_axis=0, concat_axis=0, tiled=True)
    attn_parts, lse_parts, grad_parts, totals = [], [], [], None
    for part in range(2):
        attn_part, lse_part = attend(part, own_blocks, key_pos, query, bias_rows, kaug, vt, hl, hs)
        attn_parts.append(attn_part)
        lse_parts.append(lse_part)
    packed, attn_parts[1] = lax.optimization_barrier((packed, attn_parts[1]))
    weights = (packed,)
    if rows_out % 16:
        up_rows = packed[:, :, rows_down:-rows_out].reshape(pieces, -1, rows_out, D)
        weights = (packed[:, :, -rows_out:].reshape(D, D), jnp.transpose(up_rows, (0, 2, 1, 3)).reshape(D, ff), packed[:, :, :rows_down].reshape(ff, D))
    for part in range(2):
        attn_rows = exchange(attn_parts[part].reshape(heads_count, row_count // 2, cp)[..., :cols])
        grad_part, *totals = dense(part, live_total[None], attn_rows, features, side, dense_vec, enc_b, weights, ff, totals)
        grad_parts.append(exchange(grad_part))
    grad_down, grad_up, grad_out, denc_own, dense_sums = totals
    grad_parts[0], grad_down = lax.optimization_barrier((grad_parts[0], grad_down))
    slab = pair(grad_down, grad_up, grad_out, nodes_count, heads_count)
    moved = [slab[0]] + [
        lax.ppermute(slab[s], "nodes", [(i, (i + 2 * s) % nodes_count) for i in range(nodes_count)]) for s in range(1, nodes_count // 2)]
    grad_heads = [jnp.pad(g.reshape(group_rows // 2, cols), ((0, 0), (0, cp - cols))) for g in grad_parts]
    dq, dkv, edge_sums = attend_back(own_blocks, key_pos, query, grad_heads, attn_parts, lse_parts, bias_rows, kaug, value, kt, hl, hs)
    moved, dkv = lax.optimization_barrier((moved, dkv))
    planes = exchange(functools.reduce(jnp.add, [a.astype(f32) for a in moved]))
    slot_sums = jnp.sum(edge_sums.reshape(group_blocks, slots, hl, BLOCK), axis=3)
    edge_grad = jnp.einsum("bst,bsh->th", kind_hot, slot_sums, precision=highest)
    edge_full = lax.dynamic_update_slice(jnp.zeros((kinds, HEADS), f32), edge_grad, (jnp.int32(0), head_index * hl)).reshape(1, D)
    dw, grad_enc, grad_vec = encode_back(feats, dkv, dq, enc_b, vectors, qkv_cols, denc_own, dense_sums, edge_full)
    planes, dw = lax.optimization_barrier((planes, dw))
    dw_sum, enc_sum, vec_total, bulk = finish(dw, grad_enc, grad_vec, [planes], nodes_count, heads_count)
    total_loss = vec_total[5, 0]
    vec_sum = lax.dynamic_slice_in_dim(jnp.concatenate([vec_total[:5], vec_total[6:7]]), head_index * (D // heads_count), D // heads_count, 1)
    states = (enc_weight, enc_first, enc_second, qkv_weight, qkv_first, qkv_second, out_weight, out_first, out_second,
              up_weight, up_first, up_second, down_weight, down_first, down_second)
    vec_res = adamw(vec_weight, vec_first, vec_second, vec_sum)
    if rows_out % 16:
        qkv_sum = jnp.transpose(dw_sum, (0, 2, 1, 3)).reshape(-1, heads_count, 3, cp)[..., :cols].reshape(-1, heads_count, 3, hl, hs)
        qkv_sum = jnp.transpose(qkv_sum, (0, 1, 3, 2, 4)).reshape(qkv_weight.shape)
        flat = lambda a: a.reshape(-1, a.shape[-1])
        up_sum = bulk[:, rows_down:-rows_out].reshape(nodes_count, -1, rows_out, D)
        up_sum = jnp.transpose(up_sum, (0, 2, 1, 3)).reshape(up_weight.shape)
        summed = (flat(enc_sum), qkv_sum, flat(bulk[:, -rows_out:]), up_sum, flat(bulk[:, :rows_down]))
        results = []
        for n, grad in enumerate(summed):
            results += adamw(*states[3 * n:3 * n + 3], grad)
        results += [low(r) for r in results[::3]]
    else:
        results = adam(enc_sum, dw_sum, bulk, states, hl, hs, cp)
    loss_value = (total_loss / live_total).reshape(1)
    return (loss_value, *results[:15], *vec_res, *results[15:])


def solution(mesh):
    rows = P("heads", None)
    both = P(("nodes", "heads"))
    lanes = P(None, "heads")
    in_specs = (P(("nodes", "heads"), None), both, P(), P("nodes", None), P("nodes", None)) + (rows,) * 15 + (lanes,) * 3
    out_specs = (P(),) + (rows,) * 15 + (lanes,) * 3 + (rows,) * 5
    return jax.shard_map(local, mesh=mesh, in_specs=in_specs, out_specs=out_specs, check_vma=False)


def adam_kernel(hl, hs, cp, *refs):
    g_enc, g_qkv, g_bulk = refs[:3]
    ins, outs = refs[3:18], refs[18:]
    rows_down, rows_out = ins[12].shape[0], ins[6].shape[0]
    heads = g_qkv.shape[1]
    bulk = g_bulk[0]
    parts = []
    for h in range(heads):
        part = g_qkv[0, h]
        for k in range(hl):
            parts += [part[:, j * cp + k * hs:j * cp + (k + 1) * hs] for j in range(3)]
    up_at = lambda c: rows_down + c * rows_out
    grads = [g_enc[0], jnp.concatenate(parts, axis=1), bulk[-rows_out:],
             jnp.concatenate([bulk[up_at(c):up_at(c) + rows_out] for c in range(ins[9].shape[1] // bulk.shape[1])], axis=1), bulk[:rows_down]]
    for n, grad in enumerate(grads):
        new = adamw(*(ref[...] for ref in ins[3 * n:3 * n + 3]), grad)
        for ref, value in zip(outs[3 * n:3 * n + 3], new):
            ref[...] = value
        outs[15 + n][...] = new[0].astype(bf16)


def adam(g_enc, g_qkv, g_bulk, states, hl, hs, cp):
    nodes = g_enc.shape[0]
    rows = lambda a: pl.BlockSpec((a.shape[0] // nodes, a.shape[1]), lambda i: (i, 0))
    lead = lambda a: pl.BlockSpec((1, *a.shape[1:]), lambda i: (i,) + (0,) * (a.ndim - 1))
    shapes = [jax.ShapeDtypeStruct(a.shape, f32) for a in states] + [jax.ShapeDtypeStruct(a.shape, bf16) for a in states[::3]]
    return pl.pallas_call(
        functools.partial(adam_kernel, hl, hs, cp),
        grid=(nodes,),
        in_specs=[lead(g_enc), lead(g_qkv), lead(g_bulk)] + [rows(a) for a in states],
        out_specs=[rows(a) for a in shapes], out_shape=shapes,
        compiler_params=pltpu.CompilerParams(vmem_limit_bytes=67043328),
        name="adam",
    )(g_enc, g_qkv, g_bulk, *states)
```

```python
import functools

import jax
import jax.numpy as jnp
from jax import lax
from jax.experimental import pallas as pl
from jax.experimental.pallas import tpu as pltpu
from jax.sharding import PartitionSpec as P

BLOCK = 128
NT = (((1,), (1,)), ((), ()))
NN = (((1,), (0,)), ((), ()))
f32 = jnp.float32
bf16 = jnp.bfloat16


def dotf(a, b, dims):
    return lax.dot_general(a, b, dims, preferred_element_type=f32)


def head_rows(x, hl, hs, cp):
    if hl == 1:
        return x
    lane = lax.broadcasted_iota(jnp.int32, (BLOCK, cp), 1)
    zero = jnp.zeros_like(x)
    return jnp.concatenate([jnp.where(lane // hs == h, x, zero) for h in range(hl)], axis=0)


def ones_lane(hl, cp, ka):
    rows = hl * BLOCK
    lane = lax.broadcasted_iota(jnp.int32, (rows, ka - cp), 1)
    return jnp.where(lane == 0, 1.0, 0.0).astype(bf16)


def attend_kernel(hl, hs, cp, ka, slots, unit, unit_of, pos_ref, q_ref, brow_ref, kaug_ref, vt_ref, o_ref, lse_ref, *scratch):
    first = unit_of(pl.program_id(0)) * unit
    rows = hl * BLOCK

    def spot(u, s):
        return pos_ref[(first + u) * slots + s]

    def score(u):
        s_ref = scratch[2 * (u % 2)]
        q2 = head_rows(q_ref[u * BLOCK:(u + 1) * BLOCK, :], hl, hs, cp)
        qa = jnp.concatenate([q2, ones_lane(hl, cp, ka)], axis=1) if ka > cp else q2
        keys = [kaug_ref[pl.ds(pl.multiple_of(spot(u, s) * BLOCK, BLOCK), BLOCK), :] for s in range(slots)]
        scores = dotf(jnp.concatenate(keys, axis=0), qa, NT)
        top = None
        for s in range(slots):
            sc = scores[s * BLOCK:(s + 1) * BLOCK]
            s_ref[s] = sc
            t = jnp.max(sc, axis=0, keepdims=True) + brow_ref[u, s:s + 1, :]
            top = t if top is None else jnp.maximum(top, t)
        return top

    def weigh(u, top):
        s_ref, p_ref = scratch[2 * (u % 2):2 * (u % 2) + 2]
        tot = jnp.zeros((1, rows), f32)
        for s in range(slots):
            e = jnp.exp(s_ref[s] - (top - brow_ref[u, s:s + 1, :]))
            s_ref[s] = e
            tot = tot + jnp.sum(e, axis=0, keepdims=True)
        lse_ref[u] = top + jnp.log(tot)
        inv = 1.0 / tot
        for s in range(slots):
            p_ref[s * BLOCK:(s + 1) * BLOCK, :] = (s_ref[s] * inv).astype(bf16)

    def total(u):
        p_ref = scratch[2 * (u % 2) + 1]
        ot = dotf(jnp.concatenate([vt_ref[spot(u, s)] for s in range(slots)], axis=1), p_ref[...], NN)
        parts = [ot[h * hs:(h + 1) * hs, h * BLOCK:(h + 1) * BLOCK] for h in range(hl)]
        if hl * hs < cp:
            parts.append(jnp.zeros((cp - hl * hs, BLOCK), f32))
        o_ref[u * BLOCK:(u + 1) * BLOCK, :] = jnp.concatenate(parts, axis=0).T.astype(bf16)

    top = score(0)
    for u in range(unit):
        following = score(u + 1) if u + 1 < unit else None
        weigh(u, top)
        total(u)
        top = following


def attend(part, own, pos, q, brow, kaug, vt, hl, hs, unit=4):
    cp, ka = q.shape[1], kaug.shape[1]
    nb = q.shape[0] // BLOCK // 2
    half, own = own // 2 // unit, own // unit
    unit_of = lambda i: lax.div(i, half) * own + part * half + lax.rem(i, half)
    slots = brow.shape[1]
    rows = hl * BLOCK
    whole = lambda a: pl.BlockSpec(a.shape, lambda i, *_: (0,) * a.ndim, pipeline_mode=pl.Buffered(1))
    return pl.pallas_call(
        functools.partial(attend_kernel, hl, hs, cp, ka, slots, unit, unit_of),
        grid_spec=pltpu.PrefetchScalarGridSpec(
            num_scalar_prefetch=1, grid=(nb // unit,),
            in_specs=[pl.BlockSpec((unit * BLOCK, cp), lambda i, *_: (unit_of(i), 0)),
                      pl.BlockSpec((unit, slots, rows), lambda i, *_: (unit_of(i), 0, 0)),
                      whole(kaug), whole(vt)],
            out_specs=[pl.BlockSpec((unit * BLOCK, cp), lambda i, *_: (i, 0)),
                       pl.BlockSpec((unit, 1, rows), lambda i, *_: (i, 0, 0))],
            scratch_shapes=[pltpu.VMEM((slots, BLOCK, rows), f32), pltpu.VMEM((slots * BLOCK, rows), bf16)] * 2),
        out_shape=[jax.ShapeDtypeStruct((nb * BLOCK, cp), bf16), jax.ShapeDtypeStruct((nb, 1, rows), f32)],
        cost_estimate=pl.CostEstimate(flops=nb * 10**9, bytes_accessed=3 * 10**7, transcendentals=0),
        compiler_params=pltpu.CompilerParams(vmem_limit_bytes=67043328),
        name="attend",
    )(pos, q, brow, kaug, vt)


def attend_back_kernel(hl, hs, cp, ka, slots, scale, unit, unit_of, pos_ref, q_ref, da_ref, db_ref, oa_ref, ob_ref, la_ref, lb_ref, brow_ref, kaug_ref, v_ref,
                       kt_ref, dq_ref, dkv_ref, edge_ref, *scratch):
    i = pl.program_id(0)
    first = unit_of(i) * unit
    late = i >= pl.num_programs(0) // 2

    @pl.when(i == 0)
    def _():
        @pl.loop(0, dkv_ref.shape[0] // BLOCK)
        def _(n):
            dkv_ref[pl.ds(pl.multiple_of(n * BLOCK, BLOCK), BLOCK), :] = jnp.zeros((BLOCK, dkv_ref.shape[1]), f32)

    for u in range(unit):
        p_ref, d_ref = scratch[2 * (u % 2):2 * (u % 2) + 2]
        own = slice(u * BLOCK, (u + 1) * BLOCK)
        q2 = head_rows(q_ref[own, :], hl, hs, cp)
        qa = jnp.concatenate([q2, ones_lane(hl, cp, ka)], axis=1) if ka > cp else q2
        do = jnp.where(late, db_ref[own, :], da_ref[own, :])
        do2 = head_rows(do, hl, hs, cp)
        prod = (do.astype(f32) * jnp.where(late, ob_ref[own, :], oa_ref[own, :]).astype(f32)).T
        dd = jnp.concatenate([jnp.sum(prod[h * hs:(h + 1) * hs], axis=0, keepdims=True) for h in range(hl)], axis=1)
        lse = jnp.where(late, lb_ref[u], la_ref[u])
        blocks = [pos_ref[(first + u) * slots + s] for s in range(slots)]
        spots = [pl.ds(pl.multiple_of(p * BLOCK, BLOCK), BLOCK) for p in blocks]
        scores = dotf(jnp.concatenate([kaug_ref[at, :] for at in spots], axis=0), qa, NT)
        grads = dotf(jnp.concatenate([v_ref[at, :] for at in spots], axis=0), do2, NT)
        for s in range(slots):
            here = slice(s * BLOCK, (s + 1) * BLOCK)
            pr = jnp.exp(scores[here] - (lse - brow_ref[u, s:s + 1, :]))
            ds = pr * (grads[here] - dd)
            edge_ref[u, s:s + 1, :] = jnp.sum(ds, axis=0, keepdims=True)
            p_ref[here, :] = pr.astype(bf16)
            d_ref[here, :] = ds.astype(bf16)
        dv = dotf(p_ref[...], do2, NN)
        dk = dotf(d_ref[...], q2, NN)
        dqt = dotf(jnp.concatenate([kt_ref[p] for p in blocks], axis=1), d_ref[...], NN)
        for s, at in enumerate(spots):
            here = slice(s * BLOCK, (s + 1) * BLOCK)
            dkv_ref[at, 0:cp] += dk[here]
            dkv_ref[at, cp:2 * cp] += dv[here]
        parts = [dqt[h * hs:(h + 1) * hs, h * BLOCK:(h + 1) * BLOCK] for h in range(hl)]
        if hl * hs < cp:
            parts.append(jnp.zeros((cp - hl * hs, BLOCK), f32))
        dq_ref[own, :] = (jnp.concatenate(parts, axis=0).T * scale).astype(bf16)


def attend_back(own, pos, q, dos, outs, lses, brow, kaug, v, kt, hl, hs, unit=4):
    cp, ka = q.shape[1], kaug.shape[1]
    nb = q.shape[0] // BLOCK
    slots = brow.shape[1]
    rows = hl * BLOCK
    half, mid, own = own // 2 // unit, nb // 2 // unit, own // unit
    unit_of = lambda i: lax.div(lax.rem(i, mid), half) * own + lax.div(i, mid) * half + lax.rem(i, half)
    whole = lambda a: pl.BlockSpec(a.shape, lambda i, *_: (0,) * a.ndim, pipeline_mode=pl.Buffered(1))
    tile = pl.BlockSpec((unit * BLOCK, cp), lambda i, *_: (unit_of(i), 0))
    early = lambda i: jnp.minimum(i, mid - 1)
    late = lambda i: jnp.maximum(i - mid, 0)
    return pl.pallas_call(
        functools.partial(attend_back_kernel, hl, hs, cp, ka, slots, hs ** -0.5, unit, unit_of),
        grid_spec=pltpu.PrefetchScalarGridSpec(
            num_scalar_prefetch=1, grid=(nb // unit,),
            in_specs=[tile] + [pl.BlockSpec((unit * BLOCK, cp), lambda i, *_: (early(i), 0)), pl.BlockSpec((unit * BLOCK, cp), lambda i, *_: (late(i), 0))] * 2 + [
                      pl.BlockSpec((unit, 1, rows), lambda i, *_: (early(i), 0, 0)), pl.BlockSpec((unit, 1, rows), lambda i, *_: (late(i), 0, 0)),
                      pl.BlockSpec((unit, slots, rows), lambda i, *_: (unit_of(i), 0, 0)),
                      whole(kaug), whole(v), whole(kt)],
            out_specs=[tile, pl.BlockSpec((v.shape[0], 2 * cp), lambda i, *_: (0, 0), pipeline_mode=pl.Buffered(1)),
                       pl.BlockSpec((unit, slots, rows), lambda i, *_: (unit_of(i), 0, 0))],
            scratch_shapes=[pltpu.VMEM((slots * BLOCK, rows), bf16)] * 4),
        out_shape=[jax.ShapeDtypeStruct(q.shape, bf16), jax.ShapeDtypeStruct((v.shape[0], 2 * cp), f32),
                   jax.ShapeDtypeStruct((nb, slots, rows), f32)],
        cost_estimate=pl.CostEstimate(flops=nb * 2 * 10**9, bytes_accessed=6 * 10**7, transcendentals=0),
        compiler_params=pltpu.CompilerParams(vmem_limit_bytes=67043328),
        name="attend_back",
    )(pos, q, *dos, *outs, *lses, brow, kaug, v, kt)
norm_eps = 1e-05


def over(count):
    return (lambda body: body(0)) if count == 1 else pl.loop(0, count)


def encode_kernel(cp, ka, cols, scale, per_group, inner, cnt_ref, x_all, enc_ref, bias_ref, gain_ref, w_ref,
                  kaug_all, kt_all, v_all, vt_all, q_all):
    @over(x_all.shape[0] // inner)
    def _(n):
        rows = pl.ds(n * inner if isinstance(n, int) else pl.multiple_of(n * inner, inner), inner)
        blocks = pl.ds(n * (inner // BLOCK), inner // BLOCK)
        encode_rows(cp, ka, cols, scale, per_group, pl.program_id(0), n, x_all.shape[0] // inner, cnt_ref, x_all.at[rows], enc_ref, bias_ref, gain_ref,
                    w_ref, kaug_all.at[rows], kt_all.at[blocks], v_all.at[rows], vt_all.at[blocks], q_all.at[rows])


def encode_rows(cp, ka, cols, scale, per_group, i, n, count, cnt_ref, x_ref, enc_ref, bias_ref, gain_ref, w_ref,
                kaug_ref, kt_ref, v_ref, vt_ref, q_ref):
    group = i // per_group
    tile = x_ref.shape[0]
    resid = dotf(x_ref[...], enc_ref[...], NN) + bias_ref[...]
    centred = resid - jnp.mean(resid, axis=-1, keepdims=True)
    variance = jnp.mean(centred * centred, axis=-1, keepdims=True)
    act = (centred * lax.rsqrt(variance + norm_eps) * gain_ref[...]).astype(bf16)
    kv = dotf(act, w_ref[:, cp:], NN).astype(bf16)
    key, value = kv[:, :cp], kv[:, cp:]
    row = lax.broadcasted_iota(jnp.int32, (BLOCK, 128), 0)
    lane = lax.broadcasted_iota(jnp.int32, (BLOCK, 128), 1)
    first = (i * count + n) * (tile // BLOCK)
    dead = jnp.concatenate(
        [jnp.where((row >= cnt_ref[first + j]) & (lane == cols % 128), -1e30, 0.0) for j in range(tile // BLOCK)], axis=0).astype(bf16)
    if ka > cp:
        kaug_ref[:, :cp] = key
        kaug_ref[:, cp:] = dead
    else:
        kaug_ref[...] = key + dead
    v_ref[...] = value
    for j in range(tile // BLOCK):
        kt_ref[j] = key[j * BLOCK:(j + 1) * BLOCK].T
        vt_ref[j] = value[j * BLOCK:(j + 1) * BLOCK].T

    @pl.when(group == 1)
    def _():
        q = (dotf(act, w_ref[:, :cp], NN) * scale).astype(bf16)
        if ka == cp:
            lanes = lax.broadcasted_iota(jnp.int32, q.shape, 1)
            q = jnp.where(lanes == cols, jnp.ones_like(q), q)
        q_ref[...] = q


def encode(counts, feats, enc, bias, gain, w, cp, ka, cols, scale, tile=2048):
    rows, feat = feats.shape[0] // 3, feats.shape[1]
    width = enc.shape[1]
    per = rows // tile
    blocks = tile // BLOCK
    whole = lambda a: pl.BlockSpec(a.shape, lambda i, *_: (0,) * a.ndim, pipeline_mode=pl.Buffered(1))
    return pl.pallas_call(
        functools.partial(encode_kernel, cp, ka, cols, scale, per, 2048),
        grid_spec=pltpu.PrefetchScalarGridSpec(
            num_scalar_prefetch=1, grid=(3 * per,),
            in_specs=[pl.BlockSpec((tile, feat), lambda i, *_: (i, 0)), whole(enc), whole(bias), whole(gain), whole(w)],
            out_specs=[pl.BlockSpec((tile, ka), lambda i, *_: (i, 0)),
                       pl.BlockSpec((blocks, cp, BLOCK), lambda i, *_: (i, 0, 0)),
                       pl.BlockSpec((tile, cp), lambda i, *_: (i, 0)),
                       pl.BlockSpec((blocks, cp, BLOCK), lambda i, *_: (i, 0, 0)),
                       pl.BlockSpec((tile, cp), lambda i, *_: (jnp.clip(i - per, 0, per - 1), 0))]),
        out_shape=[jax.ShapeDtypeStruct((3 * rows, ka), bf16),
                   jax.ShapeDtypeStruct((3 * rows // BLOCK, cp, BLOCK), bf16),
                   jax.ShapeDtypeStruct((3 * rows, cp), bf16),
                   jax.ShapeDtypeStruct((3 * rows // BLOCK, cp, BLOCK), bf16),
                   jax.ShapeDtypeStruct((rows, cp), bf16)],
        compiler_params=pltpu.CompilerParams(vmem_limit_bytes=67043328),
        cost_estimate=pl.CostEstimate(flops=rows * 6 * 10**6, bytes_accessed=3 * 10**7, transcendentals=0),
        name="encode",
    )(counts, feats, enc, bias, gain, w)


def encode_back_kernel(cp, per_group, inner, x_all, dkv_all, dq_all, enc_ref, vec_ref, w_ref, own_ref, sums_ref, edge_ref,
                       dw_ref, denc_ref, dvec_ref, g_ref, enct_ref, bias_ref, gain_ref, denct_ref, dgain_ref, dbias_ref):
    i = pl.program_id(0)

    @pl.when(i == 0)
    def _():
        for ref in (dw_ref, denct_ref, dgain_ref, dbias_ref):
            ref[...] = jnp.zeros_like(ref)
        enct_ref[...] = enc_ref[...].T
        for r, ref in enumerate((bias_ref, gain_ref)):
            ref[...] = jnp.broadcast_to(vec_ref[r:r + 1, :], (128, vec_ref.shape[1])).T

    @over(x_all.shape[0] // inner)
    def _(n):
        rows = pl.ds(n * inner if isinstance(n, int) else pl.multiple_of(n * inner, inner), inner)
        encode_back_rows(cp, i // per_group, x_all.at[rows], dkv_all.at[rows], dq_all.at[rows], enct_ref, bias_ref, gain_ref, w_ref,
                         dw_ref, denct_ref, dgain_ref, dbias_ref, g_ref)

    @pl.when(i == pl.num_programs(0) - 1)
    def _():
        denc_ref[...] = denct_ref[...].T + own_ref[...]
        line = lambda ref: jnp.sum(ref[...].T, axis=0, keepdims=True)
        dvec_ref[...] = jnp.concatenate(
            [line(dbias_ref) + sums_ref[0:1, :], line(dgain_ref), sums_ref[1:5, :], edge_ref[...], jnp.zeros_like(edge_ref[...])], axis=0)


def encode_back_rows(cp, group, x_ref, dkv_ref, dq_ref, enct_ref, bias_ref, gain_ref, w_ref,
                     dw_ref, denc_ref, dgain_ref, dbias_ref, g_ref):
    tile = x_ref.shape[0]
    width = enct_ref.shape[0]
    reps = tile // 128

    x = x_ref[...]
    wide = lambda c: jnp.concatenate([c] * reps, axis=1)
    fold = lambda a: functools.reduce(jnp.add, [a[:, r * 128:(r + 1) * 128] for r in range(reps)])
    resid = dotf(enct_ref[...], x, NT) + wide(bias_ref[...])
    centred = resid - jnp.sum(resid, axis=0, keepdims=True) * (1.0 / width)
    variance = jnp.sum(centred * centred, axis=0, keepdims=True) * (1.0 / width)
    inv = lax.rsqrt(variance + norm_eps)
    norm = centred * inv
    gain = wide(gain_ref[...])
    act = (norm * gain).astype(bf16)
    dkv = dkv_ref[...].astype(bf16)
    g_ref[...] = dotf(w_ref[:, cp:], dkv, NT)
    dw_ref[:, cp:] += dotf(act, dkv, NN)

    @pl.when(group == 1)
    def _():
        dq = dq_ref[...]
        g_ref[...] += dotf(w_ref[:, :cp], dq, NT)
        dw_ref[:, :cp] += dotf(act, dq, NN)

    grad = g_ref[...]
    dgain_ref[...] += fold(grad * norm)
    back = grad * gain
    mean_one = jnp.sum(back, axis=0, keepdims=True) * (1.0 / width)
    mean_two = jnp.sum(back * norm, axis=0, keepdims=True) * (1.0 / width)
    din = inv * (back - mean_one - norm * mean_two)
    dbias_ref[...] += fold(din)
    denc_ref[...] += dotf(din.astype(bf16), x, NN)


def encode_back(feats, dkv, dq, enc, vec, w, own, sums, edge, tile=2048, inner=2048):
    rows, feat = feats.shape[0] // 3, feats.shape[1]
    width = enc.shape[1]
    cp = dq.shape[1]
    per = rows // tile
    whole = lambda a: pl.BlockSpec(a.shape, lambda i: (0,) * a.ndim, pipeline_mode=pl.Buffered(1))
    keep = lambda s: pl.BlockSpec(s, lambda i: (0,) * len(s), pipeline_mode=pl.Buffered(1))
    shapes = [(width, 3 * cp), (feat, width), (8, width)]
    column = pltpu.VMEM((width, 128), f32)
    return pl.pallas_call(
        functools.partial(encode_back_kernel, cp, per, inner),
        grid=(3 * per,),
        in_specs=[pl.BlockSpec((tile, feat), lambda i: (i, 0)), pl.BlockSpec((tile, 2 * cp), lambda i: (i, 0)),
                  pl.BlockSpec((tile, cp), lambda i: (jnp.clip(i - per, 0, per - 1), 0))] + [whole(a) for a in (enc, vec, w, own, sums, edge)],
        out_specs=[keep(s) for s in shapes],
        out_shape=[jax.ShapeDtypeStruct(s, f32) for s in shapes],
        scratch_shapes=[pltpu.VMEM((width, inner), f32), pltpu.VMEM((width, feat), bf16), column, column, pltpu.VMEM((width, feat), f32), column, column],
        compiler_params=pltpu.CompilerParams(vmem_limit_bytes=67043328),
        cost_estimate=pl.CostEstimate(flops=rows * 10**7, bytes_accessed=4 * 10**7, transcendentals=0),
        name="encode_back",
    )(feats, dkv, dq, enc, vec, w, own, sums, edge)


def row_norm(values):
    centred = values - jnp.mean(values, axis=-1, keepdims=True)
    inv = lax.rsqrt(jnp.mean(centred * centred, axis=-1, keepdims=True) + norm_eps)
    return centred * inv, inv


def norm_back(grad, norm, inv):
    return inv * (grad - jnp.mean(grad, axis=-1, keepdims=True) - norm * jnp.mean(grad * norm, axis=-1, keepdims=True))


def packed_dense_kernel(split, first, part, chunk, *refs):
    rows_down, rows_out = split
    packed, out_ref, up_ref, down_ref = refs[7], *refs[-3:]
    width = packed.shape[-1]

    @pl.when(pl.program_id(0) == 0)
    def _():
        for h in range(packed.shape[0]):
            for j in range(packed.shape[1]):
                k = h * packed.shape[1] + j
                down_ref[k * rows_down:(k + 1) * rows_down, :] = packed[h, j, :rows_down]
                for c in range(up_ref.shape[1] // width):
                    at = rows_down + c * rows_out
                    up_ref[k * rows_out:(k + 1) * rows_out, c * width:(c + 1) * width] = packed[h, j, at:at + rows_out]
                out_ref[k * rows_out:(k + 1) * rows_out, :] = packed[h, j, packed.shape[2] - rows_out:]

    dense_kernel(first, part, chunk, *refs[:7], out_ref, up_ref, down_ref, *refs[8:-3])


def dense_kernel(first, part, chunk, own_ref, counts_ref, attn_ref, feat_ref, target_ref, vec_ref, enc_ref, *refs):
    out_ref, up_ref, down_ref = refs[:3]
    refs = refs[3:]
    if not first:
        olds, refs = refs[:5], refs[5:]
    gattn_ref, ddown_ref, dup_ref, dout_ref, denc_ref, dvec_ref, u_ref, g_ref = refs
    i = pl.program_id(0)

    @pl.when(i == 0)
    def _():
        for n, ref in enumerate((ddown_ref, dup_ref, dout_ref, denc_ref, dvec_ref)):
            ref[...] = jnp.zeros_like(ref) if first else olds[n][...]

    heads = attn_ref.shape[0]
    ff = up_ref.shape[1]
    bias, gain_two, gain_three, head_vec = (vec_ref[r:r + 1, :] for r in (0, 2, 3, 4))
    total = jnp.sum(counts_ref[...].astype(f32))
    blocks = target_ref.shape[1]
    turned = jnp.concatenate([target_ref[0]] + [jnp.zeros((8 - blocks % 8, BLOCK), f32)] * (blocks % 8 > 0), axis=0).T
    target = jnp.concatenate([turned[:, r:r + 1] for r in range(blocks)], axis=0)
    slot = lax.broadcasted_iota(jnp.int32, (BLOCK, 1), 0)
    block = (part * pl.num_programs(0) + i) * blocks
    live = jnp.concatenate([jnp.where(slot < own_ref[block + r], 1.0, 0.0) for r in range(blocks)], axis=0)
    attn = jnp.concatenate([attn_ref[h] for h in range(heads)], axis=1)
    feat = feat_ref[...]
    hidden_one = dotf(feat, enc_ref[...], NN) + bias + dotf(attn, out_ref[...], NN)
    norm_two, inv_two = row_norm(hidden_one)
    act_two = (norm_two * gain_two).astype(bf16)
    root = 0.7978845608028654
    acts = []
    for c in range(0, ff, chunk):
        u = dotf(act_two, up_ref[:, c:c + chunk], NN)
        square = u * u
        half = 0.5 * (1.0 + jnp.tanh(root * (u + 0.044715 * (u * square))))
        act = (u * half).astype(bf16)
        u_ref[:, c:c + chunk] = half + 2.0 * u * half * (1.0 - half) * (root * (1.0 + 0.134145 * square))
        g_ref[:, c:c + chunk] = act
    hidden_two = hidden_one + dotf(g_ref[...], down_ref[...], NN)
    norm_three, inv_three = row_norm(hidden_two)
    scaled = norm_three * gain_three
    error = jnp.sum(scaled * head_vec, axis=-1, keepdims=True) - target
    weighed = live * error
    grad_pred = 2.0 * weighed / total
    grad_two = norm_back(grad_pred * (head_vec * gain_three), norm_three, inv_three)
    low_two = grad_two.astype(bf16)
    act_two_t = act_two.T
    for c in range(0, ff, chunk):
        ddown_ref[c:c + chunk, :] += dotf(g_ref[:, c:c + chunk].T, low_two, NN)
        grad_up = (u_ref[:, c:c + chunk] * dotf(low_two, down_ref[c:c + chunk, :], NT)).astype(bf16)
        dup_ref[:, c:c + chunk] += dotf(act_two_t, grad_up, NN)
        g_ref[:, c:c + chunk] = grad_up
    grad_act_two = dotf(g_ref[...], up_ref[...], NT)
    grad_one = grad_two + norm_back(grad_act_two * gain_two, norm_two, inv_two)
    low_one = grad_one.astype(bf16)
    dout_ref[...] += dotf(attn.T, low_one, NN)
    denc_ref[...] += dotf(feat.T, low_one, NN)
    gattn = dotf(low_one, out_ref[...], NT).astype(bf16)
    width = gattn.shape[1] // heads
    for h in range(heads):
        gattn_ref[h] = gattn[:, h * width:(h + 1) * width]
    down = lambda a: jnp.sum(a, axis=0, keepdims=True)
    loss = jnp.broadcast_to(jnp.sum(weighed * error, axis=0, keepdims=True) / total, (1, bias.shape[1]))
    dvec_ref[...] += jnp.concatenate(
        [down(grad_one), down(grad_act_two * norm_two), down(grad_pred * head_vec * norm_three), down(grad_pred * scaled), loss,
         jnp.zeros((3, bias.shape[1]), f32)], axis=0)


def dense(part, own_counts, counts, attn, feat, target, vec, enc, weights, ff, olds=None, tile=512, chunk=1024):
    heads, rows, cols = attn.shape
    width = enc.shape[1]
    per = rows // tile
    first = olds is None
    target = target.reshape(-1, tile // BLOCK, BLOCK)
    whole = lambda a: pl.BlockSpec(a.shape, lambda i: (0,) * a.ndim, pipeline_mode=pl.Buffered(1))
    keep = lambda s: pl.BlockSpec(s, lambda i: (0,) * len(s), pipeline_mode=pl.Buffered(1))
    shapes = [(ff, width), (width, ff), (width, width), (feat.shape[1], width), (8, width)]
    olds = () if first else tuple(olds)
    kernel, extra = dense_kernel, []
    if len(weights) == 1:
        pieces = weights[0].shape[0] * weights[0].shape[1]
        kernel = functools.partial(packed_dense_kernel, (ff // pieces, width // pieces))
        extra = [pltpu.VMEM((width, width), bf16), pltpu.VMEM((width, ff), bf16), pltpu.VMEM((ff, width), bf16)]
    return pl.pallas_call(
        functools.partial(kernel, first, part, chunk),
        grid=(per,),
        in_specs=[pl.BlockSpec(memory_space=pltpu.SMEM), whole(counts),
                  pl.BlockSpec((heads, tile, cols), lambda i: (0, i, 0)),
                  pl.BlockSpec((tile, feat.shape[1]), lambda i: (part * per + i, 0)),
                  pl.BlockSpec((1, *target.shape[1:]), lambda i: (part * per + i, 0, 0)),
                  whole(vec), whole(enc)] + [whole(w) for w in weights] + [whole(o) for o in olds],
        out_specs=[pl.BlockSpec((heads, tile, cols), lambda i: (0, i, 0))] + [keep(s) for s in shapes],
        out_shape=[jax.ShapeDtypeStruct((heads, rows, cols), bf16)] + [jax.ShapeDtypeStruct(s, f32) for s in shapes],
        scratch_shapes=[pltpu.VMEM((tile, ff), f32), pltpu.VMEM((tile, ff), bf16)] + extra,
        compiler_params=pltpu.CompilerParams(vmem_limit_bytes=67043328),
        cost_estimate=pl.CostEstimate(flops=rows * 5 * 10**7, bytes_accessed=3 * 10**7, transcendentals=0),
        name="dense",
    )(own_counts, counts, attn, feat, target, vec, enc, *weights, *olds)
MESH = pl.DeviceIdType.MESH


def front_kernel(nodes, heads, parts, feat, enc, qkv, vec, down, up, out, out_f, out_e, out_q, out_v, packed, up_s, up_r, down_s, down_r, halo_s, halo_r,
                 w_s, w_r, l_sem, down_v, up_v, out_v2):
    node, head = lax.axis_index("nodes"), lax.axis_index("heads")
    after, before = lax.rem(node + 1, nodes), lax.rem(node + nodes - 1, nodes)
    barrier = pltpu.get_barrier_semaphore()
    for other in (after, before):
        pl.semaphore_signal(barrier, inc=1, device_id=(other, head), device_id_type=MESH)
    for s in range(1, heads):
        pl.semaphore_signal(barrier, inc=1, device_id=(node, lax.rem(head + s, heads)), device_id_type=MESH)
    pl.semaphore_wait(barrier, heads + 1)

    rows = feat.shape[0] // parts
    cut = lambda k: pl.ds(k * rows, rows)

    def relay(step, k, upward):
        shard = jnp.clip(head - step if upward else head + step, 0, heads - 1)
        target = jnp.clip(head + 1 if upward else head - 1, 0, heads - 1)
        sems = (up_s, up_r) if upward else (down_s, down_r)
        src = feat.at[cut(k)] if step == 0 else out_f.at[1, shard, cut(k)]
        return pltpu.make_async_remote_copy(
            src_ref=src, dst_ref=out_f.at[1, shard, cut(k)], send_sem=sems[0].at[step, k], recv_sem=sems[1].at[step, k],
            device_id=(node, target), device_id_type=MESH)

    def halo(shard, k, src, way):
        return pltpu.make_async_remote_copy(
            src_ref=src, dst_ref=out_f.at[0 if way == 0 else 2, shard, cut(k)], send_sem=halo_s.at[way, shard, k], recv_sem=halo_r.at[way, shard, k],
            device_id=(after if way == 0 else before, head), device_id_type=MESH)

    def sends(step, upward):
        return (head - step >= 0) & (head + 1 <= heads - 1) if upward else (head + step <= heads - 1) & (head - 1 >= 0)

    def gets(step, upward):
        return head - 1 - step >= 0 if upward else head + 1 + step <= heads - 1

    for k in range(parts):
        for upward in (True, False):
            @pl.when(sends(0, upward))
            def _(k=k, upward=upward):
                relay(0, k, upward).start()
        for way in range(2):
            halo(head, k, feat.at[cut(k)], way).start()
    own = [pltpu.make_async_copy(feat, out_f.at[1, head], l_sem.at[0]),
           pltpu.make_async_copy(enc, out_e.at[head], l_sem.at[1]),
           pltpu.make_async_copy(qkv.at[head], out_q.at[head], l_sem.at[2]),
           pltpu.make_async_copy(vec, out_v.at[head], l_sem.at[3])]
    own += [pltpu.make_async_copy(src.at[node], dst, l_sem.at[4 + i]) for i, (src, dst) in enumerate(((down, down_v), (up, up_v), (out, out_v2)))]
    for copy in own:
        copy.start()
    for copy in own:
        copy.wait()
    width = out_v2.shape[1]
    rows_down, rows_out = down_v.shape[0], out_v2.shape[0]
    packed[:rows_down, :] = down_v[...].astype(bf16)
    at = rows_down
    for c in range(0, up_v.shape[1], width):
        packed[at:at + rows_out, :] = up_v[:, c:c + width].astype(bf16)
        at += rows_out
    packed[at:at + rows_out, :] = out_v2[...].astype(bf16)

    weights = []
    for step in range(heads - 1):
        if step == heads - 2:
            for s in range(1, heads):
                there = lax.rem(head + s, heads)
                for i, (src, dst) in enumerate(((enc, out_e.at[head]), (qkv.at[there], out_q.at[head]), (vec, out_v.at[head]))):
                    slot = (s - 1) * 3 + i
                    weights.append(pltpu.make_async_remote_copy(
                        src_ref=src, dst_ref=dst, send_sem=w_s.at[slot], recv_sem=w_r.at[slot], device_id=(node, there), device_id_type=MESH))
                    weights[-1].start()
        for k in range(parts):
            for upward in (True, False):
                @pl.when(gets(step, upward))
                def _(step=step, k=k, upward=upward):
                    relay(step, k, upward).wait_recv()
                    if step + 1 < heads - 1:
                        @pl.when(sends(step + 1, upward))
                        def _():
                            relay(step + 1, k, upward).start()
                    shard = head - 1 - step if upward else head + 1 + step
                    for way in range(2):
                        halo(shard, k, out_f.at[1, shard, cut(k)], way).start()
    for step in range(heads - 1):
        for k in range(parts):
            for upward in (True, False):
                @pl.when(sends(step, upward))
                def _(step=step, k=k, upward=upward):
                    relay(step, k, upward).wait_send()
    for copy in weights:
        copy.wait()
    for shard in range(heads):
        for k in range(parts):
            for way in range(2):
                halo(shard, k, feat.at[cut(k)], way).wait()


def front(feat, enc, qkv, vec, down, up, out, nodes, heads, parts=4):
    dma = pltpu.SemaphoreType.DMA
    vmem, anywhere = pl.BlockSpec(memory_space=pltpu.VMEM), pl.BlockSpec(memory_space=pl.ANY)
    n = 3 * (heads - 1)
    width = out.shape[2]
    rows = down.shape[1] + up.shape[1] * up.shape[2] // width + out.shape[1]
    return pl.pallas_call(
        functools.partial(front_kernel, nodes, heads, parts),
        in_specs=[vmem] * 4 + [anywhere] * 3, out_specs=[anywhere] + [vmem] * 4,
        out_shape=[jax.ShapeDtypeStruct((3, heads, *feat.shape), feat.dtype), jax.ShapeDtypeStruct((heads, *enc.shape), enc.dtype),
                   jax.ShapeDtypeStruct(qkv.shape, qkv.dtype), jax.ShapeDtypeStruct((heads, *vec.shape), vec.dtype),
                   jax.ShapeDtypeStruct((rows, width), bf16)],
        scratch_shapes=[dma((heads - 1, parts))] * 4 + [dma((2, heads, parts))] * 2 + [dma((n,))] * 2 + [dma((7,))]
        + [pltpu.VMEM(a.shape[1:], f32) for a in (down, up, out)],
        compiler_params=pltpu.CompilerParams(collective_id=2, has_side_effects=True, vmem_limit_bytes=67043328),
        name="front",
    )(feat, enc, qkv, vec, down, up, out)


def pair_kernel(nodes, heads, down, up, out, *refs):
    slabs, (got_d, got_u, got_o, own_d, own_u, own_o, s_sem, r_sem, l_sem) = refs[:nodes // 2], refs[nodes // 2:]
    node, head = lax.axis_index("nodes"), lax.axis_index("heads")
    chips = nodes // 2
    chip, side = lax.div(node, 2), lax.rem(node, 2)
    twin = chip * 2 + 1 - side
    barrier = pltpu.get_barrier_semaphore()
    pl.semaphore_signal(barrier, inc=1, device_id=(twin, head), device_id_type=MESH)
    pl.semaphore_wait(barrier, 1)
    moves = []
    for i, (src, got, own) in enumerate(((down, got_d, own_d), (up, got_u, own_u), (out, got_o, own_o))):
        local = pltpu.make_async_copy(src.at[:, :, side], own, l_sem.at[i])
        remote = pltpu.make_async_remote_copy(
            src_ref=src.at[:, :, 1 - side], dst_ref=got, send_sem=s_sem.at[i], recv_sem=r_sem.at[i], device_id=(twin, head), device_id_type=MESH)
        local.start()
        remote.start()
        moves.append((local, remote))
    width = out.shape[-1]
    at = 0
    for (local, remote), got, own in zip(moves, (got_d, got_u, got_o), (own_d, own_u, own_o)):
        local.wait()
        remote.wait()
        rows = own.shape[2]
        for c in range(0, own.shape[3], width):
            for s in range(chips):
                there = lax.rem(chip + s, chips)
                slabs[s][:, at:at + rows, :] = (own[:, there, :, c:c + width] + got[:, there, :, c:c + width]).astype(slabs[s].dtype)
            at += rows


def pair(down, up, out, nodes, heads):
    chips = nodes // 2
    split = lambda a: a.reshape(heads, chips, 2, -1, a.shape[-1])
    down, up, out = split(down), split(up), split(out)
    width = out.shape[-1]
    rows = sum(a.shape[3] * a.shape[4] // width for a in (down, up, out))
    half = [pltpu.VMEM((heads, chips, *a.shape[3:]), f32) for a in (down, up, out)]
    dma = pltpu.SemaphoreType.DMA
    return pl.pallas_call(
        functools.partial(pair_kernel, nodes, heads),
        in_specs=[pl.BlockSpec(memory_space=pl.ANY)] * 3, out_specs=[pl.BlockSpec(memory_space=pltpu.VMEM)] * chips,
        out_shape=[jax.ShapeDtypeStruct((heads, rows, width), bf16 if s else f32) for s in range(chips)],
        scratch_shapes=half + half + [dma((3,))] * 3,
        compiler_params=pltpu.CompilerParams(collective_id=3, has_side_effects=True, vmem_limit_bytes=67043328),
        cost_estimate=pl.CostEstimate(flops=10**10, bytes_accessed=2 * 10**7, transcendentals=0),
        name="pair",
    )(down, up, out)


def send(src, dst, sems, slot, node, head):
    copy = pltpu.make_async_remote_copy(
        src_ref=src, dst_ref=dst, send_sem=sems[0].at[slot], recv_sem=sems[1].at[slot], device_id=(node, head), device_id_type=MESH)
    copy.start()
    return copy


def greet(nodes, heads, node, head):
    barrier = pltpu.get_barrier_semaphore()
    for s in range(1, nodes):
        pl.semaphore_signal(barrier, inc=1, device_id=(lax.rem(node + s, nodes), head), device_id_type=MESH)
    for s in range(1, heads):
        pl.semaphore_signal(barrier, inc=1, device_id=(node, lax.rem(head + s, heads)), device_id_type=MESH)
    pl.semaphore_wait(barrier, nodes + heads - 2)


def finish_kernel(nodes, heads, *refs):
    (qkv, enc, vec, *bulk), refs = refs[:4], refs[4:]
    (out_q, out_e, out_v, *out_b), refs = refs[:4], refs[4:]
    (q_half, q_one, q_two, q_part, q_sum, q_own, e_half, e_one, e_two, e_sum, e_three, e_own, v_half, v_two, v_three, v_one, v_sum), refs = refs[:17], refs[17:]
    s_one, r_one, s_two, r_two, s_three, r_three, s_four, r_four, s_bulk, r_bulk, s_pass, r_pass, l_sem, piece = refs
    node, head = lax.axis_index("nodes"), lax.axis_index("heads")
    chips = nodes // 2
    chip, side = lax.div(node, 2), lax.rem(node, 2)
    twin = chip * 2 + 1 - side
    cuts = 3 if piece.shape[0] % 24 == 0 else 1
    step = piece.shape[0] // cuts
    piece[...] = functools.reduce(jnp.add, [bulk[0][h] for h in range(heads)])
    greet(nodes, heads, node, head)
    first = [send(ref.at[:, :, 1 - side], dst, (s_one, r_one), i, twin, head) for i, (ref, dst) in enumerate(((qkv, q_half), (enc, e_half)))]
    first.append(send(vec, v_half, (s_one, r_one), 2, twin, head))
    keep = [pltpu.make_async_copy(src, dst.at[node], l_sem.at[i]) for i, (src, dst) in enumerate(zip((piece,), out_b))]
    for copy in keep:
        copy.start()
    spread = {}

    def bulk_out(which):
        for k in which:
            for s in range(chips):
                other = lax.rem(chip + s, chips) * 2 + side if s else twin
                at = pl.ds(k * step, step)
                spread[k, s] = send(piece.at[at], out_b[0].at[node, at], (s_bulk, r_bulk), k * chips + s, other, head)

    bulk_out(range(1))
    for copy in first:
        copy.wait()
    q_one[...] = qkv[:, :, side] + q_half[...]
    e_one[...] = enc[:, :, side] + e_half[...]
    v_one[...] = vec[...] + v_half[...]
    second = []
    for s in range(1, chips):
        there = lax.rem(chip + s, chips)
        target = there * 2 + side
        i = (s - 1) * 3
        second.append(send(q_one.at[:, there], q_two.at[s - 1], (s_two, r_two), i, target, head))
        second.append(send(e_one.at[:, there], e_two.at[s - 1], (s_two, r_two), i + 1, target, head))
        second.append(send(v_one, v_two.at[s - 1], (s_two, r_two), i + 2, target, head))
    bulk_out(range(1, cuts))
    for copy in second:
        copy.wait()
    q_part[...] = functools.reduce(jnp.add, [q_two[s] for s in range(chips - 1)], q_one[:, chip])
    e_sum[...] = functools.reduce(jnp.add, [e_two[s] for s in range(chips - 1)], e_one[:, chip])
    v_sum[...] = functools.reduce(jnp.add, [v_two[s] for s in range(chips - 1)], v_one[...])
    third = []
    for s in range(1, heads):
        there = lax.rem(head + s, heads)
        i = (s - 1) * 3
        third.append(send(q_part.at[there], q_sum.at[head], (s_three, r_three), i, node, there))
        third.append(send(e_sum.at[there], e_three.at[s - 1], (s_three, r_three), i + 1, node, there))
        third.append(send(v_sum, v_three.at[s - 1], (s_three, r_three), i + 2, node, there))
    for copy in third:
        copy.wait()
    q_sum[pl.ds(head, 1)] = q_part[pl.ds(head, 1)]
    e_own[...] = functools.reduce(jnp.add, [e_three[s] for s in range(heads - 1)], e_sum[head])
    out_v[...] = functools.reduce(jnp.add, [v_three[s] for s in range(heads - 1)], v_sum[...])
    fourth = []
    for s in range(1, nodes):
        there = lax.rem(node + s, nodes)
        fourth.append(send(q_sum, out_q.at[node], (s_four, r_four), (s - 1) * 2, there, head))
        fourth.append(send(e_own, out_e.at[node], (s_four, r_four), (s - 1) * 2 + 1, there, head))
    out_q[node] = q_sum[...]
    out_e[node] = e_own[...]
    for copy in keep:
        copy.wait()
    passed = []
    for k in range(cuts):
        for s in range(chips):
            spread[k, s].wait()
            if s:
                origin = lax.rem(chip + chips - s, chips) * 2 + side
                here = out_b[0].at[origin, pl.ds(k * step, step)]
                passed.append(send(here, here, (s_pass, r_pass), k * (chips - 1) + s - 1, twin, head))
    for copy in passed:
        copy.wait()
    for copy in fourth:
        copy.wait()


def finish(qkv, enc, vec, bulk, nodes, heads):
    chips = nodes // 2
    split = lambda a: a.reshape(heads, chips, 2, -1, a.shape[-1])
    qkv, enc = split(qkv), split(enc)
    vm = lambda *s: pltpu.VMEM(s, f32)
    rq, wq, re, we = *qkv.shape[3:], *enc.shape[3:]
    dma = pltpu.SemaphoreType.DMA
    wv = vec.shape
    scratch = [vm(heads, chips, rq, wq), vm(heads, chips, rq, wq), vm(chips - 1, heads, rq, wq), vm(heads, rq, wq), vm(heads, rq, wq), vm(8, 128),
               vm(heads, chips, re, we), vm(heads, chips, re, we), vm(chips - 1, heads, re, we), vm(heads, re, we), vm(heads - 1, re, we), vm(re, we),
               vm(*wv), vm(chips - 1, *wv), vm(heads - 1, *wv), vm(*wv), vm(*wv)]
    counts = (3, 3, 3 * chips - 3, 3 * chips - 3, 3 * heads - 3, 3 * heads - 3, 2 * nodes - 2, 2 * nodes - 2, 3 * chips, 3 * chips, 3 * chips - 3, 3 * chips - 3, 1)
    out_shape = [jax.ShapeDtypeStruct(s, f32) for s in [(nodes, heads, rq, wq), (nodes, re, we), wv] + [(nodes, *b.shape[1:]) for b in bulk]]
    spec = pl.BlockSpec(memory_space=pltpu.VMEM)
    return pl.pallas_call(
        functools.partial(finish_kernel, nodes, heads),
        in_specs=[spec] * 4, out_specs=[spec] * 4, out_shape=out_shape,
        scratch_shapes=scratch + [dma((n,)) for n in counts] + [vm(*bulk[0].shape[1:])],
        compiler_params=pltpu.CompilerParams(collective_id=1, has_side_effects=True, vmem_limit_bytes=48 << 20),
        name="finish",
    )(qkv, enc, vec, *bulk)
D = 512
HEADS = 8
NBR = 8
ADAM_STEP = 3
highest = lax.Precision.HIGHEST
beta_one = 0.5
beta_two = 0.5
learn_rate = 0.02
weight_decay = 0.1
adam_eps = 1e-08


def adamw(weight, first_moment, second, gradient):
    first_new = beta_one * first_moment + (1.0 - beta_one) * gradient
    second_new = beta_two * second + (1.0 - beta_two) * gradient * gradient
    first_hat = first_new / (1.0 - beta_one**ADAM_STEP)
    second_hat = second_new / (1.0 - beta_two**ADAM_STEP)
    weight_new = weight - learn_rate * (
        first_hat / (jnp.sqrt(second_hat) + adam_eps) + weight_decay * weight
    )
    return (weight_new, first_new, second_new)


def local(
    features, target, counts, neighbours, edge_kinds,
    enc_weight, enc_first, enc_second, qkv_weight, qkv_first, qkv_second,
    out_weight, out_first, out_second, up_weight, up_first, up_second,
    down_weight, down_first, down_second, vec_weight, vec_first, vec_second,
):
    heads_count = lax.axis_size("heads")
    nodes_count = lax.axis_size("nodes")
    head_index = lax.axis_index("heads")
    node_index = lax.axis_index("nodes")
    row_count = features.shape[0]
    own_blocks = row_count // BLOCK
    group_blocks = own_blocks * heads_count
    group_rows = group_blocks * BLOCK
    hl = HEADS // heads_count
    hs = D // HEADS
    cols = hl * hs
    cp = -(-cols // 128) * 128
    ka = -(-(cols + 1) // 128) * 128
    kinds = D // HEADS
    slots = NBR + 1
    low = lambda a: a.astype(bf16)
    gather = lambda a, axis: lax.all_gather(low(a), "heads", axis=axis, tiled=True)

    qkv_parts = jnp.transpose(low(qkv_weight).reshape(-1, heads_count, hl, 3, hs), (1, 0, 3, 2, 4)).reshape(heads_count, -1, 3, cols)
    qkv_parts = jnp.pad(qkv_parts, ((0, 0), (0, 0), (0, 0), (0, cp - cols))).reshape(heads_count, -1, 3 * cp)
    vec_part = jnp.pad(low(vec_weight).astype(f32), ((0, 2), (0, 0)))
    ff = up_weight.shape[1]
    pieces = heads_count * nodes_count
    rows_down, rows_out = ff // pieces, D // pieces
    by_node = lambda a: a.reshape(nodes_count, -1, a.shape[1])
    feats, enc_b, qkv_cols, vectors, packed = front(
        features, low(enc_weight), qkv_parts, vec_part, by_node(down_weight), by_node(up_weight), by_node(out_weight), nodes_count, heads_count)
    feats = feats.reshape(3 * group_rows, -1)
    enc_b = enc_b.reshape(-1, D)
    qkv_cols = qkv_cols.reshape(D, 3 * cp)
    vectors = jnp.transpose(vectors, (1, 0, 2)).reshape(8, D)
    packed = lax.all_gather(packed, ("heads", "nodes"), axis=0, tiled=False).reshape(heads_count, nodes_count, -1, D)

    enc_bias, gain_one, gain_two, gain_three, head_vec = (vectors[r] for r in range(5))
    edge_local = lax.dynamic_slice_in_dim(vectors[5].reshape(kinds, HEADS), head_index * hl, hl, 1)
    own_counts = lax.dynamic_slice_in_dim(counts, (node_index * heads_count + head_index) * own_blocks, own_blocks)

    def group_counts(offset):
        return lax.dynamic_slice_in_dim(counts, (node_index + offset) % nodes_count * group_blocks, group_blocks)

    pool_counts = jnp.concatenate([group_counts(nodes_count - 1), group_counts(0), group_counts(1)])
    relative = (neighbours // group_blocks - node_index + 1) % nodes_count
    nbr_pos = relative * group_blocks + neighbours % group_blocks
    self_pos = group_blocks + jnp.arange(group_blocks, dtype=jnp.int32)
    key_pos = jnp.concatenate([self_pos[:, None], nbr_pos], axis=1).reshape(-1)
    kind_hot = jax.nn.one_hot(edge_kinds, kinds, dtype=f32)
    slot_bias = jnp.einsum("bst,th->bsh", kind_hot, edge_local, precision=highest)
    bias_rows = jnp.repeat(slot_bias, BLOCK, axis=2)

    kaug, kt, value, vt, query = encode(
        pool_counts, feats, enc_b, enc_bias[None], gain_one[None], qkv_cols, cp, ka, cols, hs**-0.5)
    half = lambda a: a.reshape(heads_count, 2, row_count // 2, -1)
    exchange = lambda a: lax.all_to_all(a, "heads", split_axis=0, concat_axis=0, tiled=True)
    attn_parts, lse_parts, grad_parts, totals = [], [], [], None
    for part in range(2):
        attn_part, lse_part = attend(part, own_blocks, key_pos, query, bias_rows, kaug, vt, hl, hs)
        attn_parts.append(attn_part)
        lse_parts.append(lse_part)
    packed, attn_parts[1] = lax.optimization_barrier((packed, attn_parts[1]))
    weights = (packed,)
    if rows_out % 16:
        up_rows = packed[:, :, rows_down:-rows_out].reshape(pieces, -1, rows_out, D)
        weights = (packed[:, :, -rows_out:].reshape(D, D), jnp.transpose(up_rows, (0, 2, 1, 3)).reshape(D, ff), packed[:, :, :rows_down].reshape(ff, D))
    for part in range(2):
        attn_rows = exchange(attn_parts[part].reshape(heads_count, row_count // 2, cp)[..., :cols])
        grad_part, *totals = dense(part, own_counts, counts.reshape(-1, BLOCK), attn_rows, features, target, vectors, enc_b, weights, ff, totals)
        grad_parts.append(exchange(grad_part))
    grad_down, grad_up, grad_out, denc_own, dense_sums = totals
    grad_parts[0], grad_down = lax.optimization_barrier((grad_parts[0], grad_down))
    slab = pair(grad_down, grad_up, grad_out, nodes_count, heads_count)
    moved = [slab[0]] + [
        lax.ppermute(slab[s], "nodes", [(i, (i + 2 * s) % nodes_count) for i in range(nodes_count)]) for s in range(1, nodes_count // 2)]
    grad_heads = [jnp.pad(g.reshape(group_rows // 2, cols), ((0, 0), (0, cp - cols))) for g in grad_parts]
    dq, dkv, edge_sums = attend_back(own_blocks, key_pos, query, grad_heads, attn_parts, lse_parts, bias_rows, kaug, value, kt, hl, hs)
    moved, dkv = lax.optimization_barrier((moved, dkv))
    planes = exchange(functools.reduce(jnp.add, [a.astype(f32) for a in moved]))
    slot_sums = jnp.sum(edge_sums.reshape(group_blocks, slots, hl, BLOCK), axis=3)
    edge_grad = jnp.einsum("bst,bsh->th", kind_hot, slot_sums, precision=highest)
    edge_full = lax.dynamic_update_slice(jnp.zeros((kinds, HEADS), f32), edge_grad, (jnp.int32(0), head_index * hl)).reshape(1, D)
    dw, grad_enc, grad_vec = encode_back(feats, dkv, dq, enc_b, vectors, qkv_cols, denc_own, dense_sums, edge_full)
    planes, dw = lax.optimization_barrier((planes, dw))
    dw_sum, enc_sum, vec_total, bulk = finish(dw, grad_enc, grad_vec, [planes], nodes_count, heads_count)
    vec_sum = lax.dynamic_slice_in_dim(jnp.concatenate([vec_total[:5], vec_total[6:7]]), head_index * (D // heads_count), D // heads_count, 1)
    states = (enc_weight, enc_first, enc_second, qkv_weight, qkv_first, qkv_second, out_weight, out_first, out_second,
              up_weight, up_first, up_second, down_weight, down_first, down_second)
    vec_res = adamw(vec_weight, vec_first, vec_second, vec_sum)
    if rows_out % 16:
        qkv_sum = jnp.transpose(dw_sum, (0, 2, 1, 3)).reshape(-1, heads_count, 3, cp)[..., :cols].reshape(-1, heads_count, 3, hl, hs)
        qkv_sum = jnp.transpose(qkv_sum, (0, 1, 3, 2, 4)).reshape(qkv_weight.shape)
        flat = lambda a: a.reshape(-1, a.shape[-1])
        up_sum = bulk[:, rows_down:-rows_out].reshape(nodes_count, -1, rows_out, D)
        up_sum = jnp.transpose(up_sum, (0, 2, 1, 3)).reshape(up_weight.shape)
        summed = (flat(enc_sum), qkv_sum, flat(bulk[:, -rows_out:]), up_sum, flat(bulk[:, :rows_down]))
        results = []
        for n, grad in enumerate(summed):
            results += adamw(*states[3 * n:3 * n + 3], grad)
        results += [low(r) for r in results[::3]]
    else:
        results = adam(enc_sum, dw_sum, bulk, states, hl, hs, cp)
    loss_value = vec_total[5, :1]
    return (loss_value, *results[:15], *vec_res, *results[15:])


def solution(mesh):
    rows = P("heads", None)
    both = P(("nodes", "heads"))
    lanes = P(None, "heads")
    in_specs = (P(("nodes", "heads"), None), both, P(), P("nodes", None), P("nodes", None)) + (rows,) * 15 + (lanes,) * 3
    out_specs = (P(),) + (rows,) * 15 + (lanes,) * 3 + (rows,) * 5
    return jax.shard_map(local, mesh=mesh, in_specs=in_specs, out_specs=out_specs, check_vma=False)


def adam_kernel(hl, hs, cp, *refs):
    g_enc, g_qkv, g_bulk = refs[:3]
    ins, outs = refs[3:18], refs[18:]
    rows_down, rows_out = ins[12].shape[0], ins[6].shape[0]
    heads = g_qkv.shape[1]
    bulk = g_bulk[0]
    parts = []
    for h in range(heads):
        part = g_qkv[0, h]
        for k in range(hl):
            parts += [part[:, j * cp + k * hs:j * cp + (k + 1) * hs] for j in range(3)]
    up_at = lambda c: rows_down + c * rows_out
    grads = [g_enc[0], jnp.concatenate(parts, axis=1), bulk[-rows_out:],
             jnp.concatenate([bulk[up_at(c):up_at(c) + rows_out] for c in range(ins[9].shape[1] // bulk.shape[1])], axis=1), bulk[:rows_down]]
    for n, grad in enumerate(grads):
        new = adamw(*(ref[...] for ref in ins[3 * n:3 * n + 3]), grad)
        for ref, value in zip(outs[3 * n:3 * n + 3], new):
            ref[...] = value
        outs[15 + n][...] = new[0].astype(bf16)


def adam(g_enc, g_qkv, g_bulk, states, hl, hs, cp):
    nodes = g_enc.shape[0]
    rows = lambda a: pl.BlockSpec((a.shape[0] // nodes, a.shape[1]), lambda i: (i, 0))
    lead = lambda a: pl.BlockSpec((1, *a.shape[1:]), lambda i: (i,) + (0,) * (a.ndim - 1))
    shapes = [jax.ShapeDtypeStruct(a.shape, f32) for a in states] + [jax.ShapeDtypeStruct(a.shape, bf16) for a in states[::3]]
    return pl.pallas_call(
        functools.partial(adam_kernel, hl, hs, cp),
        grid=(nodes,),
        in_specs=[lead(g_enc), lead(g_qkv), lead(g_bulk)] + [rows(a) for a in states],
        out_specs=[rows(a) for a in shapes], out_shape=shapes,
        compiler_params=pltpu.CompilerParams(vmem_limit_bytes=67043328),
        name="adam",
    )(g_enc, g_qkv, g_bulk, *states)
```
